32 devices in a mesh: seq: 8 (over z, x), head: 4 (over y, core).
Axes of the slice: x: 2, y: 2, z: 4, core: 2. Of those that a mesh axis runs over, the one named last changes fastest.
Arguments:
- queries: bfloat16 [8192, 4096], P('seq', 'head'), may hold values from -8 to 8
- key_rows: bfloat16 [8192, 4096], P('seq', 'head'), may hold values from -8 to 8
- value_rows: bfloat16 [8192, 4096], P('seq', 'head'), may hold values from -6 to 6
- random_owner: int32 [128, 3], P('seq'), may hold values from 0 to 7, all different within a row; in each aligned block of 16 rows (0 to 15, 16 to 31, ...) at most 8 rows name the same one
- random_local: int32 [128, 3], P('seq'), may hold values from 0 to 15
- output_weight: bfloat16 [4096, 4096], P('head'), may hold values from -0.09375 to 0.09375
Outputs:
- layer_output: bfloat16 [8192, 4096], P(('seq', 'head'))
The draws below stay inside these ranges and needn't reach their ends.
Inputs may be any that keep to these rules, and one draw needn't show every extreme that they name: `random_owner`: each row names 3 different owners. Among the rows of one device (16 aligned rows) no owner is named more than 8 times, and in some device's rows one owner is named exactly 8 times.
All inputs are finite; a program needn't handle non-finite values.
Results may differ from the reference program's by a relative error of at most 0.0052.
Values may be sent and summed in bfloat16 or wider, within the bound.
A program may use at most 192 MiB of HBM per device.

```python
import math
import jax
import jax.numpy as jnp
import numpy as np
from jax import lax

D = 4096
HEADS = 32
HEAD_DIM = 128
BLOCK = 64
RANDOM = 3
GLOBAL = 128
NB_DEV = 16
CAP = 8
NBLK = 128
TOKENS = 8192
N_SEQ = 8


def query_key_pair(key):
    folded = jax.random.fold_in(key, 11)
    streams = jax.random.split(folded, 8)
    total_width = HEADS * HEAD_DIM
    row_ids = jnp.arange(TOKENS, dtype=jnp.int32)[:, None]
    query_scale = jnp.where(row_ids < GLOBAL, 3.0, 2.0)
    query_values = jax.random.normal(streams[0], (TOKENS, total_width), jnp.float32) * query_scale
    key_values = jax.random.normal(streams[1], (TOKENS, total_width), jnp.float32)
    return (jnp.clip(query_values, -8.0, 8.0), jnp.clip(key_values, -8.0, 8.0))


def draw_queries(key, part):
    return query_key_pair(key)[0].astype(jnp.bfloat16)


def draw_key_rows(key, part):
    return query_key_pair(key)[1].astype(jnp.bfloat16)


def with_ends(values, key, low, largest):
    longest = values.shape.index(max(values.shape))
    spots = []
    for shift in (0, 1):
        where = [jax.random.randint(jax.random.fold_in(key, axis), (), 0, length) for axis, length in enumerate(values.shape)]
        where[longest] = (where[longest] + shift) % values.shape[longest]
        spots.append(tuple(where))
    return values.at[spots[0]].set(low).at[spots[1]].set(largest)


def level_of(stream_key, extent, cuts, low, high):
    gain = 1.0
    for dim, shards_of in cuts:
        steps = jax.random.uniform(jax.random.fold_in(jax.random.fold_in(stream_key, 6), dim), (shards_of,), jnp.float32, low / len(cuts), high / len(cuts))
        gain = gain * jnp.repeat(jnp.exp(steps), extent[dim] // shards_of).reshape((-1,) + (1,) * (len(extent) - 1 - dim))
    return gain


def assign_block(rng, own, number, rows, amount, top, most, slope):
    order = jax.random.permutation(rng, amount)
    crowded, common = shares(amount, rows * top, most, slope, True), shares(amount, rows * top, most, slope, False)
    places = jnp.arange(amount)

    def named(tallies, turn):
        used = int((tallies > 0).sum())
        fixed = max(1, used // 4)
        passed = fixed + (places - fixed + turn * (used - fixed)) % max(1, amount - fixed)
        return jnp.zeros((amount,), jnp.int32).at[order[jnp.where(places < fixed, places, passed)]].set(jnp.asarray(tallies, jnp.int32))

    tallies = jnp.where(number % 4 == 0, named(crowded, number // 4), named(common, number - number // 4 - 1))
    mixed = jax.random.permutation(jax.random.fold_in(own, 3), amount)
    giver, taker = mixed[0:amount // 2 * 2:2], mixed[1:amount // 2 * 2:2]
    margin = jnp.minimum(tallies[giver] - 1, most - tallies[taker]) // 2
    margin = jnp.where((giver == order[0]) | (taker == order[0]) | (tallies[taker] == 0), 0, jnp.maximum(margin, 0))
    passed = jax.random.randint(jax.random.fold_in(own, 4), (amount // 2,), 0, 1 << 20) % (margin + 1)
    tallies = tallies.at[giver].add(-passed).at[taker].add(passed)
    labels = jnp.searchsorted(jnp.cumsum(tallies), jnp.arange(rows * top), side="right").astype(jnp.int32)
    listing = labels.reshape(top, rows).T
    listing = listing[jax.random.permutation(jax.random.fold_in(own, 1), rows)]
    turn = jax.random.randint(jax.random.fold_in(own, 2), (rows, 1), 0, top)
    return jnp.take_along_axis(listing, (jnp.arange(top)[None, :] + turn) % top, axis=1)


def shares(number_of, total, bound, slope, full):
    weights = [(1 << 20) // math.isqrt(grade ** slope) + 1 for grade in range(1, number_of + 1)]
    largest = bound if full else min(bound, max(-(-total // number_of), total * weights[0] // sum(weights)))
    least = 1 if total - largest >= number_of - 1 else 0
    counts, surplus = [largest] + [least] * (number_of - 1), total - largest - least * (number_of - 1)
    while surplus > 0:
        movable = [i for i in range(1, number_of) if counts[i] < largest] or [i for i in range(1, number_of) if counts[i] < bound]
        mass, budget = sum([weights[i] for i in movable]), surplus
        for i in movable:
            extra = min(bound - counts[i], max(1, budget * weights[i] // mass), surplus)
            counts[i] = counts[i] + extra
            surplus = surplus - extra
    return np.array(counts)


def noise(own_key, dims, spread, limit, cuts=(), kind=jnp.bfloat16):
    level = level_of(own_key, dims, cuts, -0.22, 0.18) if cuts else 1.0
    values = jax.random.normal(own_key, dims, jnp.float32) * spread * level
    return jnp.minimum(jnp.maximum(values, -limit), limit).astype(kind)


def setup_inputs(seed: int = 0) -> dict:
    arg_keys = jax.random.split(jax.random.key(seed), 7)
    queries = draw_queries(jax.random.fold_in(arg_keys[6], 71), 0)
    key_rows = draw_key_rows(jax.random.fold_in(arg_keys[6], 71), 0)
    value_rows = noise(arg_keys[2], (TOKENS, HEADS * HEAD_DIM), 1.0, 6.0, ((0, 8), (1, 4)))
    random_owner_keys = jax.random.split(jax.random.fold_in(arg_keys[3], 1), NBLK // NB_DEV)
    random_owner_turns = jax.random.permutation(jax.random.fold_in(arg_keys[3], 3), NBLK // NB_DEV)
    random_owner = jax.vmap(lambda own, number: assign_block(jax.random.fold_in(arg_keys[3], 2), own, number, NB_DEV, NBLK // NB_DEV, RANDOM, CAP, 2))(random_owner_keys, random_owner_turns).reshape((NBLK, RANDOM))
    random_local = with_ends(jax.random.randint(arg_keys[4], (NBLK, RANDOM), 0, NB_DEV), jax.random.fold_in(arg_keys[4], 1), 0, NB_DEV - 1).astype(jnp.int32)
    output_weight = noise(arg_keys[5], (HEADS * HEAD_DIM, D), (HEADS * HEAD_DIM) ** -0.5, 0.09375, ((0, 4),))
    return dict(queries=queries, key_rows=key_rows, value_rows=value_rows, random_owner=random_owner, random_local=random_local, output_weight=output_weight)


masked_score = -1e30


def sparse_block(block_index, queries, key_padded, value_padded, key_rows, value_rows, random_block):
    score_scale = HEAD_DIM ** -0.5
    first_row = block_index * BLOCK
    query_block = lax.dynamic_slice_in_dim(queries, first_row, BLOCK, 0)
    window_keys = lax.dynamic_slice_in_dim(key_padded, first_row, 3 * BLOCK, 0)
    window_values = lax.dynamic_slice_in_dim(value_padded, first_row, 3 * BLOCK, 0)
    picked = random_block[block_index]
    offsets = (picked[:, None] * BLOCK + jnp.arange(BLOCK, dtype=jnp.int32)[None, :]).reshape(-1).astype(jnp.int32)
    random_keys = jnp.take(key_rows, offsets, axis=0)
    random_values = jnp.take(value_rows, offsets, axis=0)
    listed_keys = jnp.concatenate([window_keys, random_keys, key_rows[:GLOBAL]], axis=0)
    listed_values = jnp.concatenate([window_values, random_values, value_rows[:GLOBAL]], axis=0)
    listed = listed_keys.shape[0]
    slot_number = jnp.arange(listed, dtype=jnp.int32) // BLOCK
    usable = jnp.logical_and(jnp.logical_or(slot_number != 0, block_index > 0), jnp.logical_or(slot_number != 2, block_index < NBLK - 1))
    query_heads = query_block.astype(jnp.float32).reshape(BLOCK, HEADS, HEAD_DIM)
    key_heads = listed_keys.astype(jnp.float32).reshape(listed, HEADS, HEAD_DIM)
    value_heads = listed_values.astype(jnp.float32).reshape(listed, HEADS, HEAD_DIM)
    scores = jnp.einsum("qhd,khd->hqk", query_heads, key_heads) * score_scale
    scores = jnp.where(usable[None, None, :], scores, masked_score)
    row_max = jnp.max(scores, axis=2, keepdims=True)
    weight = jnp.where(usable[None, None, :], jnp.exp(scores - row_max), 0.0)
    row_total = jnp.sum(weight, axis=2)
    rounded = lax.optimization_barrier(weight.astype(jnp.bfloat16)).astype(jnp.float32)
    context = jnp.einsum("hqk,khd->qhd", rounded, value_heads) / jnp.transpose(row_total)[:, :, None]
    return context.reshape(BLOCK, HEADS * HEAD_DIM).astype(jnp.bfloat16)


def segment_part(segment, global_query, key_rows, value_rows):
    segment_rows = NB_DEV * BLOCK
    score_scale = HEAD_DIM ** -0.5
    segment_keys = lax.dynamic_slice_in_dim(key_rows, segment * segment_rows, segment_rows, 0)
    segment_values = lax.dynamic_slice_in_dim(value_rows, segment * segment_rows, segment_rows, 0)
    query_heads = global_query.astype(jnp.float32).reshape(GLOBAL, HEADS, HEAD_DIM)
    key_heads = segment_keys.astype(jnp.float32).reshape(segment_rows, HEADS, HEAD_DIM)
    value_heads = segment_values.astype(jnp.float32).reshape(segment_rows, HEADS, HEAD_DIM)
    scores = jnp.einsum("qhd,khd->hqk", query_heads, key_heads) * score_scale
    row_max = jnp.max(scores, axis=2)
    weight = jnp.exp(scores - row_max[:, :, None])
    row_total = jnp.sum(weight, axis=2)
    rounded = lax.optimization_barrier(weight.astype(jnp.bfloat16)).astype(jnp.float32)
    partial_value = jnp.einsum("hqk,khd->hqd", rounded, value_heads)
    return row_max, row_total, partial_value


def reference(queries, key_rows, value_rows, random_owner, random_local, output_weight):
    random_block = (random_owner * NB_DEV + random_local).astype(jnp.int32)
    total_width = HEADS * HEAD_DIM
    zero_block = jnp.zeros((BLOCK, total_width), key_rows.dtype)
    key_padded = jnp.concatenate([zero_block, key_rows, zero_block], axis=0)
    value_padded = jnp.concatenate([zero_block, value_rows, zero_block], axis=0)

    def one_block(block_index):
        return sparse_block(block_index, queries, key_padded, value_padded, key_rows, value_rows, random_block)

    sparse = lax.map(one_block, jnp.arange(NBLK, dtype=jnp.int32)).reshape(TOKENS, total_width)
    global_query = queries[:GLOBAL]

    def one_segment(segment):
        return segment_part(segment, global_query, key_rows, value_rows)

    segment_max, segment_total, segment_acc = lax.map(one_segment, jnp.arange(N_SEQ, dtype=jnp.int32))
    overall_max = jnp.max(segment_max, axis=0)
    factor = jnp.exp(segment_max - overall_max[None])
    global_out = jnp.sum(factor[..., None] * segment_acc, axis=0) / jnp.sum(factor * segment_total, axis=0)[..., None]
    global_out = jnp.transpose(global_out, (1, 0, 2)).reshape(GLOBAL, total_width)
    attention = jnp.concatenate([global_out.astype(jnp.bfloat16), sparse[GLOBAL:]], axis=0)
    return jnp.dot(attention, output_weight, preferred_element_type=jnp.float32).astype(jnp.bfloat16)
```

```python
import functools
import math

import jax
import jax.numpy as jnp
from jax import lax
from jax.experimental import pallas as pl
from jax.experimental.pallas import tpu as pltpu
from jax.sharding import PartitionSpec as P

HEAD_DIM = 128
BLOCK = 64
RANDOM = 3
GLOBAL = 128
CHUNKS = 2
PAIR = 2


masked_score = -1e30


def slot_table(owner_ids, local_ids, seq_count, slot_count):
    owner_hits = (owner_ids[:, None] == jnp.arange(seq_count, dtype=jnp.int32)[None, :]).astype(
        jnp.int32
    )
    earlier = jnp.cumsum(owner_hits, axis=0) - owner_hits
    slot_ids = jnp.sum(earlier * owner_hits, axis=1)
    slot_hits = (slot_ids[:, None] == jnp.arange(slot_count, dtype=jnp.int32)[None, :]).astype(
        jnp.int32
    )
    request_table = jnp.sum(
        (owner_hits * local_ids[:, None])[:, :, None] * slot_hits[:, None, :], axis=0
    )
    return (request_table, slot_ids)


def attend_kernel(heads, index_ref, flag_ref, q_ref, *refs):
    near, out_ref = refs[:-1], refs[-1]
    step = pl.program_id(0)
    rate = HEAD_DIM ** (-0.5) * math.log2(math.e)
    first, last = flag_ref[0, step], flag_ref[1, step]
    listed = len(near) * BLOCK
    column = lax.broadcasted_iota(jnp.int32, (1, listed), 1) // BLOCK
    hidden = jnp.logical_or(
        jnp.logical_and(column == 0, first == 1), jnp.logical_and(column == 2, last == 1)
    )
    bias = jnp.where(hidden, masked_score, 0.0).astype(jnp.float32)
    for head in range(heads):
        here = pl.ds(head * HEAD_DIM, HEAD_DIM)
        keys = jnp.concatenate([ref[0, 0, :, here] for ref in near], axis=0)
        values = jnp.concatenate([ref[0, 1, :, here] for ref in near], axis=0)
        scores = lax.dot_general(
            q_ref[:, here], keys, (((1,), (1,)), ((), ())), preferred_element_type=jnp.float32
        )
        scores = scores + bias
        top = jnp.max(scores, axis=1, keepdims=True)
        weight = jnp.exp2((scores - top) * rate)
        total = jnp.sum(weight, axis=1, keepdims=True)
        context = jnp.dot(
            weight.astype(jnp.bfloat16), values, preferred_element_type=jnp.float32
        )
        out_ref[:, here] = (context / total).astype(out_ref.dtype)


def attend(queries, pool, index, flags):
    tokens, width = queries.shape
    blocks = tokens // BLOCK
    heads = width // HEAD_DIM
    listed = index.shape[0]

    def picked(r):
        return pl.BlockSpec(
            (1, 2, BLOCK, width), lambda i, index_ref, flag_ref: (index_ref[r, i], 0, 0, 0)
        )

    return pl.pallas_call(
        functools.partial(attend_kernel, heads),
        grid_spec=pltpu.PrefetchScalarGridSpec(
            num_scalar_prefetch=2,
            grid=(blocks,),
            in_specs=[pl.BlockSpec((BLOCK, width), lambda i, a, b: (i, 0))]
            + [picked(r) for r in range(listed)],
            out_specs=pl.BlockSpec((BLOCK, width), lambda i, a, b: (i, 0)),
        ),
        out_shape=jax.ShapeDtypeStruct(queries.shape, jnp.bfloat16),
        compiler_params=pltpu.CompilerParams(dimension_semantics=("arbitrary",)),
        cost_estimate=pl.CostEstimate(
            flops=60 * tokens * width * 8 * BLOCK,
            bytes_accessed=blocks * 14 * BLOCK * width * 2,
            transcendentals=tokens * heads * 8 * BLOCK,
        ),
    )(index, flags, queries, *([pool] * listed))


def merged(left, right):
    joint = jnp.maximum(left[0], right[0])
    a, b = jnp.exp(left[0] - joint), jnp.exp(right[0] - joint)
    return (
        joint,
        left[1] * a + right[1] * b,
        left[2] * a[:, :, None] + right[2] * b[:, :, None],
    )


def partial_softmax(query, keys, values):
    tokens, width = query.shape
    heads = width // HEAD_DIM
    query = query.reshape(tokens, heads, HEAD_DIM)
    keys, values = (a.reshape(-1, heads, HEAD_DIM) for a in (keys, values))
    scores = jnp.einsum("qhd,khd->hqk", query, keys, preferred_element_type=jnp.float32)
    scores = scores * HEAD_DIM ** (-0.5)
    row_max = jnp.max(scores, axis=2)
    weight = jnp.exp(scores - row_max[:, :, None])
    row_total = jnp.sum(weight, axis=2)
    value = jnp.einsum(
        "hqk,khd->hqd", weight.astype(jnp.bfloat16), values, preferred_element_type=jnp.float32
    )
    return row_max, row_total, value


def after(array, *others):
    return lax.optimization_barrier((array,) + others)[0]


def local_plain(queries, key_rows, value_rows, random_owner, random_local, output_weight):
    n = lax.axis_size("seq")
    me = lax.axis_index("seq")
    heads_n = lax.axis_size("head")
    h = lax.axis_index("head")
    token_count, width_here = queries.shape
    nb = token_count // BLOCK
    gb = GLOBAL // BLOCK
    heads_here = width_here // HEAD_DIM
    slot_count = max(2, 4 * nb // n)
    depth = n // PAIR
    z, x = me // PAIR, me % PAIR

    def send(array, pairs, axis="seq"):
        return jax.tree.map(lambda part: lax.ppermute(part, axis, pairs), array)

    def swapped(array, m):
        return lax.ppermute(array, "head", [(i, i ^ m) for i in range(heads_n)])

    def folded(part, pairs, here):
        packed = jnp.concatenate([part[2], part[0][:, None], part[1][:, None]], axis=1)
        got = send(packed, pairs)
        both = merged(part, (got[:, GLOBAL], got[:, GLOBAL + 1], got[:, :GLOBAL]))
        return jax.tree.map(lambda a, b: jnp.where(here, a, b), both, part)

    def finished(part):
        out = jnp.transpose(part[2] / part[1][:, :, None], (1, 0, 2))
        return out.reshape(GLOBAL, -1).astype(jnp.bfloat16)

    chunks = math.gcd(CHUNKS, heads_here)
    cw = width_here // chunks
    cuts = [slice(c * cw, (c + 1) * cw) for c in range(chunks)]
    key_blocks = key_rows.reshape(nb, BLOCK, width_here)
    value_blocks = value_rows.reshape(nb, BLOCK, width_here)
    owned = [jnp.stack([key_blocks[..., sl], value_blocks[..., sl]], axis=1) for sl in cuts]
    up = [(i, i + 1) for i in range(n - 1)]
    down = [(i + 1, i) for i in range(n - 1)]
    mates = [(i, i + 1 if i % PAIR == 0 else i - 1) for i in range(n)]
    owner_flat = random_owner.reshape(-1)
    local_flat = random_local.reshape(-1)
    request_table, slot_ids = slot_table(owner_flat, local_flat, n, slot_count)
    line_wins = n % PAIR == 0 and nb <= PAIR * slot_count
    global_ids = jnp.arange(gb, dtype=jnp.int32)
    pools, tops, last = [], [], None

    if line_wins:
        mate_owner, mate_local = send((owner_flat, local_flat), mates)
        near_query = jnp.where(me == 1, send(queries[:GLOBAL], [(0, 1)]), queries[:GLOBAL])
        befores = [send(own[-1:], up) for own in owned]
        afters = [send(own[:1], down) for own in owned]
        mate_table, _ = slot_table(mate_owner, mate_local, n, slot_count)
        fetch = slot_count + gb
        mate_table = jnp.concatenate(
            [mate_table, jnp.broadcast_to(global_ids[None], (n, gb))], axis=1
        )
        offsets = [0]
        for s in range(1, depth):
            offsets += [-s, s]
        bufs = [{0: own} for own in owned]
        for s in range(1, depth):
            upward = [(i, i + PAIR) for i in range((s - 1) * PAIR, n - PAIR)]
            downward = [(i, i - PAIR) for i in range(PAIR, n - (s - 1) * PAIR)]
            for held in bufs:
                held[-s] = send(held[1 - s], upward)
                held[s] = send(held[s - 1], downward)
        for c in range(chunks):
            crossed = []
            for d in offsets:
                holder = jnp.clip((z + d) * PAIR + x, 0, n - 1)
                asked = jnp.take(bufs[c][d], mate_table[holder], axis=0)
                good = [(i, j) for i, j in mates if 0 <= i // PAIR + d < depth]
                crossed.append(send(asked, good))
            part = None
            for s in range(depth):
                held = bufs[c][s]
                term = partial_softmax(near_query[:, cuts[c]], held[:, 0], held[:, 1])
                part = term if part is None else merged(part, term)
            tops.append(finished(folded(part, [(1, 0)], me == 0)))
            pools.append(
                jnp.concatenate(
                    [bufs[c][d] for d in offsets] + crossed + [befores[c], afters[c]], axis=0
                )
            )
        last = bufs[0][depth - 1]
        place = jnp.where(owner_flat // PAIR < z, 2 * (z - owner_flat // PAIR) - 1,
                          2 * (owner_flat // PAIR - z))
        line_total = len(offsets) * nb
        cell = jnp.where(
            owner_flat % PAIR == x,
            place * nb + local_flat,
            line_total + place * fetch + slot_ids,
        )
        root = jnp.maximum(2 * z - 1, 0)
        global_cell = global_ids + jnp.where(
            x == 0, root * nb, line_total + root * fetch + slot_count
        )
        edge = line_total + len(offsets) * fetch
    else:
        rows = jnp.stack([queries[:GLOBAL], key_rows[:GLOBAL], value_rows[:GLOBAL]])
        rows = jnp.where(me == 1, send(rows, [(0, 1)]), rows)
        for s in range(1, depth):
            got = send(rows, [((s - 1) * PAIR + q, s * PAIR + q) for q in range(PAIR)])
            rows = jnp.where(z == s, got, rows)
        part = partial_softmax(rows[0], key_rows, value_rows)
        for s in range(depth - 1, 0, -1):
            pairs = [(s * PAIR + q, (s - 1) * PAIR + q) for q in range(PAIR)]
            part = folded(part, pairs, z == s - 1)
        top = finished(folded(part, [(1, 0)], me == 0))
        wanted = lax.all_to_all(request_table, "seq", split_axis=0, concat_axis=0, tiled=True)
        for c, own in enumerate(owned):
            tops.append(top[:, cuts[c]])
            sent = jnp.take(own, wanted.reshape(-1), axis=0)
            got = lax.all_to_all(sent, "seq", split_axis=0, concat_axis=0, tiled=True)
            shared = jnp.stack(
                [rows[i][:, cuts[c]].reshape(gb, BLOCK, cw) for i in (1, 2)], axis=1
            )
            edges = [send(own[-1:], up), send(own[:1], down)]
            pools.append(jnp.concatenate([own, got, shared] + edges, axis=0))
        cell = nb + owner_flat * slot_count + slot_ids
        global_cell = nb + n * slot_count + global_ids
        edge = nb + n * slot_count + gb

    weights, order, bit = [output_weight], [0], heads_n
    while bit > 1:
        bit //= 2
        for m in list(order):
            held = weights[order.index(m)]
            if m and last is not None:
                held = after(held, last)
            weights.append(swapped(held, bit))
            order.append(m ^ bit)

    steps = jnp.arange(nb, dtype=jnp.int32)
    cell = cell.reshape(nb, RANDOM)
    index = jnp.stack(
        [
            jnp.where(steps == 0, edge, steps - 1),
            steps,
            jnp.where(steps == nb - 1, edge + 1, steps + 1),
        ]
        + [cell[:, r] for r in range(RANDOM)]
        + [jnp.broadcast_to(global_cell[g], (nb,)) for g in range(gb)]
    ).astype(jnp.int32)
    numbers = me * nb + steps
    flags = jnp.stack([numbers == 0, numbers == n * nb - 1]).astype(jnp.int32)

    share = token_count // heads_n
    pieces = [[] for _ in order]
    for c, sl in enumerate(cuts):
        sparse = attend(queries[:, sl], pools[c], index, flags)
        top = jnp.where(me == 0, tops[c], sparse[:GLOBAL])
        sparse = jnp.concatenate([top, sparse[GLOBAL:]], axis=0)
        for k, m in enumerate(order):
            piece = lax.dynamic_slice_in_dim(sparse, (h ^ m) * share, share, 0)
            pieces[k].append(piece if m == 0 else swapped(piece, m))
    total = None
    for k in range(len(order)):
        term = jnp.dot(
            jnp.concatenate(pieces[k], axis=1), weights[k], preferred_element_type=jnp.float32
        )
        total = term if total is None else total + term
    return total.astype(jnp.bfloat16)


MESH = pl.DeviceIdType.MESH
RATE = HEAD_DIM ** (-0.5) * math.log2(math.e)
NT = (((1,), (1,)), ((), ()))


def attend_rows(query, keys, values, bias):
    scores = lax.dot_general(query, keys, NT, preferred_element_type=jnp.float32) + bias
    top = jnp.max(scores, axis=1, keepdims=True)
    weight = jnp.exp2((scores - top) * RATE)
    total = jnp.sum(weight, axis=1, keepdims=True)
    acc = jnp.dot(weight.astype(jnp.bfloat16), values, preferred_element_type=jnp.float32)
    return acc / total, top * RATE + jnp.log2(total)


def attend_all(query, k_ref, v_ref, step):
    rows = query.shape[0]
    cells = k_ref.shape[0]

    def body(c, carry):
        top, total, acc = carry
        keys = k_ref[pl.ds(c * step, step)].reshape(step * BLOCK, HEAD_DIM)
        values = v_ref[pl.ds(c * step, step)].reshape(step * BLOCK, HEAD_DIM)
        scores = lax.dot_general(query, keys, NT, preferred_element_type=jnp.float32)
        joint = jnp.maximum(top, jnp.max(scores, axis=1, keepdims=True))
        keep = jnp.exp2((top - joint) * RATE)
        weight = jnp.exp2((scores - joint) * RATE)
        total = total * keep + jnp.sum(weight, axis=1, keepdims=True)
        acc = acc * keep + jnp.dot(
            weight.astype(jnp.bfloat16), values, preferred_element_type=jnp.float32
        )
        return joint, total, acc

    start = (
        jnp.full((rows, 1), masked_score, jnp.float32),
        jnp.zeros((rows, 1), jnp.float32),
        jnp.zeros((rows, HEAD_DIM), jnp.float32),
    )
    top, total, acc = lax.fori_loop(0, cells // step, body, start)
    return acc / total, top * RATE + jnp.log2(total)


def joined(o1, l1, o2, l2):
    top = jnp.maximum(l1, l2)
    a, b = jnp.exp2(l1 - top), jnp.exp2(l2 - top)
    total = a + b
    return (o1 * a + o2 * b) / total, top + jnp.log2(total)


def hub_kernel(heads, nb, picks, cell_ref, bias_ref, q_hbm, k_hbm, v_hbm, w_hbm, out_ref, w_all, *rest):
    kcol, vcol = rest[:heads], rest[heads:2 * heads]
    (qown, qend, qmate, kwin, vwin, rsend, rrecv, ssend, srecv, esend, estat, loc, lstat,
     attn, attn_all, acc, wbuf, own_sem, col_sem, edge_s, edge_r, m1_s, m1_r, fw_s, fw_r,
     hb_s, hb_r, re_s, re_r, er_s, er_r, at_s, at_r, w_s, w_r, wl_sem, lc_sem) = rest[2 * heads:]
    me = lax.axis_index("seq")
    h = lax.axis_index("head")
    n = lax.axis_size("seq")
    heads_n = lax.axis_size("head")
    z, x = me // PAIR, me % PAIR
    hub = jnp.logical_or(z == 1, z == 2)
    end = jnp.logical_not(hub)
    own_end = jnp.where(z == 1, 0, 3)
    partner = jnp.where(hub, jnp.where(z == 1, 0, 3), jnp.where(z == 0, 1, 2)) * PAIR + x
    other = (3 - z) * PAIR + x
    mate = z * PAIR + (1 - x)
    wide = HEAD_DIM
    lanes = lambda i: slice(i * wide, (i + 1) * wide)
    finish = []

    def remote(src, dst, ss, rs, seq, head=None):
        return pltpu.make_async_remote_copy(
            src_ref=src, dst_ref=dst, send_sem=ss, recv_sem=rs,
            device_id=(seq, h if head is None else head), device_id_type=MESH,
        )

    def planes(p):
        return pl.ds(p * nb, nb)

    def m1(i):
        return [
            remote(k_hbm.at[:, :, lanes(i)], kcol[i].at[planes(z)], m1_s.at[i, 0], m1_r.at[i, 0], partner),
            remote(v_hbm.at[:, :, lanes(i)], vcol[i].at[planes(z)], m1_s.at[i, 1], m1_r.at[i, 1], partner),
            remote(q_hbm.at[:, :, lanes(i)], qend.at[i], m1_s.at[i, 2], m1_r.at[i, 2], partner),
        ]

    def forward(i):
        return [
            remote(kcol[i].at[planes(own_end)], kcol[i].at[planes(own_end)], fw_s.at[i, 0], fw_r.at[i, 0], other),
            remote(vcol[i].at[planes(own_end)], vcol[i].at[planes(own_end)], fw_s.at[i, 1], fw_r.at[i, 1], other),
            remote(qend.at[i], qmate.at[i, pl.ds(nb, nb)], fw_s.at[i, 2], fw_r.at[i, 2], mate),
        ]

    def first(i):
        return [
            remote(k_hbm.at[:, :, lanes(i)], kcol[i].at[planes(z)], hb_s.at[i, 0], hb_r.at[i, 0], other),
            remote(v_hbm.at[:, :, lanes(i)], vcol[i].at[planes(z)], hb_s.at[i, 1], hb_r.at[i, 1], other),
            remote(q_hbm.at[:, :, lanes(i)], qmate.at[i, pl.ds(0, nb)], hb_s.at[i, 2], hb_r.at[i, 2], mate),
        ]

    def results(i):
        return [
            remote(rsend.at[i], rrecv.at[i], re_s.at[i, 0], re_r.at[i, 0], mate),
            remote(ssend.at[i], srecv.at[i], re_s.at[i, 1], re_r.at[i, 1], mate),
        ]

    def ended(i):
        return [
            remote(esend.at[i], rrecv.at[i, pl.ds(0, nb)], er_s.at[i, 0], er_r.at[i, 0], partner),
            remote(estat.at[i], srecv.at[i], er_s.at[i, 1], er_r.at[i, 1], partner),
        ]

    def shares(i):
        return [
            remote(attn.at[i, h ^ k], attn_all.at[i, h], at_s.at[i, k - 1], at_r.at[i, k - 1], me, h ^ k)
            for k in range(1, heads_n)
        ]

    def weights(i):
        return [
            remote(w_hbm.at[i], w_all.at[h, i], w_s.at[i, 0], w_r.at[i, 0], me, h ^ 2),
            remote(w_hbm.at[i], w_all.at[h, i], w_s.at[i, 1], w_r.at[i, 1], me, h ^ 1),
            remote(w_all.at[h ^ 2, i], w_all.at[h ^ 2, i], w_s.at[i, 2], w_r.at[i, 2], me, h ^ 1),
        ]

    def own_copies():
        return [
            pltpu.make_async_copy(q_hbm, qown, own_sem.at[0]),
            pltpu.make_async_copy(k_hbm, kwin.at[pl.ds(1, nb)], own_sem.at[1]),
            pltpu.make_async_copy(v_hbm, vwin.at[pl.ds(1, nb)], own_sem.at[2]),
        ]

    def column(i):
        return [
            pltpu.make_async_copy(k_hbm.at[:, :, lanes(i)], kcol[i].at[planes(z)], col_sem.at[i, 0]),
            pltpu.make_async_copy(v_hbm.at[:, :, lanes(i)], vcol[i].at[planes(z)], col_sem.at[i, 1]),
        ]

    def edges():
        return [
            remote(k_hbm.at[nb - 1], kwin.at[0], edge_s.at[0], edge_r.at[0], me + 1),
            remote(v_hbm.at[nb - 1], vwin.at[0], edge_s.at[1], edge_r.at[1], me + 1),
        ], [
            remote(k_hbm.at[0], kwin.at[nb + 1], edge_s.at[2], edge_r.at[2], me - 1),
            remote(v_hbm.at[0], vwin.at[nb + 1], edge_s.at[3], edge_r.at[3], me - 1),
        ]

    def start(copies):
        for copy in copies:
            copy.start()

    def landed(copies):
        for copy in copies:
            copy.wait_recv()

    def sent(copies):
        for copy in copies:
            copy.wait_send()

    def pump(i):
        coming = m1(i)
        landed(coming[:2])
        start(forward(i)[:2])
        coming[2].wait_recv()
        start(forward(i)[2:])
        if i + 1 < heads:
            start(first(i + 1))

    up, down = edges()
    for copy in own_copies():
        copy.start()

    @pl.when(me < n - 1)
    def _():
        start(up)

    @pl.when(me > 0)
    def _():
        start(down)

    @pl.when(me == 0)
    def _():
        kwin[0] = jnp.zeros(kwin.shape[1:], kwin.dtype)
        vwin[0] = jnp.zeros(vwin.shape[1:], vwin.dtype)

    @pl.when(me == n - 1)
    def _():
        kwin[nb + 1] = jnp.zeros(kwin.shape[1:], kwin.dtype)
        vwin[nb + 1] = jnp.zeros(vwin.shape[1:], vwin.dtype)

    @pl.when(end)
    def _():
        for i in range(heads):
            start(m1(i))

    @pl.when(hub)
    def _():
        start(first(0))
        for i in range(heads):
            start(column(i))

    for i in range(2):
        weights(i)[0].start()
    for i in range(heads):
        weights(i)[1].start()

    for copy in own_copies():
        copy.wait()

    @pl.when(me > 0)
    def _():
        landed(up)

    @pl.when(me < n - 1)
    def _():
        landed(down)

    row = lax.broadcasted_iota(jnp.int32, (1, 3 * BLOCK), 1) // BLOCK
    lane = lax.broadcasted_iota(jnp.int32, (BLOCK, 128), 1)
    pick_row = lax.broadcasted_iota(jnp.int32, (1, picks * BLOCK), 1) // BLOCK

    def stat(i, value, table):
        return jnp.where(lane == i, value, table)

    def read_stat(i, table):
        return jnp.sum(jnp.where(lane == i, table, 0.0), axis=1, keepdims=True)

    def window_bias(b):
        gone = jnp.logical_or(
            jnp.logical_and(row == 0, jnp.logical_and(me == 0, b == 0)),
            jnp.logical_and(row == 2, jnp.logical_and(me == n - 1, b == nb - 1)),
        )
        return jnp.where(gone, masked_score, 0.0).astype(jnp.float32)

    def listed(i, number):
        cells = [cell_ref[number * picks + r] for r in range(picks)]
        keys = [kcol[i][cell] for cell in cells]
        values = [vcol[i][cell] for cell in cells]
        bias = jnp.full((1, picks * BLOCK), bias_ref[number * picks], jnp.float32)
        for r in range(1, picks):
            bias = jnp.where(pick_row == r, bias_ref[number * picks + r], bias)
        return keys, values, bias

    def window(i, b):
        keys = [kwin[b + s, :, lanes(i)] for s in range(3)]
        values = [vwin[b + s, :, lanes(i)] for s in range(3)]
        return keys, values, window_bias(b)

    def attend_lists(query, lists):
        keys = jnp.concatenate([k for part in lists for k in part[0]], axis=0)
        values = jnp.concatenate([v for part in lists for v in part[1]], axis=0)
        bias = jnp.concatenate([part[2] for part in lists], axis=1) if len(lists) > 1 else lists[0][2]
        return attend_rows(query, keys, values, bias)

    def looped(count, unroll, body, table):
        def step(j, table):
            for u in range(unroll):
                table = body(j * unroll + u, table)
            return table

        return lax.fori_loop(0, count // unroll, step, table)

    def global_rows(i, query_of, store, table, base):
        query = jnp.concatenate([query_of(0), query_of(1)], axis=0)
        out, lse = attend_all(query, kcol[i], vcol[i], 8)
        for g in range(GLOBAL // BLOCK):
            part = slice(g * BLOCK, (g + 1) * BLOCK)
            store(g, out[part])
            table[...] = stat(base + g, lse[part], table[...])

    blank = jnp.zeros((BLOCK, 128), jnp.float32)

    def compute_hub(i):
        landed(forward(i))
        landed(first(i))
        for copy in column(i):
            copy.wait()

        def for_mate(b, table):
            out, lse = attend_lists(qmate[i, b], [listed(i, 2 * nb + b)])
            rsend[i, b] = out.astype(jnp.bfloat16)
            return stat(b, lse, table)

        ssend[i] = looped(2 * nb, UNROLL, for_mate, blank)

        @pl.when(jnp.logical_and(z == 1, x == 1))
        def _():
            def store(g, value):
                rsend[i, nb + g] = value.astype(jnp.bfloat16)

            global_rows(i, lambda g: qmate[i, nb + g], store, ssend.at[i], nb)

        start(results(i))

        def for_own(b, table):
            query = qown[b, :, lanes(i)]
            out, lse = attend_lists(query, [window(i, b), listed(i, b)])
            loc[i % 2, b] = out
            return stat(b, lse, table)

        def for_end(b, table):
            out, lse = attend_lists(qend[i, b], [listed(i, nb + b)])
            loc[i % 2, nb + b] = out
            return stat(nb + b, lse, table)

        table = looped(nb, UNROLL, for_own, blank)
        lstat[i % 2] = looped(nb, UNROLL, for_end, table)

        @pl.when(jnp.logical_and(z == 1, x == 0))
        def _():
            def store(g, value):
                loc[i % 2, nb + g] = value

            global_rows(i, lambda g: qend[i, g], store, lstat.at[i % 2], nb)

    def compute_end(i):
        def for_own(b, table):
            query = qown[b, :, lanes(i)]
            out, lse = attend_lists(query, [window(i, b)])
            loc[i % 2, b] = out
            replaced = jnp.logical_and(me == 0, b < GLOBAL // BLOCK)
            return stat(b, jnp.where(replaced, masked_score, lse), table)

        lstat[i % 2] = looped(nb, UNROLL, for_own, blank)

    def put_attn(i, b, value):
        per = nb // heads_n
        attn[i, b // per, pl.ds(pl.multiple_of((b % per) * BLOCK, BLOCK), BLOCK)] = value.astype(jnp.bfloat16)

    def merge_pair(i, b):
        return joined(
            loc[i % 2, b], read_stat(b, lstat[i % 2]),
            rrecv[i, b].astype(jnp.float32), read_stat(b, srecv[i]),
        )

    def merge_own(i):
        def body(b, _):
            out, _lse = merge_pair(i, b)
            put_attn(i, b, out)
            return _

        looped(nb, UNROLL, body, 0)

    def merge_hub(i):
        landed(results(i))

        def body(b, table):
            out, lse = merge_pair(i, nb + b)
            esend[i, b] = out.astype(jnp.bfloat16)
            return stat(b, lse, table)

        estat[i] = looped(nb, UNROLL, body, blank)
        start(ended(i))
        merge_own(i)

    def merge_end(i):
        landed(ended(i))
        merge_own(i)

    def share(i):
        start(shares(i))
        pltpu.make_async_copy(attn.at[i, h], attn_all.at[i, h], lc_sem.at[i]).start()

    def load_weights(i):
        copies = []
        for k in range(heads_n):
            source = (w_hbm.at[i] if k == 0 else w_all.at[h ^ k, i])
            target = wbuf.at[i % 2, pl.ds((h ^ k) * wide, wide)]
            copies.append(pltpu.make_async_copy(source, target, wl_sem.at[i % 2, k]))
        return copies

    def project(i):
        landed(weights(i)[1:])
        for copy in load_weights(i):
            copy.start()
        landed(shares(i))
        pltpu.make_async_copy(attn.at[i, h], attn_all.at[i, h], lc_sem.at[i]).wait()
        for copy in load_weights(i):
            copy.wait()
        left = jnp.concatenate([attn_all[i, g] for g in range(heads_n)], axis=1)
        tile = 512

        def body(c, _):
            here = pl.ds(pl.multiple_of(c * tile, tile), tile)
            term = jnp.dot(left, wbuf[i % 2, :, here], preferred_element_type=jnp.float32)
            if i > 0:
                term = term + acc[:, here]
            if i < heads - 1:
                acc[:, here] = term
            else:
                out_ref[:, here] = term.astype(jnp.bfloat16)
            return _

        lax.fori_loop(0, acc.shape[1] // tile, body, 0)

    @pl.when(hub)
    def _():
        pump(0)
        pump(1)

    for t in range(heads + 2):
        if t < heads:
            @pl.when(hub)
            def _():
                compute_hub(t)
                if t + 2 < heads:
                    pump(t + 2)

            @pl.when(end)
            def _():
                compute_end(t)

            if t + 2 < heads:
                weights(t + 2)[0].start()
        if 1 <= t <= heads:
            @pl.when(hub)
            def _():
                merge_hub(t - 1)

            @pl.when(end)
            def _():
                merge_end(t - 1)

            share(t - 1)
        if t < heads:
            weights(t)[0].wait_recv()
            weights(t)[2].start()
        if t >= 2:
            project(t - 2)

    @pl.when(me < n - 1)
    def _():
        sent(up)

    @pl.when(me > 0)
    def _():
        sent(down)

    for i in range(heads):
        @pl.when(end)
        def _():
            sent(m1(i))

        @pl.when(hub)
        def _():
            sent(forward(i))
            sent(first(i))
            sent(results(i))
            sent(ended(i))

        sent(shares(i))
        sent(weights(i))


UNROLL = 2


def hub_attention(cells, bias, q, k, v, w, picks):
    nb, _, width = q.shape
    heads, wide, columns = w.shape
    heads_n = lax.axis_size("head")
    planes = lax.axis_size("seq") // PAIR
    rows = nb * BLOCK
    share = rows // heads_n
    bf, f32 = jnp.bfloat16, jnp.float32
    dma = pltpu.SemaphoreType.DMA
    col = [pltpu.VMEM((planes * nb, BLOCK, wide), bf)] * (2 * heads)
    scratch = col + [
        pltpu.VMEM((nb, BLOCK, width), bf),
        pltpu.VMEM((heads, nb, BLOCK, wide), bf),
        pltpu.VMEM((heads, 2 * nb, BLOCK, wide), bf),
        pltpu.VMEM((nb + 2, BLOCK, width), bf),
        pltpu.VMEM((nb + 2, BLOCK, width), bf),
        pltpu.VMEM((heads, 2 * nb, BLOCK, wide), bf),
        pltpu.VMEM((heads, 2 * nb, BLOCK, wide), bf),
        pltpu.VMEM((heads, BLOCK, 128), f32),
        pltpu.VMEM((heads, BLOCK, 128), f32),
        pltpu.VMEM((heads, nb, BLOCK, wide), bf),
        pltpu.VMEM((heads, BLOCK, 128), f32),
        pltpu.VMEM((2, 2 * nb, BLOCK, wide), f32),
        pltpu.VMEM((2, BLOCK, 128), f32),
        pltpu.VMEM((heads, heads_n, share, wide), bf),
        pltpu.VMEM((heads, heads_n, share, wide), bf),
        pltpu.VMEM((share, columns), f32),
        pltpu.VMEM((2, heads_n * wide, columns), bf),
        dma((3,)), dma((heads, 2)), dma((4,)), dma((4,)),
        dma((heads, 3)), dma((heads, 3)), dma((heads, 3)), dma((heads, 3)),
        dma((heads, 3)), dma((heads, 3)), dma((heads, 2)), dma((heads, 2)),
        dma((heads, 2)), dma((heads, 2)), dma((heads, 3)), dma((heads, 3)),
        dma((heads, 3)), dma((heads, 3)), dma((2, heads_n)), dma((heads,)),
    ]
    anywhere = pl.BlockSpec(memory_space=pl.ANY)
    smem = pl.BlockSpec(memory_space=pltpu.SMEM)
    out, _ = pl.pallas_call(
        functools.partial(hub_kernel, heads, nb, picks),
        out_shape=(
            jax.ShapeDtypeStruct((share, columns), bf),
            jax.ShapeDtypeStruct((heads_n,) + w.shape, bf),
        ),
        in_specs=[smem, smem] + [anywhere] * 4,
        out_specs=(pl.BlockSpec(memory_space=pltpu.VMEM), anywhere),
        scratch_shapes=scratch,
        compiler_params=pltpu.CompilerParams(
            has_side_effects=True, vmem_limit_bytes=67043328
        ),
    )(cells, bias, q, k, v, w)
    return out


def local_hub(queries, key_rows, value_rows, random_owner, random_local, output_weight):
    me = lax.axis_index("seq")
    z, x = me // PAIR, me % PAIR
    rows, width = queries.shape
    nb = rows // BLOCK
    gb = GLOBAL // BLOCK
    heads = width // HEAD_DIM
    both = jnp.stack([random_owner, random_local])
    every = lax.all_gather(both, "seq", axis=0, tiled=False)
    ze = jnp.where(z == 1, 0, 3)
    ids = jnp.stack([me, ze * PAIR + x, z * PAIR + 1 - x, ze * PAIR + 1 - x])
    mine = jnp.take(every, ids, axis=0)
    owner, local = mine[:, 0], mine[:, 1]
    here = owner % PAIR == x
    cell = jnp.where(here, owner // PAIR * nb + local, 0)
    bias = jnp.where(here, 0.0, masked_score).astype(jnp.float32)
    shape = cell.shape[:2] + (gb,)
    cell = jnp.concatenate(
        [cell, jnp.broadcast_to(jnp.arange(gb, dtype=jnp.int32), shape)], axis=2
    )
    bias = jnp.concatenate(
        [bias, jnp.full(shape, jnp.where(x == 0, 0.0, masked_score), jnp.float32)], axis=2
    )
    blocks = lambda a: a.reshape(nb, BLOCK, width)
    return hub_attention(
        cell.reshape(-1), bias.reshape(-1), blocks(queries), blocks(key_rows), blocks(value_rows),
        output_weight.reshape(heads, HEAD_DIM, -1), RANDOM + gb,
    )


def local(queries, *others):
    n, heads_n = lax.axis_size("seq"), lax.axis_size("head")
    if n == 4 * PAIR and heads_n == 4:
        return local_hub(queries, *others)
    return local_plain(queries, *others)


def solution(mesh):
    in_specs = (
        P("seq", "head"),
        P("seq", "head"),
        P("seq", "head"),
        P("seq", None),
        P("seq", None),
        P("head", None),
    )
    out_specs = P(("seq", "head"), None)
    return jax.shard_map(local, mesh=mesh, in_specs=in_specs, out_specs=out_specs, check_vma=False)
```

```python
import functools
import math

import jax
import jax.numpy as jnp
from jax import lax
from jax.experimental import pallas as pl
from jax.experimental.pallas import tpu as pltpu
from jax.sharding import PartitionSpec as P

HEAD_DIM = 128
BLOCK = 64
RANDOM = 3
GLOBAL = 128
CHUNKS = 2
PAIR = 2


masked_score = -1e30


def slot_table(owner_ids, local_ids, seq_count, slot_count):
    owner_hits = (owner_ids[:, None] == jnp.arange(seq_count, dtype=jnp.int32)[None, :]).astype(
        jnp.int32
    )
    earlier = jnp.cumsum(owner_hits, axis=0) - owner_hits
    slot_ids = jnp.sum(earlier * owner_hits, axis=1)
    slot_hits = (slot_ids[:, None] == jnp.arange(slot_count, dtype=jnp.int32)[None, :]).astype(
        jnp.int32
    )
    request_table = jnp.sum(
        (owner_hits * local_ids[:, None])[:, :, None] * slot_hits[:, None, :], axis=0
    )
    return (request_table, slot_ids)


def attend_kernel(heads, index_ref, flag_ref, q_ref, *refs):
    near, out_ref = refs[:-1], refs[-1]
    step = pl.program_id(0)
    rate = HEAD_DIM ** (-0.5) * math.log2(math.e)
    first, last = flag_ref[0, step], flag_ref[1, step]
    listed = len(near) * BLOCK
    column = lax.broadcasted_iota(jnp.int32, (1, listed), 1) // BLOCK
    hidden = jnp.logical_or(
        jnp.logical_and(column == 0, first == 1), jnp.logical_and(column == 2, last == 1)
    )
    bias = jnp.where(hidden, masked_score, 0.0).astype(jnp.float32)
    for head in range(heads):
        here = pl.ds(head * HEAD_DIM, HEAD_DIM)
        keys = jnp.concatenate([ref[0, 0, :, here] for ref in near], axis=0)
        values = jnp.concatenate([ref[0, 1, :, here] for ref in near], axis=0)
        scores = lax.dot_general(
            q_ref[:, here], keys, (((1,), (1,)), ((), ())), preferred_element_type=jnp.float32
        )
        scores = scores + bias
        top = jnp.max(scores, axis=1, keepdims=True)
        weight = jnp.exp2((scores - top) * rate)
        total = jnp.sum(weight, axis=1, keepdims=True)
        context = jnp.dot(
            weight.astype(jnp.bfloat16), values, preferred_element_type=jnp.float32
        )
        out_ref[:, here] = (context / total).astype(out_ref.dtype)


def attend(queries, pool, index, flags):
    tokens, width = queries.shape
    blocks = tokens // BLOCK
    heads = width // HEAD_DIM
    listed = index.shape[0]

    def picked(r):
        return pl.BlockSpec(
            (1, 2, BLOCK, width), lambda i, index_ref, flag_ref: (index_ref[r, i], 0, 0, 0)
        )

    return pl.pallas_call(
        functools.partial(attend_kernel, heads),
        grid_spec=pltpu.PrefetchScalarGridSpec(
            num_scalar_prefetch=2,
            grid=(blocks,),
            in_specs=[pl.BlockSpec((BLOCK, width), lambda i, a, b: (i, 0))]
            + [picked(r) for r in range(listed)],
            out_specs=pl.BlockSpec((BLOCK, width), lambda i, a, b: (i, 0)),
        ),
        out_shape=jax.ShapeDtypeStruct(queries.shape, jnp.bfloat16),
        compiler_params=pltpu.CompilerParams(dimension_semantics=("arbitrary",)),
        cost_estimate=pl.CostEstimate(
            flops=60 * tokens * width * 8 * BLOCK,
            bytes_accessed=blocks * 14 * BLOCK * width * 2,
            transcendentals=tokens * heads * 8 * BLOCK,
        ),
    )(index, flags, queries, *([pool] * listed))


def merged(left, right):
    joint = jnp.maximum(left[0], right[0])
    a, b = jnp.exp(left[0] - joint), jnp.exp(right[0] - joint)
    return (
        joint,
        left[1] * a + right[1] * b,
        left[2] * a[:, :, None] + right[2] * b[:, :, None],
    )


def partial_softmax(query, keys, values):
    tokens, width = query.shape
    heads = width // HEAD_DIM
    query = query.reshape(tokens, heads, HEAD_DIM)
    keys, values = (a.reshape(-1, heads, HEAD_DIM) for a in (keys, values))
    scores = jnp.einsum("qhd,khd->hqk", query, keys, preferred_element_type=jnp.float32)
    scores = scores * HEAD_DIM ** (-0.5)
    row_max = jnp.max(scores, axis=2)
    weight = jnp.exp(scores - row_max[:, :, None])
    row_total = jnp.sum(weight, axis=2)
    value = jnp.einsum(
        "hqk,khd->hqd", weight.astype(jnp.bfloat16), values, preferred_element_type=jnp.float32
    )
    return row_max, row_total, value


def after(array, *others):
    return lax.optimization_barrier((array,) + others)[0]


def local_plain(queries, key_rows, value_rows, random_owner, random_local, output_weight):
    n = lax.axis_size("seq")
    me = lax.axis_index("seq")
    heads_n = lax.axis_size("head")
    h = lax.axis_index("head")
    token_count, width_here = queries.shape
    nb = token_count // BLOCK
    gb = GLOBAL // BLOCK
    heads_here = width_here // HEAD_DIM
    slot_count = max(2, 4 * nb // n)
    depth = n // PAIR
    z, x = me // PAIR, me % PAIR

    def send(array, pairs, axis="seq"):
        return jax.tree.map(lambda part: lax.ppermute(part, axis, pairs), array)

    def swapped(array, m):
        return lax.ppermute(array, "head", [(i, i ^ m) for i in range(heads_n)])

    def folded(part, pairs, here):
        packed = jnp.concatenate([part[2], part[0][:, None], part[1][:, None]], axis=1)
        got = send(packed, pairs)
        both = merged(part, (got[:, GLOBAL], got[:, GLOBAL + 1], got[:, :GLOBAL]))
        return jax.tree.map(lambda a, b: jnp.where(here, a, b), both, part)

    def finished(part):
        out = jnp.transpose(part[2] / part[1][:, :, None], (1, 0, 2))
        return out.reshape(GLOBAL, -1).astype(jnp.bfloat16)

    chunks = math.gcd(CHUNKS, heads_here)
    cw = width_here // chunks
    cuts = [slice(c * cw, (c + 1) * cw) for c in range(chunks)]
    key_blocks = key_rows.reshape(nb, BLOCK, width_here)
    value_blocks = value_rows.reshape(nb, BLOCK, width_here)
    owned = [jnp.stack([key_blocks[..., sl], value_blocks[..., sl]], axis=1) for sl in cuts]
    up = [(i, i + 1) for i in range(n - 1)]
    down = [(i + 1, i) for i in range(n - 1)]
    mates = [(i, i + 1 if i % PAIR == 0 else i - 1) for i in range(n)]
    owner_flat = random_owner.reshape(-1)
    local_flat = random_local.reshape(-1)
    request_table, slot_ids = slot_table(owner_flat, local_flat, n, slot_count)
    line_wins = n % PAIR == 0 and nb <= PAIR * slot_count
    global_ids = jnp.arange(gb, dtype=jnp.int32)
    pools, tops, last = [], [], None

    if line_wins:
        mate_owner, mate_local = send((owner_flat, local_flat), mates)
        near_query = jnp.where(me == 1, send(queries[:GLOBAL], [(0, 1)]), queries[:GLOBAL])
        befores = [send(own[-1:], up) for own in owned]
        afters = [send(own[:1], down) for own in owned]
        mate_table, _ = slot_table(mate_owner, mate_local, n, slot_count)
        fetch = slot_count + gb
        mate_table = jnp.concatenate(
            [mate_table, jnp.broadcast_to(global_ids[None], (n, gb))], axis=1
        )
        offsets = [0]
        for s in range(1, depth):
            offsets += [-s, s]
        bufs = [{0: own} for own in owned]
        for s in range(1, depth):
            upward = [(i, i + PAIR) for i in range((s - 1) * PAIR, n - PAIR)]
            downward = [(i, i - PAIR) for i in range(PAIR, n - (s - 1) * PAIR)]
            for held in bufs:
                held[-s] = send(held[1 - s], upward)
                held[s] = send(held[s - 1], downward)
        for c in range(chunks):
            crossed = []
            for d in offsets:
                holder = jnp.clip((z + d) * PAIR + x, 0, n - 1)
                asked = jnp.take(bufs[c][d], mate_table[holder], axis=0)
                good = [(i, j) for i, j in mates if 0 <= i // PAIR + d < depth]
                crossed.append(send(asked, good))
            part = None
            for s in range(depth):
                held = bufs[c][s]
                term = partial_softmax(near_query[:, cuts[c]], held[:, 0], held[:, 1])
                part = term if part is None else merged(part, term)
            tops.append(finished(folded(part, [(1, 0)], me == 0)))
            pools.append(
                jnp.concatenate(
                    [bufs[c][d] for d in offsets] + crossed + [befores[c], afters[c]], axis=0
                )
            )
        last = bufs[0][depth - 1]
        place = jnp.where(owner_flat // PAIR < z, 2 * (z - owner_flat // PAIR) - 1,
                          2 * (owner_flat // PAIR - z))
        line_total = len(offsets) * nb
        cell = jnp.where(
            owner_flat % PAIR == x,
            place * nb + local_flat,
            line_total + place * fetch + slot_ids,
        )
        root = jnp.maximum(2 * z - 1, 0)
        global_cell = global_ids + jnp.where(
            x == 0, root * nb, line_total + root * fetch + slot_count
        )
        edge = line_total + len(offsets) * fetch
    else:
        rows = jnp.stack([queries[:GLOBAL], key_rows[:GLOBAL], value_rows[:GLOBAL]])
        rows = jnp.where(me == 1, send(rows, [(0, 1)]), rows)
        for s in range(1, depth):
            got = send(rows, [((s - 1) * PAIR + q, s * PAIR + q) for q in range(PAIR)])
            rows = jnp.where(z == s, got, rows)
        part = partial_softmax(rows[0], key_rows, value_rows)
        for s in range(depth - 1, 0, -1):
            pairs = [(s * PAIR + q, (s - 1) * PAIR + q) for q in range(PAIR)]
            part = folded(part, pairs, z == s - 1)
        top = finished(folded(part, [(1, 0)], me == 0))
        wanted = lax.all_to_all(request_table, "seq", split_axis=0, concat_axis=0, tiled=True)
        for c, own in enumerate(owned):
            tops.append(top[:, cuts[c]])
            sent = jnp.take(own, wanted.reshape(-1), axis=0)
            got = lax.all_to_all(sent, "seq", split_axis=0, concat_axis=0, tiled=True)
            shared = jnp.stack(
                [rows[i][:, cuts[c]].reshape(gb, BLOCK, cw) for i in (1, 2)], axis=1
            )
            edges = [send(own[-1:], up), send(own[:1], down)]
            pools.append(jnp.concatenate([own, got, shared] + edges, axis=0))
        cell = nb + owner_flat * slot_count + slot_ids
        global_cell = nb + n * slot_count + global_ids
        edge = nb + n * slot_count + gb

    weights, order, bit = [output_weight], [0], heads_n
    while bit > 1:
        bit //= 2
        for m in list(order):
            held = weights[order.index(m)]
            if m and last is not None:
                held = after(held, last)
            weights.append(swapped(held, bit))
            order.append(m ^ bit)

    steps = jnp.arange(nb, dtype=jnp.int32)
    cell = cell.reshape(nb, RANDOM)
    index = jnp.stack(
        [
            jnp.where(steps == 0, edge, steps - 1),
            steps,
            jnp.where(steps == nb - 1, edge + 1, steps + 1),
        ]
        + [cell[:, r] for r in range(RANDOM)]
        + [jnp.broadcast_to(global_cell[g], (nb,)) for g in range(gb)]
    ).astype(jnp.int32)
    numbers = me * nb + steps
    flags = jnp.stack([numbers == 0, numbers == n * nb - 1]).astype(jnp.int32)

    share = token_count // heads_n
    pieces = [[] for _ in order]
    for c, sl in enumerate(cuts):
        sparse = attend(queries[:, sl], pools[c], index, flags)
        top = jnp.where(me == 0, tops[c], sparse[:GLOBAL])
        sparse = jnp.concatenate([top, sparse[GLOBAL:]], axis=0)
        for k, m in enumerate(order):
            piece = lax.dynamic_slice_in_dim(sparse, (h ^ m) * share, share, 0)
            pieces[k].append(piece if m == 0 else swapped(piece, m))
    total = None
    for k in range(len(order)):
        term = jnp.dot(
            jnp.concatenate(pieces[k], axis=1), weights[k], preferred_element_type=jnp.float32
        )
        total = term if total is None else total + term
    return total.astype(jnp.bfloat16)


MESH = pl.DeviceIdType.MESH
RATE = HEAD_DIM ** (-0.5) * math.log2(math.e)
NT = (((1,), (1,)), ((), ()))


def attend_group(items):
    scores = [
        lax.dot_general(query, keys, NT, preferred_element_type=jnp.float32)
        for query, keys, _, _ in items
    ]
    scores = [a if item[3] is None else a + item[3] for a, item in zip(scores, items)]
    tops = [jnp.max(a, axis=1, keepdims=True) for a in scores]
    parts = [jnp.exp2((a - top) * RATE) for a, top in zip(scores, tops)]
    totals = [jnp.sum(a, axis=1, keepdims=True) for a in parts]
    accs = [
        jnp.dot(a.astype(jnp.bfloat16), item[2], preferred_element_type=jnp.float32)
        for a, item in zip(parts, items)
    ]
    return [
        (acc * (1.0 / total), top * RATE + jnp.log2(total))
        for acc, total, top in zip(accs, totals, tops)
    ]


def attend_all(query, k_ref, v_ref, step):
    rows = query.shape[0]
    cells = k_ref.shape[0]

    def chunk(c):
        keys = k_ref[pl.ds(c * step, step)].reshape(step * BLOCK, HEAD_DIM)
        values = v_ref[pl.ds(c * step, step)].reshape(step * BLOCK, HEAD_DIM)
        return query, keys, values, None

    def body(c, carry):
        for part in attend_group([chunk(2 * c), chunk(2 * c + 1)]):
            carry = joined(*carry, *part)
        return carry

    start = (
        jnp.zeros((rows, HEAD_DIM), jnp.float32),
        jnp.full((rows, 1), masked_score, jnp.float32),
    )
    return lax.fori_loop(0, cells // (2 * step), body, start)


def joined(o1, l1, o2, l2):
    top = jnp.maximum(l1, l2)
    a, b = jnp.exp2(l1 - top), jnp.exp2(l2 - top)
    total = a + b
    return (o1 * a + o2 * b) / total, top + jnp.log2(total)


def hub_kernel(heads, nb, picks, codes, q_hbm, k_hbm, v_hbm, w_hbm, out_ref, w_all, *rest):
    kcol, vcol = rest[:heads], rest[heads:2 * heads]
    (qown, qend, qmate, kwin, vwin, rsend, rrecv, ssend, srecv, esend, estat, loc, lstat, lend, tmp,
     attn, attn_all, acc, wbuf, own_sem, col_sem, edge_s, edge_r, m1_s, m1_r, fw_s, fw_r,
     hb_s, hb_r, re_s, re_r, er_s, er_r, at_s, at_r, w_s, w_r, wl_sem, lc_sem,
     landed_codes, codes_s, cell_ref, bias_ref, cd_s, cd_r, cd_sem) = rest[2 * heads:]
    me = lax.axis_index("seq")
    h = lax.axis_index("head")
    n = lax.axis_size("seq")
    heads_n = lax.axis_size("head")
    z, x = me // PAIR, me % PAIR
    hub = jnp.logical_or(z == 1, z == 2)
    end = jnp.logical_not(hub)
    own_end = jnp.where(z == 1, 0, 3)
    partner = jnp.where(hub, jnp.where(z == 1, 0, 3), jnp.where(z == 0, 1, 2)) * PAIR + x
    other = (3 - z) * PAIR + x
    mate = z * PAIR + (1 - x)
    wide = HEAD_DIM
    lanes = lambda i: slice(i * wide, (i + 1) * wide)
    finish = []

    def remote(src, dst, ss, rs, seq, head=None):
        return pltpu.make_async_remote_copy(
            src_ref=src, dst_ref=dst, send_sem=ss, recv_sem=rs,
            device_id=(seq, h if head is None else head), device_id_type=MESH,
        )

    def planes(p):
        return pl.ds(p * nb, nb)

    def m1(i):
        return [
            remote(k_hbm.at[:, :, lanes(i)], kcol[i].at[planes(z)], m1_s.at[i, 0], m1_r.at[i, 0], partner),
            remote(v_hbm.at[:, :, lanes(i)], vcol[i].at[planes(z)], m1_s.at[i, 1], m1_r.at[i, 1], partner),
            remote(q_hbm.at[:, :, lanes(i)], qend.at[i], m1_s.at[i, 2], m1_r.at[i, 2], partner),
        ]

    def forward(i):
        return [
            remote(kcol[i].at[planes(own_end)], kcol[i].at[planes(own_end)], fw_s.at[i, 0], fw_r.at[i, 0], other),
            remote(vcol[i].at[planes(own_end)], vcol[i].at[planes(own_end)], fw_s.at[i, 1], fw_r.at[i, 1], other),
            remote(qend.at[i], qmate.at[i, pl.ds(nb, nb)], fw_s.at[i, 2], fw_r.at[i, 2], mate),
        ]

    def first(i):
        return [
            remote(k_hbm.at[:, :, lanes(i)], kcol[i].at[planes(z)], hb_s.at[i, 0], hb_r.at[i, 0], other),
            remote(v_hbm.at[:, :, lanes(i)], vcol[i].at[planes(z)], hb_s.at[i, 1], hb_r.at[i, 1], other),
            remote(q_hbm.at[:, :, lanes(i)], qmate.at[i, pl.ds(0, nb)], hb_s.at[i, 2], hb_r.at[i, 2], mate),
        ]

    def results(i, j):
        return [
            remote(part.at[i, j], into.at[i, j], re_s.at[i, j, k], re_r.at[i, j, k], mate)
            for k, (part, into) in enumerate(((rsend, rrecv), (ssend, srecv)))
        ]

    def ended(i):
        return [
            remote(esend.at[i], rrecv.at[i, 0], er_s.at[i, 0], er_r.at[i, 0], partner),
            remote(estat.at[i], srecv.at[i, 0], er_s.at[i, 1], er_r.at[i, 1], partner),
        ]

    def shares(i):
        return [
            remote(attn.at[i, h ^ k], attn_all.at[i, h], at_s.at[i, k - 1], at_r.at[i, k - 1], me, h ^ k)
            for k in range(1, heads_n)
        ]

    def weights(i):
        return [
            remote(w_hbm.at[i], w_all.at[h, i], w_s.at[i, 0], w_r.at[i, 0], me, h ^ 2),
            remote(w_hbm.at[i], w_all.at[h, i], w_s.at[i, 1], w_r.at[i, 1], me, h ^ 1),
            remote(w_all.at[h ^ 2, i], w_all.at[h ^ 2, i], w_s.at[i, 2], w_r.at[i, 2], me, h ^ 1),
        ]

    def own_copies():
        return [
            pltpu.make_async_copy(q_hbm, qown, own_sem.at[0]),
            pltpu.make_async_copy(k_hbm, kwin.at[pl.ds(1, nb)], own_sem.at[1]),
            pltpu.make_async_copy(v_hbm, vwin.at[pl.ds(1, nb)], own_sem.at[2]),
        ]

    def column(i):
        return [
            pltpu.make_async_copy(k_hbm.at[:, :, lanes(i)], kcol[i].at[planes(z)], col_sem.at[i, 0]),
            pltpu.make_async_copy(v_hbm.at[:, :, lanes(i)], vcol[i].at[planes(z)], col_sem.at[i, 1]),
        ]

    def edges():
        return [
            remote(k_hbm.at[nb - 1], kwin.at[0], edge_s.at[0], edge_r.at[0], me + 1),
            remote(v_hbm.at[nb - 1], vwin.at[0], edge_s.at[1], edge_r.at[1], me + 1),
        ], [
            remote(k_hbm.at[0], kwin.at[nb + 1], edge_s.at[2], edge_r.at[2], me - 1),
            remote(v_hbm.at[0], vwin.at[nb + 1], edge_s.at[3], edge_r.at[3], me - 1),
        ]

    def start(copies):
        for copy in copies:
            copy.start()

    def landed(copies):
        for copy in copies:
            copy.wait_recv()

    def sent(copies):
        for copy in copies:
            copy.wait_send()

    def pump(i):
        coming = m1(i)
        landed(coming[:2])
        start(forward(i)[:2])
        coming[2].wait_recv()
        start(forward(i)[2:])
        if i + 1 < heads:
            start(first(i + 1))

    def code_copies():
        hub_of = jnp.where(hub, z, jnp.where(z == 0, 1, 2)) * PAIR
        return [
            remote(codes, landed_codes.at[0], cd_s.at[0], cd_r.at[0], hub_of + x),
            remote(codes, landed_codes.at[1], cd_s.at[1], cd_r.at[1], mate),
            remote(codes, landed_codes.at[2], cd_s.at[2], cd_r.at[2], hub_of + 1 - x),
        ]

    up, down = edges()
    to_hub, to_mate, to_other = code_copies()

    @pl.when(end)
    def _():
        start([to_hub, to_other])
        start(m1(0))

    @pl.when(hub)
    def _():
        start([to_mate])
        start(first(0))

    @pl.when(me < n - 1)
    def _():
        start(up)

    @pl.when(me > 0)
    def _():
        start(down)

    for copy in own_copies():
        copy.start()
    own_code = pltpu.make_async_copy(codes, codes_s.at[0], cd_sem.at[0])
    own_code.start()

    @pl.when(end)
    def _():
        for i in range(1, heads):
            start(m1(i))

    @pl.when(hub)
    def _():
        for i in range(heads):
            start(column(i))

    for i in range(LEAD):
        weights(i)[0].start()
    for i in range(heads):
        weights(i)[1].start()

    @pl.when(me == 0)
    def _():
        kwin[0] = jnp.zeros(kwin.shape[1:], kwin.dtype)
        vwin[0] = jnp.zeros(vwin.shape[1:], vwin.dtype)

    @pl.when(me == n - 1)
    def _():
        kwin[nb + 1] = jnp.zeros(kwin.shape[1:], kwin.dtype)
        vwin[nb + 1] = jnp.zeros(vwin.shape[1:], vwin.dtype)

    own_code.wait()

    @pl.when(hub)
    def _():
        landed([to_hub, to_mate, to_other])
        for j in range(3):
            pltpu.make_async_copy(landed_codes.at[j], codes_s.at[1 + j], cd_sem.at[1 + j]).start()
        for j in range(3):
            pltpu.make_async_copy(landed_codes.at[j], codes_s.at[1 + j], cd_sem.at[1 + j]).wait()
        for j in range(4):
            def fill(b, _):
                for r in range(RANDOM):
                    here = codes_s[j, 1, b * RANDOM + r] == x
                    spot = (j * nb + b) * picks + r
                    cell_ref[spot] = jnp.where(here, codes_s[j, 0, b * RANDOM + r], 0)
                    bias_ref[spot] = jnp.where(here, 0.0, masked_score)
                for r in range(RANDOM, picks):
                    spot = (j * nb + b) * picks + r
                    cell_ref[spot] = r - RANDOM
                    bias_ref[spot] = jnp.where(x == 0, 0.0, masked_score)
                return _

            lax.fori_loop(0, nb, fill, 0)

    for copy in own_copies():
        copy.wait()

    @pl.when(me > 0)
    def _():
        landed(up)

    @pl.when(me < n - 1)
    def _():
        landed(down)

    row = lax.broadcasted_iota(jnp.int32, (1, 3 * BLOCK), 1) // BLOCK
    lane = lax.broadcasted_iota(jnp.int32, (BLOCK, 128), 1)
    pick_row = lax.broadcasted_iota(jnp.int32, (1, picks * BLOCK), 1) // BLOCK

    def stat(i, value, table):
        return jnp.where(lane == i, value, table)

    def read_stat(i, table):
        return jnp.sum(jnp.where(lane == i, table, 0.0), axis=1, keepdims=True)

    def window_bias(b):
        gone = jnp.logical_or(
            jnp.logical_and(row == 0, jnp.logical_and(me == 0, b == 0)),
            jnp.logical_and(row == 2, jnp.logical_and(me == n - 1, b == nb - 1)),
        )
        return jnp.where(gone, masked_score, 0.0).astype(jnp.float32)

    def listed(i, number):
        cells = [cell_ref[number * picks + r] for r in range(picks)]
        keys = [kcol[i][cell] for cell in cells]
        values = [vcol[i][cell] for cell in cells]
        bias = jnp.full((1, picks * BLOCK), bias_ref[number * picks], jnp.float32)
        for r in range(1, picks):
            bias = jnp.where(pick_row == r, bias_ref[number * picks + r], bias)
        return keys, values, bias

    def window(i, b):
        keys = [kwin[b + s, :, lanes(i)] for s in range(3)]
        values = [vwin[b + s, :, lanes(i)] for s in range(3)]
        return keys, values, window_bias(b)

    def item(query, lists):
        keys = jnp.concatenate([k for part in lists for k in part[0]], axis=0)
        values = jnp.concatenate([v for part in lists for v in part[1]], axis=0)
        bias = jnp.concatenate([part[2] for part in lists], axis=1) if len(lists) > 1 else lists[0][2]
        return query, keys, values, bias

    def looped(count, unroll, body, table):
        def step(j, table):
            return body([j * unroll + u for u in range(unroll)], table)

        return lax.fori_loop(0, count // unroll, step, table)

    def attend_loop(unroll, item_of, store, base, table, lse_of=None):
        def body(blocks, table):
            done = attend_group([item_of(b) for b in blocks])
            for b, (out, lse) in zip(blocks, done):
                store(b, out)
                table = stat(base + b, lse if lse_of is None else lse_of(b, lse), table)
            return table

        return looped(nb, unroll, body, table)

    def global_rows(i, query_of, store, table, base):
        query = jnp.concatenate([query_of(g) for g in range(GLOBAL // BLOCK)], axis=0)
        out, lse = attend_all(query, kcol[i], vcol[i], 8)
        for g in range(GLOBAL // BLOCK):
            part = slice(g * BLOCK, (g + 1) * BLOCK)
            store(g, out[part])
            table[...] = stat(base + g, lse[part], table[...])

    def packed(table):
        return jnp.transpose(table)[:nb]

    def unpacked(rows):
        wide_rows = jnp.concatenate([rows, jnp.zeros((128 - nb, BLOCK), jnp.float32)], axis=0)
        return jnp.transpose(wide_rows)

    blank = jnp.zeros((BLOCK, 128), jnp.float32)

    def compute_hub(i):
        landed(forward(i))
        landed(first(i))
        for copy in column(i):
            copy.wait()

        for j in (1, 0):
            def put_mate(b, out):
                rsend[i, j, b] = out.astype(jnp.bfloat16)

            tmp[...] = attend_loop(
                UNROLL, lambda b: item(qmate[i, j * nb + b], [listed(i, (2 + j) * nb + b)]),
                put_mate, 0, blank,
            )
            if j == 1:
                @pl.when(jnp.logical_and(z == 1, x == 1))
                def _():
                    global_rows(i, lambda g: qmate[i, nb + g], put_mate, tmp, 0)

            ssend[i, j] = packed(tmp[...])
            start(results(i, j))

        def put_end(b, out):
            loc[i % 2, nb + b] = out

        lend[i % 2] = attend_loop(
            UNROLL, lambda b: item(qend[i, b], [listed(i, nb + b)]), put_end, 0, blank
        )

        @pl.when(jnp.logical_and(z == 1, x == 0))
        def _():
            global_rows(i, lambda g: qend[i, g], put_end, lend.at[i % 2], 0)

        def put_own(b, out):
            loc[i % 2, b] = out

        lstat[i % 2] = attend_loop(
            UNROLL // 2, lambda b: item(qown[b, :, lanes(i)], [window(i, b), listed(i, b)]),
            put_own, 0, blank,
        )

    def compute_end(i):
        def put_own(b, out):
            loc[i % 2, b] = out

        def lse_of(b, lse):
            replaced = jnp.logical_and(me == 0, b < GLOBAL // BLOCK)
            return jnp.where(replaced, masked_score, lse)

        lstat[i % 2] = attend_loop(
            UNROLL, lambda b: item(qown[b, :, lanes(i)], [window(i, b)]), put_own, 0, blank, lse_of
        )

    def put_attn(i, b, value):
        per = nb // heads_n
        attn[i, b // per, pl.ds(pl.multiple_of((b % per) * BLOCK, BLOCK), BLOCK)] = value.astype(jnp.bfloat16)

    def merge_loop(i, j, ours, theirs, store):
        def body(blocks, table):
            done = [
                joined(
                    loc[i % 2, j * nb + b], read_stat(b, ours),
                    rrecv[i, j, b].astype(jnp.float32), read_stat(b, theirs),
                )
                for b in blocks
            ]
            for b, (out, lse) in zip(blocks, done):
                store(b, out)
                table = stat(b, lse, table)
            return table

        return looped(nb, UNROLL, body, blank)

    def merge_own(i):
        merge_loop(i, 0, lstat[i % 2], unpacked(srecv[i, 0]), lambda b, out: put_attn(i, b, out))

    def merge_hub(i):
        landed(results(i, 1))

        def put(b, out):
            esend[i, b] = out.astype(jnp.bfloat16)

        estat[i] = packed(merge_loop(i, 1, lend[i % 2], unpacked(srecv[i, 1]), put))
        start(ended(i))
        landed(results(i, 0))
        merge_own(i)

    def merge_end(i):
        landed(ended(i))
        merge_own(i)

    def share(i):
        start(shares(i))
        pltpu.make_async_copy(attn.at[i, h], attn_all.at[i, h], lc_sem.at[i]).start()

    def load_weights(i):
        copies = []
        for k in range(heads_n):
            source = (w_hbm.at[i] if k == 0 else w_all.at[h ^ k, i])
            target = wbuf.at[i % 2, pl.ds((h ^ k) * wide, wide)]
            copies.append(pltpu.make_async_copy(source, target, wl_sem.at[i % 2, k]))
        return copies

    def project(i):
        landed(shares(i))
        pltpu.make_async_copy(attn.at[i, h], attn_all.at[i, h], lc_sem.at[i]).wait()
        for copy in load_weights(i):
            copy.wait()
        left = jnp.concatenate([attn_all[i, g] for g in range(heads_n)], axis=1)
        tile = 512

        def body(c, _):
            here = pl.ds(pl.multiple_of(c * tile, tile), tile)
            term = jnp.dot(left, wbuf[i % 2, :, here], preferred_element_type=jnp.float32)
            if i > 0:
                term = term + acc[:, here]
            if i < heads - 1:
                acc[:, here] = term
            else:
                out_ref[:, here] = term.astype(jnp.bfloat16)
            return _

        lax.fori_loop(0, acc.shape[1] // tile, body, 0)

    @pl.when(hub)
    def _():
        pump(0)
        pump(1)

    for t in range(heads + LAG):
        if t >= LAG:
            landed(weights(t - LAG)[1:])
            for copy in load_weights(t - LAG):
                copy.start()
        if t < heads:
            @pl.when(hub)
            def _():
                compute_hub(t)
                if t + 2 < heads:
                    pump(t + 2)

            @pl.when(end)
            def _():
                compute_end(t)

        if 1 <= t <= heads:
            @pl.when(hub)
            def _():
                merge_hub(t - 1)

            @pl.when(end)
            def _():
                merge_end(t - 1)

            share(t - 1)
        if t + LEAD < heads:
            weights(t + LEAD)[0].start()
        if t < heads:
            weights(t)[0].wait_recv()
            weights(t)[2].start()
        if t >= LAG:
            project(t - LAG)

    @pl.when(me < n - 1)
    def _():
        sent(up)

    @pl.when(me > 0)
    def _():
        sent(down)

    @pl.when(end)
    def _():
        sent([to_hub, to_other])

    @pl.when(hub)
    def _():
        sent([to_mate])

    for i in range(heads):
        @pl.when(end)
        def _():
            sent(m1(i))

        @pl.when(hub)
        def _():
            sent(forward(i))
            sent(first(i))
            sent(results(i, 0))
            sent(results(i, 1))
            sent(ended(i))

        sent(shares(i))
        sent(weights(i))


UNROLL = 4
LEAD = 3
LAG = 3


def hub_attention(codes, q, k, v, w, picks):
    nb, _, width = q.shape
    heads, wide, columns = w.shape
    heads_n = lax.axis_size("head")
    planes = lax.axis_size("seq") // PAIR
    rows = nb * BLOCK
    share = rows // heads_n
    bf, f32 = jnp.bfloat16, jnp.float32
    dma = pltpu.SemaphoreType.DMA
    col = [pltpu.VMEM((planes * nb, BLOCK, wide), bf)] * (2 * heads)
    scratch = col + [
        pltpu.VMEM((nb, BLOCK, width), bf),
        pltpu.VMEM((heads, nb, BLOCK, wide), bf),
        pltpu.VMEM((heads, 2 * nb, BLOCK, wide), bf),
        pltpu.VMEM((nb + 2, BLOCK, width), bf),
        pltpu.VMEM((nb + 2, BLOCK, width), bf),
        pltpu.VMEM((heads, 2, nb, BLOCK, wide), bf),
        pltpu.VMEM((heads, 2, nb, BLOCK, wide), bf),
        pltpu.VMEM((heads, 2, nb, BLOCK), f32),
        pltpu.VMEM((heads, 2, nb, BLOCK), f32),
        pltpu.VMEM((heads, nb, BLOCK, wide), bf),
        pltpu.VMEM((heads, nb, BLOCK), f32),
        pltpu.VMEM((2, 2 * nb, BLOCK, wide), f32),
        pltpu.VMEM((2, BLOCK, 128), f32),
        pltpu.VMEM((2, BLOCK, 128), f32),
        pltpu.VMEM((BLOCK, 128), f32),
        pltpu.VMEM((heads, heads_n, share, wide), bf),
        pltpu.VMEM((heads, heads_n, share, wide), bf),
        pltpu.VMEM((share, columns), f32),
        pltpu.VMEM((2, heads_n * wide, columns), bf),
        dma((3,)), dma((heads, 2)), dma((4,)), dma((4,)),
        dma((heads, 3)), dma((heads, 3)), dma((heads, 3)), dma((heads, 3)),
        dma((heads, 3)), dma((heads, 3)), dma((heads, 2, 2)), dma((heads, 2, 2)),
        dma((heads, 2)), dma((heads, 2)), dma((heads, 3)), dma((heads, 3)),
        dma((heads, 3)), dma((heads, 3)), dma((2, heads_n)), dma((heads,)),
        pltpu.VMEM((3,) + codes.shape, jnp.int32), pltpu.SMEM((4,) + codes.shape, jnp.int32),
        pltpu.SMEM((4 * nb * picks,), jnp.int32), pltpu.SMEM((4 * nb * picks,), f32),
        dma((3,)), dma((3,)), dma((4,)),
    ]
    anywhere = pl.BlockSpec(memory_space=pl.ANY)
    out, _ = pl.pallas_call(
        functools.partial(hub_kernel, heads, nb, picks),
        out_shape=(
            jax.ShapeDtypeStruct((share, columns), bf),
            jax.ShapeDtypeStruct((heads_n,) + w.shape, bf),
        ),
        in_specs=[anywhere] * 5,
        out_specs=(pl.BlockSpec(memory_space=pltpu.VMEM), anywhere),
        scratch_shapes=scratch,
        compiler_params=pltpu.CompilerParams(
            has_side_effects=True, vmem_limit_bytes=67043328
        ),
    )(codes, q, k, v, w)
    return out


def local_hub(queries, key_rows, value_rows, random_owner, random_local, output_weight):
    rows, width = queries.shape
    nb = rows // BLOCK
    heads = width // HEAD_DIM
    cell = random_owner // PAIR * nb + random_local
    codes = jnp.stack([cell.reshape(-1), (random_owner % PAIR).reshape(-1)])
    codes = jnp.pad(codes, ((0, 6), (0, 128 - codes.shape[1])))
    blocks = lambda a: a.reshape(nb, BLOCK, width)
    return hub_attention(
        codes, blocks(queries), blocks(key_rows), blocks(value_rows),
        output_weight.reshape(heads, HEAD_DIM, -1), RANDOM + GLOBAL // BLOCK,
    )


def local(queries, *others):
    n, heads_n = lax.axis_size("seq"), lax.axis_size("head")
    if n == 4 * PAIR and heads_n == 4:
        return local_hub(queries, *others)
    return local_plain(queries, *others)


def solution(mesh):
    in_specs = (
        P("seq", "head"),
        P("seq", "head"),
        P("seq", "head"),
        P("seq", None),
        P("seq", None),
        P("head", None),
    )
    out_specs = P(("seq", "head"), None)
    return jax.shard_map(local, mesh=mesh, in_specs=in_specs, out_specs=out_specs, check_vma=False)
```

```python
import functools
import math

import jax
import jax.numpy as jnp
from jax import lax
from jax.experimental import pallas as pl
from jax.experimental.pallas import tpu as pltpu
from jax.sharding import PartitionSpec as P

HEAD_DIM = 128
BLOCK = 64
RANDOM = 3
GLOBAL = 128
CHUNKS = 2
PAIR = 2


masked_score = -1e30


def slot_table(owner_ids, local_ids, seq_count, slot_count):
    owner_hits = (owner_ids[:, None] == jnp.arange(seq_count, dtype=jnp.int32)[None, :]).astype(
        jnp.int32
    )
    earlier = jnp.cumsum(owner_hits, axis=0) - owner_hits
    slot_ids = jnp.sum(earlier * owner_hits, axis=1)
    slot_hits = (slot_ids[:, None] == jnp.arange(slot_count, dtype=jnp.int32)[None, :]).astype(
        jnp.int32
    )
    request_table = jnp.sum(
        (owner_hits * local_ids[:, None])[:, :, None] * slot_hits[:, None, :], axis=0
    )
    return (request_table, slot_ids)


def attend_kernel(heads, index_ref, flag_ref, q_ref, *refs):
    near, out_ref = refs[:-1], refs[-1]
    step = pl.program_id(0)
    rate = HEAD_DIM ** (-0.5) * math.log2(math.e)
    first, last = flag_ref[0, step], flag_ref[1, step]
    listed = len(near) * BLOCK
    column = lax.broadcasted_iota(jnp.int32, (1, listed), 1) // BLOCK
    hidden = jnp.logical_or(
        jnp.logical_and(column == 0, first == 1), jnp.logical_and(column == 2, last == 1)
    )
    bias = jnp.where(hidden, masked_score, 0.0).astype(jnp.float32)
    for head in range(heads):
        here = pl.ds(head * HEAD_DIM, HEAD_DIM)
        keys = jnp.concatenate([ref[0, 0, :, here] for ref in near], axis=0)
        values = jnp.concatenate([ref[0, 1, :, here] for ref in near], axis=0)
        scores = lax.dot_general(
            q_ref[:, here], keys, (((1,), (1,)), ((), ())), preferred_element_type=jnp.float32
        )
        scores = scores + bias
        top = jnp.max(scores, axis=1, keepdims=True)
        weight = jnp.exp2((scores - top) * rate)
        total = jnp.sum(weight, axis=1, keepdims=True)
        context = jnp.dot(
            weight.astype(jnp.bfloat16), values, preferred_element_type=jnp.float32
        )
        out_ref[:, here] = (context / total).astype(out_ref.dtype)


def attend(queries, pool, index, flags):
    tokens, width = queries.shape
    blocks = tokens // BLOCK
    heads = width // HEAD_DIM
    listed = index.shape[0]

    def picked(r):
        return pl.BlockSpec(
            (1, 2, BLOCK, width), lambda i, index_ref, flag_ref: (index_ref[r, i], 0, 0, 0)
        )

    return pl.pallas_call(
        functools.partial(attend_kernel, heads),
        grid_spec=pltpu.PrefetchScalarGridSpec(
            num_scalar_prefetch=2,
            grid=(blocks,),
            in_specs=[pl.BlockSpec((BLOCK, width), lambda i, a, b: (i, 0))]
            + [picked(r) for r in range(listed)],
            out_specs=pl.BlockSpec((BLOCK, width), lambda i, a, b: (i, 0)),
        ),
        out_shape=jax.ShapeDtypeStruct(queries.shape, jnp.bfloat16),
        compiler_params=pltpu.CompilerParams(dimension_semantics=("arbitrary",)),
        cost_estimate=pl.CostEstimate(
            flops=60 * tokens * width * 8 * BLOCK,
            bytes_accessed=blocks * 14 * BLOCK * width * 2,
            transcendentals=tokens * heads * 8 * BLOCK,
        ),
    )(index, flags, queries, *([pool] * listed))


def merged(left, right):
    joint = jnp.maximum(left[0], right[0])
    a, b = jnp.exp(left[0] - joint), jnp.exp(right[0] - joint)
    return (
        joint,
        left[1] * a + right[1] * b,
        left[2] * a[:, :, None] + right[2] * b[:, :, None],
    )


def partial_softmax(query, keys, values):
    tokens, width = query.shape
    heads = width // HEAD_DIM
    query = query.reshape(tokens, heads, HEAD_DIM)
    keys, values = (a.reshape(-1, heads, HEAD_DIM) for a in (keys, values))
    scores = jnp.einsum("qhd,khd->hqk", query, keys, preferred_element_type=jnp.float32)
    scores = scores * HEAD_DIM ** (-0.5)
    row_max = jnp.max(scores, axis=2)
    weight = jnp.exp(scores - row_max[:, :, None])
    row_total = jnp.sum(weight, axis=2)
    value = jnp.einsum(
        "hqk,khd->hqd", weight.astype(jnp.bfloat16), values, preferred_element_type=jnp.float32
    )
    return row_max, row_total, value


def after(array, *others):
    return lax.optimization_barrier((array,) + others)[0]


def local_plain(queries, key_rows, value_rows, random_owner, random_local, output_weight):
    n = lax.axis_size("seq")
    me = lax.axis_index("seq")
    heads_n = lax.axis_size("head")
    h = lax.axis_index("head")
    token_count, width_here = queries.shape
    nb = token_count // BLOCK
    gb = GLOBAL // BLOCK
    heads_here = width_here // HEAD_DIM
    slot_count = max(2, 4 * nb // n)
    depth = n // PAIR
    z, x = me // PAIR, me % PAIR

    def send(array, pairs, axis="seq"):
        return jax.tree.map(lambda part: lax.ppermute(part, axis, pairs), array)

    def swapped(array, m):
        return lax.ppermute(array, "head", [(i, i ^ m) for i in range(heads_n)])

    def folded(part, pairs, here):
        packed = jnp.concatenate([part[2], part[0][:, None], part[1][:, None]], axis=1)
        got = send(packed, pairs)
        both = merged(part, (got[:, GLOBAL], got[:, GLOBAL + 1], got[:, :GLOBAL]))
        return jax.tree.map(lambda a, b: jnp.where(here, a, b), both, part)

    def finished(part):
        out = jnp.transpose(part[2] / part[1][:, :, None], (1, 0, 2))
        return out.reshape(GLOBAL, -1).astype(jnp.bfloat16)

    chunks = math.gcd(CHUNKS, heads_here)
    cw = width_here // chunks
    cuts = [slice(c * cw, (c + 1) * cw) for c in range(chunks)]
    key_blocks = key_rows.reshape(nb, BLOCK, width_here)
    value_blocks = value_rows.reshape(nb, BLOCK, width_here)
    owned = [jnp.stack([key_blocks[..., sl], value_blocks[..., sl]], axis=1) for sl in cuts]
    up = [(i, i + 1) for i in range(n - 1)]
    down = [(i + 1, i) for i in range(n - 1)]
    mates = [(i, i + 1 if i % PAIR == 0 else i - 1) for i in range(n)]
    owner_flat = random_owner.reshape(-1)
    local_flat = random_local.reshape(-1)
    request_table, slot_ids = slot_table(owner_flat, local_flat, n, slot_count)
    line_wins = n % PAIR == 0 and nb <= PAIR * slot_count
    global_ids = jnp.arange(gb, dtype=jnp.int32)
    pools, tops, last = [], [], None

    if line_wins:
        mate_owner, mate_local = send((owner_flat, local_flat), mates)
        near_query = jnp.where(me == 1, send(queries[:GLOBAL], [(0, 1)]), queries[:GLOBAL])
        befores = [send(own[-1:], up) for own in owned]
        afters = [send(own[:1], down) for own in owned]
        mate_table, _ = slot_table(mate_owner, mate_local, n, slot_count)
        fetch = slot_count + gb
        mate_table = jnp.concatenate(
            [mate_table, jnp.broadcast_to(global_ids[None], (n, gb))], axis=1
        )
        offsets = [0]
        for s in range(1, depth):
            offsets += [-s, s]
        bufs = [{0: own} for own in owned]
        for s in range(1, depth):
            upward = [(i, i + PAIR) for i in range((s - 1) * PAIR, n - PAIR)]
            downward = [(i, i - PAIR) for i in range(PAIR, n - (s - 1) * PAIR)]
            for held in bufs:
                held[-s] = send(held[1 - s], upward)
                held[s] = send(held[s - 1], downward)
        for c in range(chunks):
            crossed = []
            for d in offsets:
                holder = jnp.clip((z + d) * PAIR + x, 0, n - 1)
                asked = jnp.take(bufs[c][d], mate_table[holder], axis=0)
                good = [(i, j) for i, j in mates if 0 <= i // PAIR + d < depth]
                crossed.append(send(asked, good))
            part = None
            for s in range(depth):
                held = bufs[c][s]
                term = partial_softmax(near_query[:, cuts[c]], held[:, 0], held[:, 1])
                part = term if part is None else merged(part, term)
            tops.append(finished(folded(part, [(1, 0)], me == 0)))
            pools.append(
                jnp.concatenate(
                    [bufs[c][d] for d in offsets] + crossed + [befores[c], afters[c]], axis=0
                )
            )
        last = bufs[0][depth - 1]
        place = jnp.where(owner_flat // PAIR < z, 2 * (z - owner_flat // PAIR) - 1,
                          2 * (owner_flat // PAIR - z))
        line_total = len(offsets) * nb
        cell = jnp.where(
            owner_flat % PAIR == x,
            place * nb + local_flat,
            line_total + place * fetch + slot_ids,
        )
        root = jnp.maximum(2 * z - 1, 0)
        global_cell = global_ids + jnp.where(
            x == 0, root * nb, line_total + root * fetch + slot_count
        )
        edge = line_total + len(offsets) * fetch
    else:
        rows = jnp.stack([queries[:GLOBAL], key_rows[:GLOBAL], value_rows[:GLOBAL]])
        rows = jnp.where(me == 1, send(rows, [(0, 1)]), rows)
        for s in range(1, depth):
            got = send(rows, [((s - 1) * PAIR + q, s * PAIR + q) for q in range(PAIR)])
            rows = jnp.where(z == s, got, rows)
        part = partial_softmax(rows[0], key_rows, value_rows)
        for s in range(depth - 1, 0, -1):
            pairs = [(s * PAIR + q, (s - 1) * PAIR + q) for q in range(PAIR)]
            part = folded(part, pairs, z == s - 1)
        top = finished(folded(part, [(1, 0)], me == 0))
        wanted = lax.all_to_all(request_table, "seq", split_axis=0, concat_axis=0, tiled=True)
        for c, own in enumerate(owned):
            tops.append(top[:, cuts[c]])
            sent = jnp.take(own, wanted.reshape(-1), axis=0)
            got = lax.all_to_all(sent, "seq", split_axis=0, concat_axis=0, tiled=True)
            shared = jnp.stack(
                [rows[i][:, cuts[c]].reshape(gb, BLOCK, cw) for i in (1, 2)], axis=1
            )
            edges = [send(own[-1:], up), send(own[:1], down)]
            pools.append(jnp.concatenate([own, got, shared] + edges, axis=0))
        cell = nb + owner_flat * slot_count + slot_ids
        global_cell = nb + n * slot_count + global_ids
        edge = nb + n * slot_count + gb

    weights, order, bit = [output_weight], [0], heads_n
    while bit > 1:
        bit //= 2
        for m in list(order):
            held = weights[order.index(m)]
            if m and last is not None:
                held = after(held, last)
            weights.append(swapped(held, bit))
            order.append(m ^ bit)

    steps = jnp.arange(nb, dtype=jnp.int32)
    cell = cell.reshape(nb, RANDOM)
    index = jnp.stack(
        [
            jnp.where(steps == 0, edge, steps - 1),
            steps,
            jnp.where(steps == nb - 1, edge + 1, steps + 1),
        ]
        + [cell[:, r] for r in range(RANDOM)]
        + [jnp.broadcast_to(global_cell[g], (nb,)) for g in range(gb)]
    ).astype(jnp.int32)
    numbers = me * nb + steps
    flags = jnp.stack([numbers == 0, numbers == n * nb - 1]).astype(jnp.int32)

    share = token_count // heads_n
    pieces = [[] for _ in order]
    for c, sl in enumerate(cuts):
        sparse = attend(queries[:, sl], pools[c], index, flags)
        top = jnp.where(me == 0, tops[c], sparse[:GLOBAL])
        sparse = jnp.concatenate([top, sparse[GLOBAL:]], axis=0)
        for k, m in enumerate(order):
            piece = lax.dynamic_slice_in_dim(sparse, (h ^ m) * share, share, 0)
            pieces[k].append(piece if m == 0 else swapped(piece, m))
    total = None
    for k in range(len(order)):
        term = jnp.dot(
            jnp.concatenate(pieces[k], axis=1), weights[k], preferred_element_type=jnp.float32
        )
        total = term if total is None else total + term
    return total.astype(jnp.bfloat16)


MESH = pl.DeviceIdType.MESH
RATE = HEAD_DIM ** (-0.5) * math.log2(math.e)
NT = (((1,), (1,)), ((), ()))


def attend_group(items):
    scores = [
        lax.dot_general(query, keys, NT, preferred_element_type=jnp.float32)
        for query, keys, _, _ in items
    ]
    scores = [a if item[3] is None else a + item[3] for a, item in zip(scores, items)]
    tops = [jnp.max(a, axis=1, keepdims=True) for a in scores]
    parts = [jnp.exp2((a - top) * RATE) for a, top in zip(scores, tops)]
    totals = [jnp.sum(a, axis=1, keepdims=True) for a in parts]
    accs = [
        jnp.dot(a.astype(jnp.bfloat16), item[2], preferred_element_type=jnp.float32)
        for a, item in zip(parts, items)
    ]
    return [
        (acc * (1.0 / total), top * RATE + jnp.log2(total))
        for acc, total, top in zip(accs, totals, tops)
    ]


def attend_all(query, k_ref, v_ref, step):
    rows = query.shape[0]
    cells = k_ref.shape[0]

    def chunk(c):
        keys = k_ref[pl.ds(c * step, step)].reshape(step * BLOCK, HEAD_DIM)
        values = v_ref[pl.ds(c * step, step)].reshape(step * BLOCK, HEAD_DIM)
        return query, keys, values, None

    def body(c, carry):
        for part in attend_group([chunk(2 * c), chunk(2 * c + 1)]):
            carry = joined(*carry, *part)
        return carry

    start = (
        jnp.zeros((rows, HEAD_DIM), jnp.float32),
        jnp.full((rows, 1), masked_score, jnp.float32),
    )
    return lax.fori_loop(0, cells // (2 * step), body, start)


def joined(o1, l1, o2, l2):
    top = jnp.maximum(l1, l2)
    a, b = jnp.exp2(l1 - top), jnp.exp2(l2 - top)
    total = a + b
    return (o1 * a + o2 * b) / total, top + jnp.log2(total)


def hub_kernel(heads, nb, picks, codes, q_hbm, k_hbm, v_hbm, w_hbm, out_ref, w_all, *rest):
    kcol, vcol = rest[:heads], rest[heads:2 * heads]
    (qown, qend, qmate, kwin, vwin, rsend, rrecv, ssend, srecv, esend, estat, loc, lstat, tmp,
     attn, attn_all, acc, wbuf, own_sem, col_sem, m1_s, m1_r, fw_s, fw_r,
     hb_s, hb_r, re_s, re_r, er_s, er_r, at_s, at_r, w_s, w_r, wl_sem, lc_sem,
     landed_codes, codes_s, cell_ref, bias_ref, cd_s, cd_r, cd_sem) = rest[2 * heads:]
    me = lax.axis_index("seq")
    h = lax.axis_index("head")
    n = lax.axis_size("seq")
    heads_n = lax.axis_size("head")
    z, x = me // PAIR, me % PAIR
    hub = jnp.logical_or(z == 1, z == 2)
    end = jnp.logical_not(hub)
    own_end = jnp.where(z == 1, 0, 3)
    partner = jnp.where(hub, jnp.where(z == 1, 0, 3), jnp.where(z == 0, 1, 2)) * PAIR + x
    other = (3 - z) * PAIR + x
    mate = z * PAIR + (1 - x)
    wide = HEAD_DIM
    lanes = lambda i: slice(i * wide, (i + 1) * wide)
    finish = []

    def remote(src, dst, ss, rs, seq, head=None):
        return pltpu.make_async_remote_copy(
            src_ref=src, dst_ref=dst, send_sem=ss, recv_sem=rs,
            device_id=(seq, h if head is None else head), device_id_type=MESH,
        )

    def planes(p):
        return pl.ds(p * nb, nb)

    def m1(i):
        return [
            remote(k_hbm.at[:, :, lanes(i)], kcol[i].at[planes(z)], m1_s.at[i, 0], m1_r.at[i, 0], partner),
            remote(v_hbm.at[:, :, lanes(i)], vcol[i].at[planes(z)], m1_s.at[i, 1], m1_r.at[i, 1], partner),
            remote(q_hbm.at[:, :, lanes(i)], qend.at[i], m1_s.at[i, 2], m1_r.at[i, 2], partner),
        ]

    def forward(i):
        return [
            remote(kcol[i].at[planes(own_end)], kcol[i].at[planes(own_end)], fw_s.at[i, 0], fw_r.at[i, 0], other),
            remote(vcol[i].at[planes(own_end)], vcol[i].at[planes(own_end)], fw_s.at[i, 1], fw_r.at[i, 1], other),
            remote(qend.at[i], qmate.at[i, pl.ds(nb, nb)], fw_s.at[i, 2], fw_r.at[i, 2], mate),
        ]

    def first(i):
        return [
            remote(k_hbm.at[:, :, lanes(i)], kcol[i].at[planes(z)], hb_s.at[i, 0], hb_r.at[i, 0], other),
            remote(v_hbm.at[:, :, lanes(i)], vcol[i].at[planes(z)], hb_s.at[i, 1], hb_r.at[i, 1], other),
            remote(q_hbm.at[:, :, lanes(i)], qmate.at[i, pl.ds(0, nb)], hb_s.at[i, 2], hb_r.at[i, 2], mate),
        ]

    def results(i, j):
        to = (mate, own_end * PAIR + 1 - x)[j]
        return [
            remote(part.at[i, j], into.at[i, j], re_s.at[i, j, k], re_r.at[i, j, k], to)
            for k, (part, into) in enumerate(((rsend, rrecv), (ssend, srecv)))
        ]

    def ended(i):
        return [
            remote(esend.at[i], rrecv.at[i, 0], er_s.at[i, 0], er_r.at[i, 0], partner),
            remote(estat.at[i], srecv.at[i, 0], er_s.at[i, 1], er_r.at[i, 1], partner),
        ]

    def shares(i):
        return [
            remote(attn.at[i, h ^ k], attn_all.at[i, h], at_s.at[i, k - 1], at_r.at[i, k - 1], me, h ^ k)
            for k in range(1, heads_n)
        ]

    def weights(i):
        return [
            remote(w_hbm.at[i], w_all.at[h, i], w_s.at[i, 0], w_r.at[i, 0], me, h ^ 2),
            remote(w_hbm.at[i], w_all.at[h, i], w_s.at[i, 1], w_r.at[i, 1], me, h ^ 1),
            remote(w_all.at[h ^ 2, i], w_all.at[h ^ 2, i], w_s.at[i, 2], w_r.at[i, 2], me, h ^ 1),
        ]

    def own_copies():
        return [
            pltpu.make_async_copy(q_hbm, qown, own_sem.at[0]),
            pltpu.make_async_copy(k_hbm, kwin.at[pl.ds(1, nb)], own_sem.at[1]),
            pltpu.make_async_copy(v_hbm, vwin.at[pl.ds(1, nb)], own_sem.at[2]),
        ]

    def column(i):
        return [
            pltpu.make_async_copy(k_hbm.at[:, :, lanes(i)], kcol[i].at[planes(z)], col_sem.at[i, 0]),
            pltpu.make_async_copy(v_hbm.at[:, :, lanes(i)], vcol[i].at[planes(z)], col_sem.at[i, 1]),
        ]

    def start(copies):
        for copy in copies:
            copy.start()

    def landed(copies):
        for copy in copies:
            copy.wait_recv()

    def sent(copies):
        for copy in copies:
            copy.wait_send()

    def pump(i):
        coming = m1(i)
        landed(coming[:2])
        start(forward(i)[:2])
        coming[2].wait_recv()
        start(forward(i)[2:])
        if i + 1 < heads:
            start(first(i + 1))

    def code_copies():
        hub_of = jnp.where(hub, z, jnp.where(z == 0, 1, 2)) * PAIR
        return [
            remote(codes, landed_codes.at[0], cd_s.at[0], cd_r.at[0], hub_of + x),
            remote(codes, landed_codes.at[1], cd_s.at[1], cd_r.at[1], mate),
            remote(codes, landed_codes.at[2], cd_s.at[2], cd_r.at[2], hub_of + 1 - x),
        ]

    to_hub, to_mate, to_other = code_copies()

    @pl.when(end)
    def _():
        start([to_hub, to_other])
        start(m1(0))

    @pl.when(hub)
    def _():
        start([to_mate])
        start(first(0))

    for copy in own_copies():
        copy.start()
    own_code = pltpu.make_async_copy(codes, codes_s.at[0], cd_sem.at[0])
    own_code.start()

    @pl.when(end)
    def _():
        for i in range(1, heads):
            start(m1(i))

    @pl.when(hub)
    def _():
        for i in range(heads):
            start(column(i))

    for i in range(LEAD):
        weights(i)[0].start()
    for i in range(heads):
        weights(i)[1].start()

    for spot in (0, nb + 1):
        kwin[spot] = jnp.zeros(kwin.shape[1:], kwin.dtype)
        vwin[spot] = jnp.zeros(vwin.shape[1:], vwin.dtype)

    own_code.wait()

    @pl.when(hub)
    def _():
        landed([to_hub, to_mate, to_other])
        for j in range(3):
            pltpu.make_async_copy(landed_codes.at[j], codes_s.at[1 + j], cd_sem.at[1 + j]).start()
        for j in range(3):
            pltpu.make_async_copy(landed_codes.at[j], codes_s.at[1 + j], cd_sem.at[1 + j]).wait()
        for j in range(4):
            def fill(b, _):
                for r in range(RANDOM):
                    here = codes_s[j, 1, b * RANDOM + r] == x
                    spot = (j * nb + b) * picks + r
                    cell_ref[spot] = jnp.where(here, codes_s[j, 0, b * RANDOM + r], 0)
                    bias_ref[spot] = jnp.where(here, 0.0, masked_score)
                for r in range(RANDOM, picks - 1):
                    spot = (j * nb + b) * picks + r
                    cell_ref[spot] = r - RANDOM
                    bias_ref[spot] = jnp.where(x == 0, 0.0, masked_score)
                home = jnp.where(j % 2 == 0, z, own_end) * PAIR + jnp.where(j < 2, x, 1 - x)
                beside = jnp.where(b == 0, home - 1, home + 1)
                known = jnp.logical_and(beside >= 0, beside < n)
                known = jnp.logical_and(known, jnp.logical_or(b == 0, b == nb - 1))
                spot = (j * nb + b) * picks + picks - 1
                cell_ref[spot] = jnp.where(known, beside // PAIR * nb + jnp.where(b == 0, nb - 1, 0), 0)
                bias_ref[spot] = jnp.where(known, 0.0, masked_score)
                return _

            lax.fori_loop(0, nb, fill, 0)

    for copy in own_copies():
        copy.wait()

    row = lax.broadcasted_iota(jnp.int32, (1, 3 * BLOCK), 1) // BLOCK
    lane = lax.broadcasted_iota(jnp.int32, (BLOCK, 128), 1)
    pick_row = lax.broadcasted_iota(jnp.int32, (1, picks * BLOCK), 1) // BLOCK

    def stat(i, value, table):
        return jnp.where(lane == i, value, table)

    def read_stat(i, table):
        return jnp.sum(jnp.where(lane == i, table, 0.0), axis=1, keepdims=True)

    def window_bias(b):
        gone = jnp.logical_or(
            jnp.logical_and(row == 0, b == 0), jnp.logical_and(row == 2, b == nb - 1)
        )
        return jnp.where(gone, masked_score, 0.0).astype(jnp.float32)

    def listed(i, number, count):
        cells = [cell_ref[number * picks + r] for r in range(count)]
        keys = [kcol[i][cell] for cell in cells]
        values = [vcol[i][cell] for cell in cells]
        bias = jnp.full((1, count * BLOCK), bias_ref[number * picks], jnp.float32)
        for r in range(1, count):
            bias = jnp.where(pick_row[:, :count * BLOCK] == r, bias_ref[number * picks + r], bias)
        return keys, values, bias

    def window(i, b):
        keys = [kwin[b + s, :, lanes(i)] for s in range(3)]
        values = [vwin[b + s, :, lanes(i)] for s in range(3)]
        return keys, values, window_bias(b)

    def item(query, lists):
        keys = jnp.concatenate([k for part in lists for k in part[0]], axis=0)
        values = jnp.concatenate([v for part in lists for v in part[1]], axis=0)
        bias = jnp.concatenate([part[2] for part in lists], axis=1) if len(lists) > 1 else lists[0][2]
        return query, keys, values, bias

    def looped(count, unroll, body, table):
        def step(j, table):
            return body([j * unroll + u for u in range(unroll)], table)

        return lax.fori_loop(0, count // unroll, step, table)

    def attend_loop(unroll, item_of, store, base, table, lse_of=None):
        def body(blocks, table):
            done = attend_group([item_of(b) for b in blocks])
            for b, (out, lse) in zip(blocks, done):
                store(b, out)
                table = stat(base + b, lse if lse_of is None else lse_of(b, lse), table)
            return table

        return looped(nb, unroll, body, table)

    def global_rows(i, query_of, store, table, base):
        query = jnp.concatenate([query_of(g) for g in range(GLOBAL // BLOCK)], axis=0)
        out, lse = attend_all(query, kcol[i], vcol[i], 8)
        for g in range(GLOBAL // BLOCK):
            part = slice(g * BLOCK, (g + 1) * BLOCK)
            store(g, out[part])
            table[...] = stat(base + g, lse[part], table[...])

    def packed(table):
        return jnp.transpose(table)[:nb]

    def unpacked(rows):
        wide_rows = jnp.concatenate([rows, jnp.zeros((128 - nb, BLOCK), jnp.float32)], axis=0)
        return jnp.transpose(wide_rows)

    blank = jnp.zeros((BLOCK, 128), jnp.float32)

    def compute_hub(i):
        landed(forward(i))
        landed(first(i))
        for copy in column(i):
            copy.wait()

        def to_mate_set(j):
            def put_mate(b, out):
                rsend[i, j, b] = out.astype(jnp.bfloat16)

            tmp[...] = attend_loop(
                UNROLL, lambda b: item(qmate[i, j * nb + b], [listed(i, (2 + j) * nb + b, picks)]),
                put_mate, 0, blank,
            )
            if j == 1:
                @pl.when(jnp.logical_and(z == 1, x == 1))
                def _():
                    global_rows(i, lambda g: qmate[i, nb + g], put_mate, tmp, 0)

            ssend[i, j] = packed(tmp[...])
            start(results(i, j))

        def put_end(b, out):
            esend[i, b] = out.astype(jnp.bfloat16)

        to_mate_set(1)
        tmp[...] = attend_loop(
            UNROLL, lambda b: item(qend[i, b], [listed(i, nb + b, picks - 1)]), put_end, 0, blank
        )

        @pl.when(jnp.logical_and(z == 1, x == 0))
        def _():
            global_rows(i, lambda g: qend[i, g], put_end, tmp, 0)

        estat[i] = packed(tmp[...])
        start(ended(i))
        to_mate_set(0)

        def put_own(b, out):
            loc[i % 2, b] = out

        lstat[i % 2] = attend_loop(
            UNROLL // 2, lambda b: item(qown[b, :, lanes(i)], [window(i, b), listed(i, b, picks - 1)]),
            put_own, 0, blank,
        )

    def compute_end(i):
        def put_own(b, out):
            loc[i % 2, b] = out

        def lse_of(b, lse):
            replaced = jnp.logical_and(me == 0, b < GLOBAL // BLOCK)
            return jnp.where(replaced, masked_score, lse)

        lstat[i % 2] = attend_loop(
            UNROLL, lambda b: item(qown[b, :, lanes(i)], [window(i, b)]), put_own, 0, blank, lse_of
        )

    def put_attn(i, b, value):
        per = nb // heads_n
        attn[i, b // per, pl.ds(pl.multiple_of((b % per) * BLOCK, BLOCK), BLOCK)] = value.astype(jnp.bfloat16)

    def merge_own(i, count):
        ours = lstat[i % 2]
        theirs = [unpacked(srecv[i, j]) for j in range(count)]

        def body(blocks, _):
            done = [(loc[i % 2, b], read_stat(b, ours)) for b in blocks]
            for j in range(count):
                done = [
                    joined(*part, rrecv[i, j, b].astype(jnp.float32), read_stat(b, theirs[j]))
                    for part, b in zip(done, blocks)
                ]
            for b, (out, _lse) in zip(blocks, done):
                put_attn(i, b, out)
            return _

        looped(nb, UNROLL, body, 0)

    def merge_hub(i):
        landed(results(i, 0))
        merge_own(i, 1)

    def merge_end(i):
        landed(results(i, 1))
        landed(ended(i))
        merge_own(i, 2)

    def share(i):
        start(shares(i))
        pltpu.make_async_copy(attn.at[i, h], attn_all.at[i, h], lc_sem.at[i]).start()

    def load_weights(i):
        copies = []
        for k in range(heads_n):
            source = (w_hbm.at[i] if k == 0 else w_all.at[h ^ k, i])
            target = wbuf.at[i % 2, pl.ds((h ^ k) * wide, wide)]
            copies.append(pltpu.make_async_copy(source, target, wl_sem.at[i % 2, k]))
        return copies

    def project(i):
        landed(shares(i))
        pltpu.make_async_copy(attn.at[i, h], attn_all.at[i, h], lc_sem.at[i]).wait()
        for copy in load_weights(i):
            copy.wait()
        left = jnp.concatenate([attn_all[i, g] for g in range(heads_n)], axis=1)
        tile = 512

        def body(c, _):
            here = pl.ds(pl.multiple_of(c * tile, tile), tile)
            term = jnp.dot(left, wbuf[i % 2, :, here], preferred_element_type=jnp.float32)
            if i > 0:
                term = term + acc[:, here]
            if i < heads - 1:
                acc[:, here] = term
            else:
                out_ref[:, here] = term.astype(jnp.bfloat16)
            return _

        lax.fori_loop(0, acc.shape[1] // tile, body, 0)

    @pl.when(hub)
    def _():
        pump(0)
        pump(1)

    def fetch(i):
        landed(weights(i)[1:])
        for copy in load_weights(i):
            copy.start()

    def relay(i):
        weights(i)[0].wait_recv()
        weights(i)[2].start()

    for t in range(heads):
        if t >= LAG:
            fetch(t - LAG)

        @pl.when(hub)
        def _():
            compute_hub(t)
            if t + 2 < heads:
                pump(t + 2)

        @pl.when(end)
        def _():
            compute_end(t)

        if t >= 1:
            @pl.when(hub)
            def _():
                merge_hub(t - 1)

            @pl.when(end)
            def _():
                merge_end(t - 1)

            share(t - 1)
        if t + LEAD < heads:
            weights(t + LEAD)[0].start()
        if t >= 1:
            relay(t - 1)
        if t >= LAG:
            project(t - LAG)

    for i in range(heads - LAG, heads - 1):
        fetch(i)
        project(i)

    @pl.when(hub)
    def _():
        merge_hub(heads - 1)

    @pl.when(end)
    def _():
        merge_end(heads - 1)

    share(heads - 1)
    relay(heads - 1)
    fetch(heads - 1)
    project(heads - 1)

    @pl.when(end)
    def _():
        sent([to_hub, to_other])

    @pl.when(hub)
    def _():
        sent([to_mate])

    for i in range(heads):
        @pl.when(end)
        def _():
            sent(m1(i))

        @pl.when(hub)
        def _():
            sent(forward(i))
            sent(first(i))
            sent(results(i, 0))
            sent(results(i, 1))
            sent(ended(i))

        sent(shares(i))
        sent(weights(i))


UNROLL = 4
LEAD = 3
LAG = 3


def hub_attention(codes, q, k, v, w, picks):
    nb, _, width = q.shape
    heads, wide, columns = w.shape
    heads_n = lax.axis_size("head")
    planes = lax.axis_size("seq") // PAIR
    rows = nb * BLOCK
    share = rows // heads_n
    bf, f32 = jnp.bfloat16, jnp.float32
    dma = pltpu.SemaphoreType.DMA
    col = [pltpu.VMEM((planes * nb, BLOCK, wide), bf)] * (2 * heads)
    scratch = col + [
        pltpu.VMEM((nb, BLOCK, width), bf),
        pltpu.VMEM((heads, nb, BLOCK, wide), bf),
        pltpu.VMEM((heads, 2 * nb, BLOCK, wide), bf),
        pltpu.VMEM((nb + 2, BLOCK, width), bf),
        pltpu.VMEM((nb + 2, BLOCK, width), bf),
        pltpu.VMEM((heads, 2, nb, BLOCK, wide), bf),
        pltpu.VMEM((heads, 2, nb, BLOCK, wide), bf),
        pltpu.VMEM((heads, 2, nb, BLOCK), f32),
        pltpu.VMEM((heads, 2, nb, BLOCK), f32),
        pltpu.VMEM((heads, nb, BLOCK, wide), bf),
        pltpu.VMEM((heads, nb, BLOCK), f32),
        pltpu.VMEM((2, nb, BLOCK, wide), f32),
        pltpu.VMEM((2, BLOCK, 128), f32),
        pltpu.VMEM((BLOCK, 128), f32),
        pltpu.VMEM((heads, heads_n, share, wide), bf),
        pltpu.VMEM((heads, heads_n, share, wide), bf),
        pltpu.VMEM((share, columns), f32),
        pltpu.VMEM((2, heads_n * wide, columns), bf),
        dma((3,)), dma((heads, 2)),
        dma((heads, 3)), dma((heads, 3)), dma((heads, 3)), dma((heads, 3)),
        dma((heads, 3)), dma((heads, 3)), dma((heads, 2, 2)), dma((heads, 2, 2)),
        dma((heads, 2)), dma((heads, 2)), dma((heads, 3)), dma((heads, 3)),
        dma((heads, 3)), dma((heads, 3)), dma((2, heads_n)), dma((heads,)),
        pltpu.VMEM((3,) + codes.shape, jnp.int32), pltpu.SMEM((4,) + codes.shape, jnp.int32),
        pltpu.SMEM((4 * nb * picks,), jnp.int32), pltpu.SMEM((4 * nb * picks,), f32),
        dma((3,)), dma((3,)), dma((4,)),
    ]
    anywhere = pl.BlockSpec(memory_space=pl.ANY)
    out, _ = pl.pallas_call(
        functools.partial(hub_kernel, heads, nb, picks),
        out_shape=(
            jax.ShapeDtypeStruct((share, columns), bf),
            jax.ShapeDtypeStruct((heads_n,) + w.shape, bf),
        ),
        in_specs=[anywhere] * 5,
        out_specs=(pl.BlockSpec(memory_space=pltpu.VMEM), anywhere),
        scratch_shapes=scratch,
        compiler_params=pltpu.CompilerParams(
            has_side_effects=True, vmem_limit_bytes=67043328
        ),
    )(codes, q, k, v, w)
    return out


def local_hub(queries, key_rows, value_rows, random_owner, random_local, output_weight):
    rows, width = queries.shape
    nb = rows // BLOCK
    heads = width // HEAD_DIM
    cell = random_owner // PAIR * nb + random_local
    codes = jnp.stack([cell.reshape(-1), (random_owner % PAIR).reshape(-1)])
    codes = jnp.pad(codes, ((0, 6), (0, 128 - codes.shape[1])))
    blocks = lambda a: a.reshape(nb, BLOCK, width)
    return hub_attention(
        codes, blocks(queries), blocks(key_rows), blocks(value_rows),
        output_weight.reshape(heads, HEAD_DIM, -1), RANDOM + GLOBAL // BLOCK + 1,
    )


def local(queries, *others):
    n, heads_n = lax.axis_size("seq"), lax.axis_size("head")
    if n == 4 * PAIR and heads_n == 4:
        return local_hub(queries, *others)
    return local_plain(queries, *others)


def solution(mesh):
    in_specs = (
        P("seq", "head"),
        P("seq", "head"),
        P("seq", "head"),
        P("seq", None),
        P("seq", None),
        P("head", None),
    )
    out_specs = P(("seq", "head"), None)
    return jax.shard_map(local, mesh=mesh, in_specs=in_specs, out_specs=out_specs, check_vma=False)
```

```python
import functools
import math

import jax
import jax.numpy as jnp
from jax import lax
from jax.experimental import pallas as pl
from jax.experimental.pallas import tpu as pltpu
from jax.sharding import PartitionSpec as P

HEAD_DIM = 128
BLOCK = 64
RANDOM = 3
GLOBAL = 128
CHUNKS = 2
PAIR = 2


masked_score = -1e30


def slot_table(owner_ids, local_ids, seq_count, slot_count):
    owner_hits = (owner_ids[:, None] == jnp.arange(seq_count, dtype=jnp.int32)[None, :]).astype(
        jnp.int32
    )
    earlier = jnp.cumsum(owner_hits, axis=0) - owner_hits
    slot_ids = jnp.sum(earlier * owner_hits, axis=1)
    slot_hits = (slot_ids[:, None] == jnp.arange(slot_count, dtype=jnp.int32)[None, :]).astype(
        jnp.int32
    )
    request_table = jnp.sum(
        (owner_hits * local_ids[:, None])[:, :, None] * slot_hits[:, None, :], axis=0
    )
    return (request_table, slot_ids)


def attend_kernel(heads, index_ref, flag_ref, q_ref, *refs):
    near, out_ref = refs[:-1], refs[-1]
    step = pl.program_id(0)
    rate = HEAD_DIM ** (-0.5) * math.log2(math.e)
    first, last = flag_ref[0, step], flag_ref[1, step]
    listed = len(near) * BLOCK
    column = lax.broadcasted_iota(jnp.int32, (1, listed), 1) // BLOCK
    hidden = jnp.logical_or(
        jnp.logical_and(column == 0, first == 1), jnp.logical_and(column == 2, last == 1)
    )
    bias = jnp.where(hidden, masked_score, 0.0).astype(jnp.float32)
    for head in range(heads):
        here = pl.ds(head * HEAD_DIM, HEAD_DIM)
        keys = jnp.concatenate([ref[0, 0, :, here] for ref in near], axis=0)
        values = jnp.concatenate([ref[0, 1, :, here] for ref in near], axis=0)
        scores = lax.dot_general(
            q_ref[:, here], keys, (((1,), (1,)), ((), ())), preferred_element_type=jnp.float32
        )
        scores = scores + bias
        top = jnp.max(scores, axis=1, keepdims=True)
        weight = jnp.exp2((scores - top) * rate)
        total = jnp.sum(weight, axis=1, keepdims=True)
        context = jnp.dot(
            weight.astype(jnp.bfloat16), values, preferred_element_type=jnp.float32
        )
        out_ref[:, here] = (context / total).astype(out_ref.dtype)


def attend(queries, pool, index, flags):
    tokens, width = queries.shape
    blocks = tokens // BLOCK
    heads = width // HEAD_DIM
    listed = index.shape[0]

    def picked(r):
        return pl.BlockSpec(
            (1, 2, BLOCK, width), lambda i, index_ref, flag_ref: (index_ref[r, i], 0, 0, 0)
        )

    return pl.pallas_call(
        functools.partial(attend_kernel, heads),
        grid_spec=pltpu.PrefetchScalarGridSpec(
            num_scalar_prefetch=2,
            grid=(blocks,),
            in_specs=[pl.BlockSpec((BLOCK, width), lambda i, a, b: (i, 0))]
            + [picked(r) for r in range(listed)],
            out_specs=pl.BlockSpec((BLOCK, width), lambda i, a, b: (i, 0)),
        ),
        out_shape=jax.ShapeDtypeStruct(queries.shape, jnp.bfloat16),
        compiler_params=pltpu.CompilerParams(dimension_semantics=("arbitrary",)),
        cost_estimate=pl.CostEstimate(
            flops=60 * tokens * width * 8 * BLOCK,
            bytes_accessed=blocks * 14 * BLOCK * width * 2,
            transcendentals=tokens * heads * 8 * BLOCK,
        ),
    )(index, flags, queries, *([pool] * listed))


def merged(left, right):
    joint = jnp.maximum(left[0], right[0])
    a, b = jnp.exp(left[0] - joint), jnp.exp(right[0] - joint)
    return (
        joint,
        left[1] * a + right[1] * b,
        left[2] * a[:, :, None] + right[2] * b[:, :, None],
    )


def partial_softmax(query, keys, values):
    tokens, width = query.shape
    heads = width // HEAD_DIM
    query = query.reshape(tokens, heads, HEAD_DIM)
    keys, values = (a.reshape(-1, heads, HEAD_DIM) for a in (keys, values))
    scores = jnp.einsum("qhd,khd->hqk", query, keys, preferred_element_type=jnp.float32)
    scores = scores * HEAD_DIM ** (-0.5)
    row_max = jnp.max(scores, axis=2)
    weight = jnp.exp(scores - row_max[:, :, None])
    row_total = jnp.sum(weight, axis=2)
    value = jnp.einsum(
        "hqk,khd->hqd", weight.astype(jnp.bfloat16), values, preferred_element_type=jnp.float32
    )
    return row_max, row_total, value


def after(array, *others):
    return lax.optimization_barrier((array,) + others)[0]


def local_plain(queries, key_rows, value_rows, random_owner, random_local, output_weight):
    n = lax.axis_size("seq")
    me = lax.axis_index("seq")
    heads_n = lax.axis_size("head")
    h = lax.axis_index("head")
    token_count, width_here = queries.shape
    nb = token_count // BLOCK
    gb = GLOBAL // BLOCK
    heads_here = width_here // HEAD_DIM
    slot_count = max(2, 4 * nb // n)
    depth = n // PAIR
    z, x = me // PAIR, me % PAIR

    def send(array, pairs, axis="seq"):
        return jax.tree.map(lambda part: lax.ppermute(part, axis, pairs), array)

    def swapped(array, m):
        return lax.ppermute(array, "head", [(i, i ^ m) for i in range(heads_n)])

    def folded(part, pairs, here):
        packed = jnp.concatenate([part[2], part[0][:, None], part[1][:, None]], axis=1)
        got = send(packed, pairs)
        both = merged(part, (got[:, GLOBAL], got[:, GLOBAL + 1], got[:, :GLOBAL]))
        return jax.tree.map(lambda a, b: jnp.where(here, a, b), both, part)

    def finished(part):
        out = jnp.transpose(part[2] / part[1][:, :, None], (1, 0, 2))
        return out.reshape(GLOBAL, -1).astype(jnp.bfloat16)

    chunks = math.gcd(CHUNKS, heads_here)
    cw = width_here // chunks
    cuts = [slice(c * cw, (c + 1) * cw) for c in range(chunks)]
    key_blocks = key_rows.reshape(nb, BLOCK, width_here)
    value_blocks = value_rows.reshape(nb, BLOCK, width_here)
    owned = [jnp.stack([key_blocks[..., sl], value_blocks[..., sl]], axis=1) for sl in cuts]
    up = [(i, i + 1) for i in range(n - 1)]
    down = [(i + 1, i) for i in range(n - 1)]
    mates = [(i, i + 1 if i % PAIR == 0 else i - 1) for i in range(n)]
    owner_flat = random_owner.reshape(-1)
    local_flat = random_local.reshape(-1)
    request_table, slot_ids = slot_table(owner_flat, local_flat, n, slot_count)
    line_wins = n % PAIR == 0 and nb <= PAIR * slot_count
    global_ids = jnp.arange(gb, dtype=jnp.int32)
    pools, tops, last = [], [], None

    if line_wins:
        mate_owner, mate_local = send((owner_flat, local_flat), mates)
        near_query = jnp.where(me == 1, send(queries[:GLOBAL], [(0, 1)]), queries[:GLOBAL])
        befores = [send(own[-1:], up) for own in owned]
        afters = [send(own[:1], down) for own in owned]
        mate_table, _ = slot_table(mate_owner, mate_local, n, slot_count)
        fetch = slot_count + gb
        mate_table = jnp.concatenate(
            [mate_table, jnp.broadcast_to(global_ids[None], (n, gb))], axis=1
        )
        offsets = [0]
        for s in range(1, depth):
            offsets += [-s, s]
        bufs = [{0: own} for own in owned]
        for s in range(1, depth):
            upward = [(i, i + PAIR) for i in range((s - 1) * PAIR, n - PAIR)]
            downward = [(i, i - PAIR) for i in range(PAIR, n - (s - 1) * PAIR)]
            for held in bufs:
                held[-s] = send(held[1 - s], upward)
                held[s] = send(held[s - 1], downward)
        for c in range(chunks):
            crossed = []
            for d in offsets:
                holder = jnp.clip((z + d) * PAIR + x, 0, n - 1)
                asked = jnp.take(bufs[c][d], mate_table[holder], axis=0)
                good = [(i, j) for i, j in mates if 0 <= i // PAIR + d < depth]
                crossed.append(send(asked, good))
            part = None
            for s in range(depth):
                held = bufs[c][s]
                term = partial_softmax(near_query[:, cuts[c]], held[:, 0], held[:, 1])
                part = term if part is None else merged(part, term)
            tops.append(finished(folded(part, [(1, 0)], me == 0)))
            pools.append(
                jnp.concatenate(
                    [bufs[c][d] for d in offsets] + crossed + [befores[c], afters[c]], axis=0
                )
            )
        last = bufs[0][depth - 1]
        place = jnp.where(owner_flat // PAIR < z, 2 * (z - owner_flat // PAIR) - 1,
                          2 * (owner_flat // PAIR - z))
        line_total = len(offsets) * nb
        cell = jnp.where(
            owner_flat % PAIR == x,
            place * nb + local_flat,
            line_total + place * fetch + slot_ids,
        )
        root = jnp.maximum(2 * z - 1, 0)
        global_cell = global_ids + jnp.where(
            x == 0, root * nb, line_total + root * fetch + slot_count
        )
        edge = line_total + len(offsets) * fetch
    else:
        rows = jnp.stack([queries[:GLOBAL], key_rows[:GLOBAL], value_rows[:GLOBAL]])
        rows = jnp.where(me == 1, send(rows, [(0, 1)]), rows)
        for s in range(1, depth):
            got = send(rows, [((s - 1) * PAIR + q, s * PAIR + q) for q in range(PAIR)])
            rows = jnp.where(z == s, got, rows)
        part = partial_softmax(rows[0], key_rows, value_rows)
        for s in range(depth - 1, 0, -1):
            pairs = [(s * PAIR + q, (s - 1) * PAIR + q) for q in range(PAIR)]
            part = folded(part, pairs, z == s - 1)
        top = finished(folded(part, [(1, 0)], me == 0))
        wanted = lax.all_to_all(request_table, "seq", split_axis=0, concat_axis=0, tiled=True)
        for c, own in enumerate(owned):
            tops.append(top[:, cuts[c]])
            sent = jnp.take(own, wanted.reshape(-1), axis=0)
            got = lax.all_to_all(sent, "seq", split_axis=0, concat_axis=0, tiled=True)
            shared = jnp.stack(
                [rows[i][:, cuts[c]].reshape(gb, BLOCK, cw) for i in (1, 2)], axis=1
            )
            edges = [send(own[-1:], up), send(own[:1], down)]
            pools.append(jnp.concatenate([own, got, shared] + edges, axis=0))
        cell = nb + owner_flat * slot_count + slot_ids
        global_cell = nb + n * slot_count + global_ids
        edge = nb + n * slot_count + gb

    weights, order, bit = [output_weight], [0], heads_n
    while bit > 1:
        bit //= 2
        for m in list(order):
            held = weights[order.index(m)]
            if m and last is not None:
                held = after(held, last)
            weights.append(swapped(held, bit))
            order.append(m ^ bit)

    steps = jnp.arange(nb, dtype=jnp.int32)
    cell = cell.reshape(nb, RANDOM)
    index = jnp.stack(
        [
            jnp.where(steps == 0, edge, steps - 1),
            steps,
            jnp.where(steps == nb - 1, edge + 1, steps + 1),
        ]
        + [cell[:, r] for r in range(RANDOM)]
        + [jnp.broadcast_to(global_cell[g], (nb,)) for g in range(gb)]
    ).astype(jnp.int32)
    numbers = me * nb + steps
    flags = jnp.stack([numbers == 0, numbers == n * nb - 1]).astype(jnp.int32)

    share = token_count // heads_n
    pieces = [[] for _ in order]
    for c, sl in enumerate(cuts):
        sparse = attend(queries[:, sl], pools[c], index, flags)
        top = jnp.where(me == 0, tops[c], sparse[:GLOBAL])
        sparse = jnp.concatenate([top, sparse[GLOBAL:]], axis=0)
        for k, m in enumerate(order):
            piece = lax.dynamic_slice_in_dim(sparse, (h ^ m) * share, share, 0)
            pieces[k].append(piece if m == 0 else swapped(piece, m))
    total = None
    for k in range(len(order)):
        term = jnp.dot(
            jnp.concatenate(pieces[k], axis=1), weights[k], preferred_element_type=jnp.float32
        )
        total = term if total is None else total + term
    return total.astype(jnp.bfloat16)


MESH = pl.DeviceIdType.MESH
RATE = HEAD_DIM ** (-0.5) * math.log2(math.e)
NT = (((1,), (1,)), ((), ()))


def attend_group(items):
    scores = [
        lax.dot_general(query, keys, NT, preferred_element_type=jnp.float32)
        for query, keys, _, _ in items
    ]
    scores = [a if item[3] is None else a + item[3] for a, item in zip(scores, items)]
    tops = [jnp.max(a, axis=1, keepdims=True) for a in scores]
    parts = [jnp.exp2((a - top) * RATE) for a, top in zip(scores, tops)]
    totals = [jnp.sum(a, axis=1, keepdims=True) for a in parts]
    accs = [
        jnp.dot(a.astype(jnp.bfloat16), item[2], preferred_element_type=jnp.float32)
        for a, item in zip(parts, items)
    ]
    return [
        (acc * (1.0 / total), top * RATE + jnp.log2(total))
        for acc, total, top in zip(accs, totals, tops)
    ]


def attend_all(query, k_ref, v_ref, step):
    rows = query.shape[0]
    cells = k_ref.shape[0]

    def chunk(c):
        keys = k_ref[pl.ds(c * step, step)].reshape(step * BLOCK, HEAD_DIM)
        values = v_ref[pl.ds(c * step, step)].reshape(step * BLOCK, HEAD_DIM)
        return query, keys, values, None

    def body(c, carry):
        for part in attend_group([chunk(2 * c), chunk(2 * c + 1)]):
            carry = joined(*carry, *part)
        return carry

    start = (
        jnp.zeros((rows, HEAD_DIM), jnp.float32),
        jnp.full((rows, 1), masked_score, jnp.float32),
    )
    return lax.fori_loop(0, cells // (2 * step), body, start)


def joined(o1, l1, o2, l2):
    top = jnp.maximum(l1, l2)
    a, b = jnp.exp2(l1 - top), jnp.exp2(l2 - top)
    total = a + b
    return (o1 * a + o2 * b) / total, top + jnp.log2(total)


def hub_kernel(heads, nb, picks, codes, q_hbm, k_hbm, v_hbm, w_hbm, out_ref, w_all, *rest):
    kcol, vcol = rest[:heads], rest[heads:2 * heads]
    (qown, qend, qmate, kwin, vwin, rsend, rrecv, ssend, srecv, esend, estat, loc, lstat, tmp,
     attn, attn_all, acc, wbuf, own_sem, col_sem, m1_s, m1_r, fw_s, fw_r,
     hb_s, hb_r, re_s, re_r, er_s, er_r, at_s, at_r, w_s, w_r, wl_sem, lc_sem,
     landed_codes, codes_s, cell_ref, bias_ref, cd_s, cd_r, cd_sem, p_in, p_s, p_r) = rest[2 * heads:]
    me = lax.axis_index("seq")
    h = lax.axis_index("head")
    n = lax.axis_size("seq")
    heads_n = lax.axis_size("head")
    z, x = me // PAIR, me % PAIR
    hub = jnp.logical_or(z == 1, z == 2)
    end = jnp.logical_not(hub)
    own_end = jnp.where(z == 1, 0, 3)
    partner = jnp.where(hub, jnp.where(z == 1, 0, 3), jnp.where(z == 0, 1, 2)) * PAIR + x
    other = (3 - z) * PAIR + x
    mate = z * PAIR + (1 - x)
    wide = HEAD_DIM
    columns = acc.shape[1]
    lanes = lambda i: slice(i * wide, (i + 1) * wide)
    finish = []

    def remote(src, dst, ss, rs, seq, head=None):
        return pltpu.make_async_remote_copy(
            src_ref=src, dst_ref=dst, send_sem=ss, recv_sem=rs,
            device_id=(seq, h if head is None else head), device_id_type=MESH,
        )

    def planes(p):
        return pl.ds(p * nb, nb)

    def m1(i):
        return [
            remote(k_hbm.at[:, :, lanes(i)], kcol[i].at[planes(z)], m1_s.at[i, 0], m1_r.at[i, 0], partner),
            remote(v_hbm.at[:, :, lanes(i)], vcol[i].at[planes(z)], m1_s.at[i, 1], m1_r.at[i, 1], partner),
            remote(q_hbm.at[:, :, lanes(i)], qend.at[i], m1_s.at[i, 2], m1_r.at[i, 2], partner),
        ]

    def forward(i):
        return [
            remote(kcol[i].at[planes(own_end)], kcol[i].at[planes(own_end)], fw_s.at[i, 0], fw_r.at[i, 0], other),
            remote(vcol[i].at[planes(own_end)], vcol[i].at[planes(own_end)], fw_s.at[i, 1], fw_r.at[i, 1], other),
            remote(qend.at[i], qmate.at[i, pl.ds(nb, nb)], fw_s.at[i, 2], fw_r.at[i, 2], mate),
        ]

    def first(i):
        return [
            remote(k_hbm.at[:, :, lanes(i)], kcol[i].at[planes(z)], hb_s.at[i, 0], hb_r.at[i, 0], other),
            remote(v_hbm.at[:, :, lanes(i)], vcol[i].at[planes(z)], hb_s.at[i, 1], hb_r.at[i, 1], other),
            remote(q_hbm.at[:, :, lanes(i)], qmate.at[i, pl.ds(0, nb)], hb_s.at[i, 2], hb_r.at[i, 2], mate),
        ]

    def results(i, j):
        to = (mate, own_end * PAIR + 1 - x)[j]
        return [
            remote(part.at[i, j], into.at[i, j], re_s.at[i, j, k], re_r.at[i, j, k], to)
            for k, (part, into) in enumerate(((rsend, rrecv), (ssend, srecv)))
        ]

    def ended(i):
        return [
            remote(esend.at[i], rrecv.at[i, 0], er_s.at[i, 0], er_r.at[i, 0], partner),
            remote(estat.at[i], srecv.at[i, 0], er_s.at[i, 1], er_r.at[i, 1], partner),
        ]

    def shares(i):
        if i < EARLY:
            return [
                remote(attn.at[i, h ^ 1], attn_all.at[i, h], at_s.at[i, 0], at_r.at[i, 0], me, h ^ 1),
                remote(attn.at[i, h ^ 3], attn_all.at[i, h ^ 2], at_s.at[i, 1], at_r.at[i, 1], me, h ^ 1),
            ]
        return [
            remote(attn.at[i, h ^ k], attn_all.at[i, h], at_s.at[i, k - 1], at_r.at[i, k - 1], me, h ^ k)
            for k in range(1, heads_n)
        ]

    def kept(i):
        return [
            pltpu.make_async_copy(attn.at[i, h ^ k], attn_all.at[i, h ^ k], lc_sem.at[i, k // 2])
            for k in ((0, 2) if i < EARLY else (0,))
        ]

    def partials(part):
        half = pl.ds(part * columns // 2, columns // 2)
        return [remote(out_ref.at[:, half], p_in.at[:, half], p_s.at[part], p_r.at[part], me, h ^ 2)]

    def weights(i):
        return [
            remote(w_hbm.at[i], w_all.at[h, i], w_s.at[i, 0], w_r.at[i, 0], me, h ^ 2),
            remote(w_hbm.at[i], w_all.at[h, i], w_s.at[i, 1], w_r.at[i, 1], me, h ^ 1),
            remote(w_all.at[h ^ 2, i], w_all.at[h ^ 2, i], w_s.at[i, 2], w_r.at[i, 2], me, h ^ 1),
        ]

    def own_copies():
        return [
            pltpu.make_async_copy(q_hbm, qown, own_sem.at[0]),
            pltpu.make_async_copy(k_hbm, kwin.at[pl.ds(1, nb)], own_sem.at[1]),
            pltpu.make_async_copy(v_hbm, vwin.at[pl.ds(1, nb)], own_sem.at[2]),
        ]

    def column(i):
        return [
            pltpu.make_async_copy(k_hbm.at[:, :, lanes(i)], kcol[i].at[planes(z)], col_sem.at[i, 0]),
            pltpu.make_async_copy(v_hbm.at[:, :, lanes(i)], vcol[i].at[planes(z)], col_sem.at[i, 1]),
        ]

    def start(copies):
        for copy in copies:
            copy.start()

    def landed(copies):
        for copy in copies:
            copy.wait_recv()

    def sent(copies):
        for copy in copies:
            copy.wait_send()

    def pump(i):
        coming = m1(i)
        landed(coming[:2])
        start(forward(i)[:2])
        coming[2].wait_recv()
        start(forward(i)[2:])
        if i + 1 < heads:
            start(first(i + 1))

    def code_copies():
        hub_of = jnp.where(hub, z, jnp.where(z == 0, 1, 2)) * PAIR
        return [
            remote(codes, landed_codes.at[0], cd_s.at[0], cd_r.at[0], hub_of + x),
            remote(codes, landed_codes.at[1], cd_s.at[1], cd_r.at[1], mate),
            remote(codes, landed_codes.at[2], cd_s.at[2], cd_r.at[2], hub_of + 1 - x),
        ]

    to_hub, to_mate, to_other = code_copies()

    @pl.when(end)
    def _():
        start([to_hub, to_other])
        start(m1(0))

    @pl.when(hub)
    def _():
        start([to_mate])
        start(first(0))

    for copy in own_copies():
        copy.start()
    own_code = pltpu.make_async_copy(codes, codes_s.at[0], cd_sem.at[0])
    own_code.start()

    @pl.when(end)
    def _():
        for i in range(1, heads):
            start(m1(i))

    @pl.when(hub)
    def _():
        for i in range(heads):
            start(column(i))

    for i in range(EARLY, heads):
        weights(i)[0].start()
    for i in range(heads):
        weights(i)[1].start()

    for spot in (0, nb + 1):
        kwin[spot] = jnp.zeros(kwin.shape[1:], kwin.dtype)
        vwin[spot] = jnp.zeros(vwin.shape[1:], vwin.dtype)

    own_code.wait()

    @pl.when(hub)
    def _():
        landed([to_hub, to_mate, to_other])
        for j in range(3):
            pltpu.make_async_copy(landed_codes.at[j], codes_s.at[1 + j], cd_sem.at[1 + j]).start()
        for j in range(3):
            pltpu.make_async_copy(landed_codes.at[j], codes_s.at[1 + j], cd_sem.at[1 + j]).wait()
        for j in range(4):
            def fill(b, _):
                for r in range(RANDOM):
                    here = codes_s[j, 1, b * RANDOM + r] == x
                    spot = (j * nb + b) * picks + r
                    cell_ref[spot] = jnp.where(here, codes_s[j, 0, b * RANDOM + r], 0)
                    bias_ref[spot] = jnp.where(here, 0.0, masked_score)
                for r in range(RANDOM, picks - 1):
                    spot = (j * nb + b) * picks + r
                    cell_ref[spot] = r - RANDOM
                    bias_ref[spot] = jnp.where(x == 0, 0.0, masked_score)
                home = jnp.where(j % 2 == 0, z, own_end) * PAIR + jnp.where(j < 2, x, 1 - x)
                beside = jnp.where(b == 0, home - 1, home + 1)
                known = jnp.logical_and(beside >= 0, beside < n)
                known = jnp.logical_and(known, jnp.logical_or(b == 0, b == nb - 1))
                spot = (j * nb + b) * picks + picks - 1
                cell_ref[spot] = jnp.where(known, beside // PAIR * nb + jnp.where(b == 0, nb - 1, 0), 0)
                bias_ref[spot] = jnp.where(known, 0.0, masked_score)
                return _

            lax.fori_loop(0, nb, fill, 0)

    for copy in own_copies():
        copy.wait()

    row = lax.broadcasted_iota(jnp.int32, (1, 3 * BLOCK), 1) // BLOCK
    lane = lax.broadcasted_iota(jnp.int32, (BLOCK, 128), 1)
    pick_row = lax.broadcasted_iota(jnp.int32, (1, picks * BLOCK), 1) // BLOCK

    def stat(i, value, table):
        return jnp.where(lane == i, value, table)

    def read_stat(i, table):
        return jnp.sum(jnp.where(lane == i, table, 0.0), axis=1, keepdims=True)

    def window_bias(b):
        gone = jnp.logical_or(
            jnp.logical_and(row == 0, b == 0), jnp.logical_and(row == 2, b == nb - 1)
        )
        return jnp.where(gone, masked_score, 0.0).astype(jnp.float32)

    def listed(i, number, count):
        cells = [cell_ref[number * picks + r] for r in range(count)]
        keys = [kcol[i][cell] for cell in cells]
        values = [vcol[i][cell] for cell in cells]
        bias = jnp.full((1, count * BLOCK), bias_ref[number * picks], jnp.float32)
        for r in range(1, count):
            bias = jnp.where(pick_row[:, :count * BLOCK] == r, bias_ref[number * picks + r], bias)
        return keys, values, bias

    def window(i, b):
        keys = [kwin[b + s, :, lanes(i)] for s in range(3)]
        values = [vwin[b + s, :, lanes(i)] for s in range(3)]
        return keys, values, window_bias(b)

    def item(query, lists):
        keys = jnp.concatenate([k for part in lists for k in part[0]], axis=0)
        values = jnp.concatenate([v for part in lists for v in part[1]], axis=0)
        bias = jnp.concatenate([part[2] for part in lists], axis=1) if len(lists) > 1 else lists[0][2]
        return query, keys, values, bias

    def looped(count, unroll, body, table):
        def step(j, table):
            return body([j * unroll + u for u in range(unroll)], table)

        return lax.fori_loop(0, count // unroll, step, table)

    def attend_loop(unroll, item_of, store, base, table, lse_of=None):
        def body(blocks, table):
            done = attend_group([item_of(b) for b in blocks])
            for b, (out, lse) in zip(blocks, done):
                store(b, out)
                table = stat(base + b, lse if lse_of is None else lse_of(b, lse), table)
            return table

        return looped(nb, unroll, body, table)

    def global_rows(i, query_of, store, table, base):
        query = jnp.concatenate([query_of(g) for g in range(GLOBAL // BLOCK)], axis=0)
        out, lse = attend_all(query, kcol[i], vcol[i], 8)
        for g in range(GLOBAL // BLOCK):
            part = slice(g * BLOCK, (g + 1) * BLOCK)
            store(g, out[part])
            table[...] = stat(base + g, lse[part], table[...])

    def packed(table):
        return jnp.transpose(table)[:nb]

    def unpacked(rows):
        wide_rows = jnp.concatenate([rows, jnp.zeros((128 - nb, BLOCK), jnp.float32)], axis=0)
        return jnp.transpose(wide_rows)

    blank = jnp.zeros((BLOCK, 128), jnp.float32)

    def compute_hub(i):
        landed(forward(i))
        landed(first(i))
        for copy in column(i):
            copy.wait()

        def to_mate_set(j):
            def put_mate(b, out):
                rsend[i, j, b] = out.astype(jnp.bfloat16)

            tmp[...] = attend_loop(
                UNROLL, lambda b: item(qmate[i, j * nb + b], [listed(i, (2 + j) * nb + b, picks)]),
                put_mate, 0, blank,
            )
            if j == 1:
                @pl.when(jnp.logical_and(z == 1, x == 1))
                def _():
                    global_rows(i, lambda g: qmate[i, nb + g], put_mate, tmp, 0)

            ssend[i, j] = packed(tmp[...])
            start(results(i, j))

        def put_end(b, out):
            esend[i, b] = out.astype(jnp.bfloat16)

        to_mate_set(1)
        tmp[...] = attend_loop(
            UNROLL, lambda b: item(qend[i, b], [listed(i, nb + b, picks - 1)]), put_end, 0, blank
        )

        @pl.when(jnp.logical_and(z == 1, x == 0))
        def _():
            global_rows(i, lambda g: qend[i, g], put_end, tmp, 0)

        estat[i] = packed(tmp[...])
        start(ended(i))
        to_mate_set(0)

        def put_own(b, out):
            loc[i % 2, b] = out

        lstat[i % 2] = attend_loop(
            UNROLL // 2, lambda b: item(qown[b, :, lanes(i)], [window(i, b), listed(i, b, picks - 1)]),
            put_own, 0, blank,
        )

    def compute_end(i):
        def put_own(b, out):
            loc[i % 2, b] = out

        def lse_of(b, lse):
            replaced = jnp.logical_and(me == 0, b < GLOBAL // BLOCK)
            return jnp.where(replaced, masked_score, lse)

        lstat[i % 2] = attend_loop(
            UNROLL, lambda b: item(qown[b, :, lanes(i)], [window(i, b)]), put_own, 0, blank, lse_of
        )

    def put_attn(i, b, value):
        per = nb // heads_n
        attn[i, b // per, pl.ds(pl.multiple_of((b % per) * BLOCK, BLOCK), BLOCK)] = value.astype(jnp.bfloat16)

    def merge_own(i, count):
        ours = lstat[i % 2]
        theirs = [unpacked(srecv[i, j]) for j in range(count)]

        def body(blocks, _):
            done = [(loc[i % 2, b], read_stat(b, ours)) for b in blocks]
            for j in range(count):
                done = [
                    joined(*part, rrecv[i, j, b].astype(jnp.float32), read_stat(b, theirs[j]))
                    for part, b in zip(done, blocks)
                ]
            for b, (out, _lse) in zip(blocks, done):
                put_attn(i, b, out)
            return _

        looped(nb, UNROLL, body, 0)

    def merge_hub(i):
        landed(results(i, 0))
        merge_own(i, 1)

    def merge_end(i):
        landed(results(i, 1))
        landed(ended(i))
        merge_own(i, 2)

    def share(i):
        start(shares(i))
        start(kept(i))

    def load_weights(i):
        copies = []
        for k in range(heads_n):
            source = (w_hbm.at[i] if k == 0 else w_all.at[h ^ k, i])
            target = wbuf.at[i % 2, pl.ds((h ^ k) * wide, wide)]
            copies.append(pltpu.make_async_copy(source, target, wl_sem.at[i % 2, k]))
        return copies

    def load_early():
        copies = []
        for i in range(EARLY):
            for k in range(2):
                source = (w_hbm.at[i] if k == 0 else w_all.at[h ^ k, i])
                spot = i % 2 * 2 + k
                target = wbuf.at[i // 2, pl.ds(spot * wide, wide)]
                copies.append(pltpu.make_async_copy(source, target, wl_sem.at[i // 2, spot]))
        return copies

    def settled(i):
        landed(shares(i))
        for copy in kept(i):
            copy.wait()

    def tiles(first, last, body):
        def step(c, _):
            body(pl.ds(pl.multiple_of(c * TILE, TILE), TILE))
            return _

        lax.fori_loop(first // TILE, last // TILE, step, 0)

    def project_early(part):
        if part == 0:
            for i in range(EARLY):
                settled(i)
            for copy in load_early():
                copy.wait()
        both = []
        for k in (0, 2):
            sides = [attn_all[i, h ^ k ^ c] for i in range(EARLY) for c in range(2)]
            both.append([jnp.concatenate(sides[s:s + 4], axis=1) for s in range(0, len(sides), 4)])

        def body(here):
            own, away = [
                sum(
                    jnp.dot(left, wbuf[s, :left.shape[1], here], preferred_element_type=jnp.float32)
                    for s, left in enumerate(lefts)
                )
                for lefts in both
            ]
            acc[:, here] = own
            out_ref[:, here] = away.astype(jnp.bfloat16)

        tiles(part * columns // 2, (part + 1) * columns // 2, body)
        start(partials(part))

    def project(i):
        settled(i)
        for copy in load_weights(i):
            copy.wait()
        left = jnp.concatenate([attn_all[i, g] for g in range(heads_n)], axis=1)

        def body(here):
            term = jnp.dot(left, wbuf[i % 2, :, here], preferred_element_type=jnp.float32)
            term = term + acc[:, here]
            if i < heads - 1:
                acc[:, here] = term
            else:
                term = term + p_in[:, here].astype(jnp.float32)
                out_ref[:, here] = term.astype(jnp.bfloat16)

        tiles(0, columns, body)

    @pl.when(hub)
    def _():
        pump(0)
        pump(1)

    def fetch(i):
        landed(weights(i)[1:])
        for copy in load_weights(i):
            copy.start()

    def relay(i):
        weights(i)[0].wait_recv()
        weights(i)[2].start()

    def merge(i):
        @pl.when(hub)
        def _():
            merge_hub(i)

        @pl.when(end)
        def _():
            merge_end(i)

    for t in range(heads):
        if t == EARLY:
            for i in range(EARLY):
                weights(i)[1].wait_recv()
            for copy in load_early():
                copy.start()
        if t - 2 >= EARLY:
            fetch(t - 2)
        if t >= 1:
            merge(t - 1)
            share(t - 1)
        if EARLY <= t + 1 < heads:
            relay(t + 1)
        if t - 2 >= EARLY:
            project(t - 2)

        @pl.when(hub)
        def _():
            compute_hub(t)
            if t + 2 < heads:
                pump(t + 2)

        @pl.when(end)
        def _():
            compute_end(t)

        if 0 <= t - EARLY < 2:
            project_early(t - EARLY)

    fetch(heads - 2)
    fetch(heads - 1)
    project(heads - 2)
    merge(heads - 1)
    share(heads - 1)
    for part in range(2):
        sent(partials(part))
        landed(partials(part))
    project(heads - 1)

    @pl.when(end)
    def _():
        sent([to_hub, to_other])

    @pl.when(hub)
    def _():
        sent([to_mate])

    for i in range(heads):
        @pl.when(end)
        def _():
            sent(m1(i))

        @pl.when(hub)
        def _():
            sent(forward(i))
            sent(first(i))
            sent(results(i, 0))
            sent(results(i, 1))
            sent(ended(i))

        sent(shares(i))
        sent(weights(i)[1:2] if i < EARLY else weights(i))


UNROLL = 4
EARLY = 3
TILE = 512


def hub_attention(codes, q, k, v, w, picks):
    nb, _, width = q.shape
    heads, wide, columns = w.shape
    heads_n = lax.axis_size("head")
    planes = lax.axis_size("seq") // PAIR
    rows = nb * BLOCK
    share = rows // heads_n
    bf, f32 = jnp.bfloat16, jnp.float32
    dma = pltpu.SemaphoreType.DMA
    col = [pltpu.VMEM((planes * nb, BLOCK, wide), bf)] * (2 * heads)
    scratch = col + [
        pltpu.VMEM((nb, BLOCK, width), bf),
        pltpu.VMEM((heads, nb, BLOCK, wide), bf),
        pltpu.VMEM((heads, 2 * nb, BLOCK, wide), bf),
        pltpu.VMEM((nb + 2, BLOCK, width), bf),
        pltpu.VMEM((nb + 2, BLOCK, width), bf),
        pltpu.VMEM((heads, 2, nb, BLOCK, wide), bf),
        pltpu.VMEM((heads, 2, nb, BLOCK, wide), bf),
        pltpu.VMEM((heads, 2, nb, BLOCK), f32),
        pltpu.VMEM((heads, 2, nb, BLOCK), f32),
        pltpu.VMEM((heads, nb, BLOCK, wide), bf),
        pltpu.VMEM((heads, nb, BLOCK), f32),
        pltpu.VMEM((2, nb, BLOCK, wide), f32),
        pltpu.VMEM((2, BLOCK, 128), f32),
        pltpu.VMEM((BLOCK, 128), f32),
        pltpu.VMEM((heads, heads_n, share, wide), bf),
        pltpu.VMEM((heads, heads_n, share, wide), bf),
        pltpu.VMEM((share, columns), f32),
        pltpu.VMEM((2, heads_n * wide, columns), bf),
        dma((3,)), dma((heads, 2)),
        dma((heads, 3)), dma((heads, 3)), dma((heads, 3)), dma((heads, 3)),
        dma((heads, 3)), dma((heads, 3)), dma((heads, 2, 2)), dma((heads, 2, 2)),
        dma((heads, 2)), dma((heads, 2)), dma((heads, 3)), dma((heads, 3)),
        dma((heads, 3)), dma((heads, 3)), dma((2, heads_n)), dma((heads, 2)),
        pltpu.VMEM((3,) + codes.shape, jnp.int32), pltpu.SMEM((4,) + codes.shape, jnp.int32),
        pltpu.SMEM((4 * nb * picks,), jnp.int32), pltpu.SMEM((4 * nb * picks,), f32),
        dma((3,)), dma((3,)), dma((4,)),
        pltpu.VMEM((share, columns), bf), dma((2,)), dma((2,)),
    ]
    anywhere = pl.BlockSpec(memory_space=pl.ANY)
    out, _ = pl.pallas_call(
        functools.partial(hub_kernel, heads, nb, picks),
        out_shape=(
            jax.ShapeDtypeStruct((share, columns), bf),
            jax.ShapeDtypeStruct((heads_n,) + w.shape, bf),
        ),
        in_specs=[anywhere] * 5,
        out_specs=(pl.BlockSpec(memory_space=pltpu.VMEM), anywhere),
        scratch_shapes=scratch,
        compiler_params=pltpu.CompilerParams(
            has_side_effects=True, vmem_limit_bytes=67043328
        ),
    )(codes, q, k, v, w)
    return out


def local_hub(queries, key_rows, value_rows, random_owner, random_local, output_weight):
    rows, width = queries.shape
    nb = rows // BLOCK
    heads = width // HEAD_DIM
    cell = random_owner // PAIR * nb + random_local
    codes = jnp.stack([cell.reshape(-1), (random_owner % PAIR).reshape(-1)])
    codes = jnp.pad(codes, ((0, 6), (0, 128 - codes.shape[1])))
    blocks = lambda a: a.reshape(nb, BLOCK, width)
    return hub_attention(
        codes, blocks(queries), blocks(key_rows), blocks(value_rows),
        output_weight.reshape(heads, HEAD_DIM, -1), RANDOM + GLOBAL // BLOCK + 1,
    )


def local(queries, *others):
    n, heads_n = lax.axis_size("seq"), lax.axis_size("head")
    if n == 4 * PAIR and heads_n == 4:
        return local_hub(queries, *others)
    return local_plain(queries, *others)


def solution(mesh):
    in_specs = (
        P("seq", "head"),
        P("seq", "head"),
        P("seq", "head"),
        P("seq", None),
        P("seq", None),
        P("head", None),
    )
    out_specs = P(("seq", "head"), None)
    return jax.shard_map(local, mesh=mesh, in_specs=in_specs, out_specs=out_specs, check_vma=False)
```

```python
import functools
import math

import jax
import jax.numpy as jnp
from jax import lax
from jax.experimental import pallas as pl
from jax.experimental.pallas import tpu as pltpu
from jax.sharding import PartitionSpec as P

HEAD_DIM = 128
BLOCK = 64
RANDOM = 3
GLOBAL = 128
CHUNKS = 2
PAIR = 2


masked_score = -1e30


def slot_table(owner_ids, local_ids, seq_count, slot_count):
    owner_hits = (owner_ids[:, None] == jnp.arange(seq_count, dtype=jnp.int32)[None, :]).astype(
        jnp.int32
    )
    earlier = jnp.cumsum(owner_hits, axis=0) - owner_hits
    slot_ids = jnp.sum(earlier * owner_hits, axis=1)
    slot_hits = (slot_ids[:, None] == jnp.arange(slot_count, dtype=jnp.int32)[None, :]).astype(
        jnp.int32
    )
    request_table = jnp.sum(
        (owner_hits * local_ids[:, None])[:, :, None] * slot_hits[:, None, :], axis=0
    )
    return (request_table, slot_ids)


def attend_kernel(heads, index_ref, flag_ref, q_ref, *refs):
    near, out_ref = refs[:-1], refs[-1]
    step = pl.program_id(0)
    rate = HEAD_DIM ** (-0.5) * math.log2(math.e)
    first, last = flag_ref[0, step], flag_ref[1, step]
    listed = len(near) * BLOCK
    column = lax.broadcasted_iota(jnp.int32, (1, listed), 1) // BLOCK
    hidden = jnp.logical_or(
        jnp.logical_and(column == 0, first == 1), jnp.logical_and(column == 2, last == 1)
    )
    bias = jnp.where(hidden, masked_score, 0.0).astype(jnp.float32)
    for head in range(heads):
        here = pl.ds(head * HEAD_DIM, HEAD_DIM)
        keys = jnp.concatenate([ref[0, 0, :, here] for ref in near], axis=0)
        values = jnp.concatenate([ref[0, 1, :, here] for ref in near], axis=0)
        scores = lax.dot_general(
            q_ref[:, here], keys, (((1,), (1,)), ((), ())), preferred_element_type=jnp.float32
        )
        scores = scores + bias
        top = jnp.max(scores, axis=1, keepdims=True)
        weight = jnp.exp2((scores - top) * rate)
        total = jnp.sum(weight, axis=1, keepdims=True)
        context = jnp.dot(
            weight.astype(jnp.bfloat16), values, preferred_element_type=jnp.float32
        )
        out_ref[:, here] = (context / total).astype(out_ref.dtype)


def attend(queries, pool, index, flags):
    tokens, width = queries.shape
    blocks = tokens // BLOCK
    heads = width // HEAD_DIM
    listed = index.shape[0]

    def picked(r):
        return pl.BlockSpec(
            (1, 2, BLOCK, width), lambda i, index_ref, flag_ref: (index_ref[r, i], 0, 0, 0)
        )

    return pl.pallas_call(
        functools.partial(attend_kernel, heads),
        grid_spec=pltpu.PrefetchScalarGridSpec(
            num_scalar_prefetch=2,
            grid=(blocks,),
            in_specs=[pl.BlockSpec((BLOCK, width), lambda i, a, b: (i, 0))]
            + [picked(r) for r in range(listed)],
            out_specs=pl.BlockSpec((BLOCK, width), lambda i, a, b: (i, 0)),
        ),
        out_shape=jax.ShapeDtypeStruct(queries.shape, jnp.bfloat16),
        compiler_params=pltpu.CompilerParams(dimension_semantics=("arbitrary",)),
        cost_estimate=pl.CostEstimate(
            flops=60 * tokens * width * 8 * BLOCK,
            bytes_accessed=blocks * 14 * BLOCK * width * 2,
            transcendentals=tokens * heads * 8 * BLOCK,
        ),
    )(index, flags, queries, *([pool] * listed))


def merged(left, right):
    joint = jnp.maximum(left[0], right[0])
    a, b = jnp.exp(left[0] - joint), jnp.exp(right[0] - joint)
    return (
        joint,
        left[1] * a + right[1] * b,
        left[2] * a[:, :, None] + right[2] * b[:, :, None],
    )


def partial_softmax(query, keys, values):
    tokens, width = query.shape
    heads = width // HEAD_DIM
    query = query.reshape(tokens, heads, HEAD_DIM)
    keys, values = (a.reshape(-1, heads, HEAD_DIM) for a in (keys, values))
    scores = jnp.einsum("qhd,khd->hqk", query, keys, preferred_element_type=jnp.float32)
    scores = scores * HEAD_DIM ** (-0.5)
    row_max = jnp.max(scores, axis=2)
    weight = jnp.exp(scores - row_max[:, :, None])
    row_total = jnp.sum(weight, axis=2)
    value = jnp.einsum(
        "hqk,khd->hqd", weight.astype(jnp.bfloat16), values, preferred_element_type=jnp.float32
    )
    return row_max, row_total, value


def after(array, *others):
    return lax.optimization_barrier((array,) + others)[0]


def local_plain(queries, key_rows, value_rows, random_owner, random_local, output_weight):
    n = lax.axis_size("seq")
    me = lax.axis_index("seq")
    heads_n = lax.axis_size("head")
    h = lax.axis_index("head")
    token_count, width_here = queries.shape
    nb = token_count // BLOCK
    gb = GLOBAL // BLOCK
    heads_here = width_here // HEAD_DIM
    slot_count = max(2, 4 * nb // n)
    depth = n // PAIR
    z, x = me // PAIR, me % PAIR

    def send(array, pairs, axis="seq"):
        return jax.tree.map(lambda part: lax.ppermute(part, axis, pairs), array)

    def swapped(array, m):
        return lax.ppermute(array, "head", [(i, i ^ m) for i in range(heads_n)])

    def folded(part, pairs, here):
        packed = jnp.concatenate([part[2], part[0][:, None], part[1][:, None]], axis=1)
        got = send(packed, pairs)
        both = merged(part, (got[:, GLOBAL], got[:, GLOBAL + 1], got[:, :GLOBAL]))
        return jax.tree.map(lambda a, b: jnp.where(here, a, b), both, part)

    def finished(part):
        out = jnp.transpose(part[2] / part[1][:, :, None], (1, 0, 2))
        return out.reshape(GLOBAL, -1).astype(jnp.bfloat16)

    chunks = math.gcd(CHUNKS, heads_here)
    cw = width_here // chunks
    cuts = [slice(c * cw, (c + 1) * cw) for c in range(chunks)]
    key_blocks = key_rows.reshape(nb, BLOCK, width_here)
    value_blocks = value_rows.reshape(nb, BLOCK, width_here)
    owned = [jnp.stack([key_blocks[..., sl], value_blocks[..., sl]], axis=1) for sl in cuts]
    up = [(i, i + 1) for i in range(n - 1)]
    down = [(i + 1, i) for i in range(n - 1)]
    mates = [(i, i + 1 if i % PAIR == 0 else i - 1) for i in range(n)]
    owner_flat = random_owner.reshape(-1)
    local_flat = random_local.reshape(-1)
    request_table, slot_ids = slot_table(owner_flat, local_flat, n, slot_count)
    line_wins = n % PAIR == 0 and nb <= PAIR * slot_count
    global_ids = jnp.arange(gb, dtype=jnp.int32)
    pools, tops, last = [], [], None

    if line_wins:
        mate_owner, mate_local = send((owner_flat, local_flat), mates)
        near_query = jnp.where(me == 1, send(queries[:GLOBAL], [(0, 1)]), queries[:GLOBAL])
        befores = [send(own[-1:], up) for own in owned]
        afters = [send(own[:1], down) for own in owned]
        mate_table, _ = slot_table(mate_owner, mate_local, n, slot_count)
        fetch = slot_count + gb
        mate_table = jnp.concatenate(
            [mate_table, jnp.broadcast_to(global_ids[None], (n, gb))], axis=1
        )
        offsets = [0]
        for s in range(1, depth):
            offsets += [-s, s]
        bufs = [{0: own} for own in owned]
        for s in range(1, depth):
            upward = [(i, i + PAIR) for i in range((s - 1) * PAIR, n - PAIR)]
            downward = [(i, i - PAIR) for i in range(PAIR, n - (s - 1) * PAIR)]
            for held in bufs:
                held[-s] = send(held[1 - s], upward)
                held[s] = send(held[s - 1], downward)
        for c in range(chunks):
            crossed = []
            for d in offsets:
                holder = jnp.clip((z + d) * PAIR + x, 0, n - 1)
                asked = jnp.take(bufs[c][d], mate_table[holder], axis=0)
                good = [(i, j) for i, j in mates if 0 <= i // PAIR + d < depth]
                crossed.append(send(asked, good))
            part = None
            for s in range(depth):
                held = bufs[c][s]
                term = partial_softmax(near_query[:, cuts[c]], held[:, 0], held[:, 1])
                part = term if part is None else merged(part, term)
            tops.append(finished(folded(part, [(1, 0)], me == 0)))
            pools.append(
                jnp.concatenate(
                    [bufs[c][d] for d in offsets] + crossed + [befores[c], afters[c]], axis=0
                )
            )
        last = bufs[0][depth - 1]
        place = jnp.where(owner_flat // PAIR < z, 2 * (z - owner_flat // PAIR) - 1,
                          2 * (owner_flat // PAIR - z))
        line_total = len(offsets) * nb
        cell = jnp.where(
            owner_flat % PAIR == x,
            place * nb + local_flat,
            line_total + place * fetch + slot_ids,
        )
        root = jnp.maximum(2 * z - 1, 0)
        global_cell = global_ids + jnp.where(
            x == 0, root * nb, line_total + root * fetch + slot_count
        )
        edge = line_total + len(offsets) * fetch
    else:
        rows = jnp.stack([queries[:GLOBAL], key_rows[:GLOBAL], value_rows[:GLOBAL]])
        rows = jnp.where(me == 1, send(rows, [(0, 1)]), rows)
        for s in range(1, depth):
            got = send(rows, [((s - 1) * PAIR + q, s * PAIR + q) for q in range(PAIR)])
            rows = jnp.where(z == s, got, rows)
        part = partial_softmax(rows[0], key_rows, value_rows)
        for s in range(depth - 1, 0, -1):
            pairs = [(s * PAIR + q, (s - 1) * PAIR + q) for q in range(PAIR)]
            part = folded(part, pairs, z == s - 1)
        top = finished(folded(part, [(1, 0)], me == 0))
        wanted = lax.all_to_all(request_table, "seq", split_axis=0, concat_axis=0, tiled=True)
        for c, own in enumerate(owned):
            tops.append(top[:, cuts[c]])
            sent = jnp.take(own, wanted.reshape(-1), axis=0)
            got = lax.all_to_all(sent, "seq", split_axis=0, concat_axis=0, tiled=True)
            shared = jnp.stack(
                [rows[i][:, cuts[c]].reshape(gb, BLOCK, cw) for i in (1, 2)], axis=1
            )
            edges = [send(own[-1:], up), send(own[:1], down)]
            pools.append(jnp.concatenate([own, got, shared] + edges, axis=0))
        cell = nb + owner_flat * slot_count + slot_ids
        global_cell = nb + n * slot_count + global_ids
        edge = nb + n * slot_count + gb

    weights, order, bit = [output_weight], [0], heads_n
    while bit > 1:
        bit //= 2
        for m in list(order):
            held = weights[order.index(m)]
            if m and last is not None:
                held = after(held, last)
            weights.append(swapped(held, bit))
            order.append(m ^ bit)

    steps = jnp.arange(nb, dtype=jnp.int32)
    cell = cell.reshape(nb, RANDOM)
    index = jnp.stack(
        [
            jnp.where(steps == 0, edge, steps - 1),
            steps,
            jnp.where(steps == nb - 1, edge + 1, steps + 1),
        ]
        + [cell[:, r] for r in range(RANDOM)]
        + [jnp.broadcast_to(global_cell[g], (nb,)) for g in range(gb)]
    ).astype(jnp.int32)
    numbers = me * nb + steps
    flags = jnp.stack([numbers == 0, numbers == n * nb - 1]).astype(jnp.int32)

    share = token_count // heads_n
    pieces = [[] for _ in order]
    for c, sl in enumerate(cuts):
        sparse = attend(queries[:, sl], pools[c], index, flags)
        top = jnp.where(me == 0, tops[c], sparse[:GLOBAL])
        sparse = jnp.concatenate([top, sparse[GLOBAL:]], axis=0)
        for k, m in enumerate(order):
            piece = lax.dynamic_slice_in_dim(sparse, (h ^ m) * share, share, 0)
            pieces[k].append(piece if m == 0 else swapped(piece, m))
    total = None
    for k in range(len(order)):
        term = jnp.dot(
            jnp.concatenate(pieces[k], axis=1), weights[k], preferred_element_type=jnp.float32
        )
        total = term if total is None else total + term
    return total.astype(jnp.bfloat16)


MESH = pl.DeviceIdType.MESH
RATE = HEAD_DIM ** (-0.5) * math.log2(math.e)
NT = (((1,), (1,)), ((), ()))


def attend_group(items):
    scores = [
        lax.dot_general(query, keys, NT, preferred_element_type=jnp.float32)
        for query, keys, _, _ in items
    ]
    scores = [a if item[3] is None else a + item[3] for a, item in zip(scores, items)]
    tops = [jnp.max(a, axis=1, keepdims=True) for a in scores]
    parts = [jnp.exp2((a - top) * RATE) for a, top in zip(scores, tops)]
    totals = [jnp.sum(a, axis=1, keepdims=True) for a in parts]
    accs = [
        jnp.dot(a.astype(jnp.bfloat16), item[2], preferred_element_type=jnp.float32)
        for a, item in zip(parts, items)
    ]
    return [
        (acc * (1.0 / total), top * RATE + jnp.log2(total))
        for acc, total, top in zip(accs, totals, tops)
    ]


def attend_all(query, k_ref, v_ref, step):
    rows = query.shape[0]
    cells = k_ref.shape[0]

    def chunk(c):
        keys = k_ref[pl.ds(c * step, step)].reshape(step * BLOCK, HEAD_DIM)
        values = v_ref[pl.ds(c * step, step)].reshape(step * BLOCK, HEAD_DIM)
        return query, keys, values, None

    def body(c, carry):
        for part in attend_group([chunk(2 * c), chunk(2 * c + 1)]):
            carry = joined(*carry, *part)
        return carry

    start = (
        jnp.zeros((rows, HEAD_DIM), jnp.float32),
        jnp.full((rows, 1), masked_score, jnp.float32),
    )
    return lax.fori_loop(0, cells // (2 * step), body, start)


def joined(o1, l1, o2, l2):
    top = jnp.maximum(l1, l2)
    a, b = jnp.exp2(l1 - top), jnp.exp2(l2 - top)
    total = a + b
    return (o1 * a + o2 * b) / total, top + jnp.log2(total)


def hub_kernel(heads, nb, picks, codes, q_hbm, k_hbm, v_hbm, w_hbm, out_ref, w_all, *rest):
    kcol, vcol = rest[:heads], rest[heads:2 * heads]
    (qown, qend, qmate, kwin, vwin, rsend, rrecv, ssend, srecv, esend, estat, loc, lstat, tmp,
     attn, attn_all, acc, wbuf, own_sem, col_sem, m1_s, m1_r, fw_s, fw_r,
     hb_s, hb_r, re_s, re_r, er_s, er_r, at_s, at_r, w_s, w_r, wl_sem, lc_sem,
     landed_codes, codes_s, cell_ref, bias_ref, cd_s, cd_r, cd_sem, p_in, p_s, p_r) = rest[2 * heads:]
    me = lax.axis_index("seq")
    h = lax.axis_index("head")
    n = lax.axis_size("seq")
    heads_n = lax.axis_size("head")
    z, x = me // PAIR, me % PAIR
    hub = jnp.logical_or(z == 1, z == 2)
    end = jnp.logical_not(hub)
    own_end = jnp.where(z == 1, 0, 3)
    partner = jnp.where(hub, jnp.where(z == 1, 0, 3), jnp.where(z == 0, 1, 2)) * PAIR + x
    other = (3 - z) * PAIR + x
    mate = z * PAIR + (1 - x)
    wide = HEAD_DIM
    columns = acc.shape[1]
    lanes = lambda i: slice(i * wide, (i + 1) * wide)
    finish = []

    def remote(src, dst, ss, rs, seq, head=None):
        return pltpu.make_async_remote_copy(
            src_ref=src, dst_ref=dst, send_sem=ss, recv_sem=rs,
            device_id=(seq, h if head is None else head), device_id_type=MESH,
        )

    def planes(p):
        return pl.ds(p * nb, nb)

    def m1(i):
        return [
            remote(k_hbm.at[:, :, lanes(i)], kcol[i].at[planes(z)], m1_s.at[i, 0], m1_r.at[i, 0], partner),
            remote(v_hbm.at[:, :, lanes(i)], vcol[i].at[planes(z)], m1_s.at[i, 1], m1_r.at[i, 1], partner),
            remote(q_hbm.at[:, :, lanes(i)], qend.at[i], m1_s.at[i, 2], m1_r.at[i, 2], partner),
        ]

    def forward(i):
        return [
            remote(kcol[i].at[planes(own_end)], kcol[i].at[planes(own_end)], fw_s.at[i, 0], fw_r.at[i, 0], other),
            remote(vcol[i].at[planes(own_end)], vcol[i].at[planes(own_end)], fw_s.at[i, 1], fw_r.at[i, 1], other),
            remote(qend.at[i], qmate.at[i, pl.ds(nb, nb)], fw_s.at[i, 2], fw_r.at[i, 2], mate),
        ]

    def first(i):
        return [
            remote(k_hbm.at[:, :, lanes(i)], kcol[i].at[planes(z)], hb_s.at[i, 0], hb_r.at[i, 0], other),
            remote(v_hbm.at[:, :, lanes(i)], vcol[i].at[planes(z)], hb_s.at[i, 1], hb_r.at[i, 1], other),
            remote(q_hbm.at[:, :, lanes(i)], qmate.at[i, pl.ds(0, nb)], hb_s.at[i, 2], hb_r.at[i, 2], mate),
        ]

    def results(i, j):
        to = (mate, own_end * PAIR + 1 - x)[j]
        return [
            remote(part.at[i, j], into.at[i, j], re_s.at[i, j, k], re_r.at[i, j, k], to)
            for k, (part, into) in enumerate(((rsend, rrecv), (ssend, srecv)))
        ]

    def ended(i):
        return [
            remote(esend.at[i], rrecv.at[i, 0], er_s.at[i, 0], er_r.at[i, 0], partner),
            remote(estat.at[i], srecv.at[i, 0], er_s.at[i, 1], er_r.at[i, 1], partner),
        ]

    def shares(i):
        if i < EARLY:
            return [
                remote(attn.at[i, h ^ 1], attn_all.at[i, h], at_s.at[i, 0], at_r.at[i, 0], me, h ^ 1),
                remote(attn.at[i, h ^ 3], attn_all.at[i, h ^ 2], at_s.at[i, 1], at_r.at[i, 1], me, h ^ 1),
            ]
        return [
            remote(attn.at[i, h ^ k], attn_all.at[i, h], at_s.at[i, k - 1], at_r.at[i, k - 1], me, h ^ k)
            for k in range(1, heads_n)
        ]

    def kept(i):
        return [
            pltpu.make_async_copy(attn.at[i, h ^ k], attn_all.at[i, h ^ k], lc_sem.at[i, k // 2])
            for k in ((0, 2) if i < EARLY else (0,))
        ]

    def partials(part):
        half = pl.ds(part * columns // 2, columns // 2)
        return [remote(out_ref.at[:, half], p_in.at[:, half], p_s.at[part], p_r.at[part], me, h ^ 2)]

    def weights(i):
        return [
            remote(w_hbm.at[i], w_all.at[h, i], w_s.at[i, 0], w_r.at[i, 0], me, h ^ 2),
            remote(w_hbm.at[i], w_all.at[h, i], w_s.at[i, 1], w_r.at[i, 1], me, h ^ 1),
            remote(w_all.at[h ^ 2, i], w_all.at[h ^ 2, i], w_s.at[i, 2], w_r.at[i, 2], me, h ^ 1),
        ]

    def own_copies():
        return [
            pltpu.make_async_copy(q_hbm, qown, own_sem.at[0]),
            pltpu.make_async_copy(k_hbm, kwin.at[pl.ds(1, nb)], own_sem.at[1]),
            pltpu.make_async_copy(v_hbm, vwin.at[pl.ds(1, nb)], own_sem.at[2]),
        ]

    def column(i):
        return [
            pltpu.make_async_copy(k_hbm.at[:, :, lanes(i)], kcol[i].at[planes(z)], col_sem.at[i, 0]),
            pltpu.make_async_copy(v_hbm.at[:, :, lanes(i)], vcol[i].at[planes(z)], col_sem.at[i, 1]),
        ]

    def start(copies):
        for copy in copies:
            copy.start()

    def landed(copies):
        for copy in copies:
            copy.wait_recv()

    def sent(copies):
        for copy in copies:
            copy.wait_send()

    def pump(i):
        coming = m1(i)
        landed(coming[:2])
        start(forward(i)[:2])
        coming[2].wait_recv()
        start(forward(i)[2:])
        if i + 1 < heads:
            start(first(i + 1))

    def code_copies():
        hub_of = jnp.where(hub, z, jnp.where(z == 0, 1, 2)) * PAIR
        return [
            remote(codes, landed_codes.at[0], cd_s.at[0], cd_r.at[0], hub_of + x),
            remote(codes, landed_codes.at[1], cd_s.at[1], cd_r.at[1], mate),
            remote(codes, landed_codes.at[2], cd_s.at[2], cd_r.at[2], hub_of + 1 - x),
        ]

    to_hub, to_mate, to_other = code_copies()

    @pl.when(end)
    def _():
        start([to_hub, to_other])
        start(m1(0))

    @pl.when(hub)
    def _():
        start([to_mate])
        start(first(0))

    for copy in own_copies():
        copy.start()
    own_code = pltpu.make_async_copy(codes, codes_s.at[0], cd_sem.at[0])
    own_code.start()

    @pl.when(end)
    def _():
        for i in range(1, heads):
            start(m1(i))

    @pl.when(hub)
    def _():
        for i in range(heads):
            start(column(i))

    for i in range(EARLY, heads):
        weights(i)[0].start()
    for i in range(heads):
        weights(i)[1].start()

    for spot in (0, nb + 1):
        kwin[spot] = jnp.zeros(kwin.shape[1:], kwin.dtype)
        vwin[spot] = jnp.zeros(vwin.shape[1:], vwin.dtype)

    own_code.wait()

    @pl.when(hub)
    def _():
        landed([to_hub, to_mate, to_other])
        for j in range(3):
            pltpu.make_async_copy(landed_codes.at[j], codes_s.at[1 + j], cd_sem.at[1 + j]).start()
        for j in range(3):
            pltpu.make_async_copy(landed_codes.at[j], codes_s.at[1 + j], cd_sem.at[1 + j]).wait()
        for j in range(4):
            def fill(b, _):
                for r in range(RANDOM):
                    here = codes_s[j, 1, b * RANDOM + r] == x
                    spot = (j * nb + b) * picks + r
                    cell_ref[spot] = jnp.where(here, codes_s[j, 0, b * RANDOM + r], 0)
                    bias_ref[spot] = jnp.where(here, 0.0, masked_score)
                for r in range(RANDOM, picks - 1):
                    spot = (j * nb + b) * picks + r
                    cell_ref[spot] = r - RANDOM
                    bias_ref[spot] = jnp.where(x == 0, 0.0, masked_score)
                home = jnp.where(j % 2 == 0, z, own_end) * PAIR + jnp.where(j < 2, x, 1 - x)
                beside = jnp.where(b == 0, home - 1, home + 1)
                known = jnp.logical_and(beside >= 0, beside < n)
                known = jnp.logical_and(known, jnp.logical_or(b == 0, b == nb - 1))
                spot = (j * nb + b) * picks + picks - 1
                cell_ref[spot] = jnp.where(known, beside // PAIR * nb + jnp.where(b == 0, nb - 1, 0), 0)
                bias_ref[spot] = jnp.where(known, 0.0, masked_score)
                return _

            lax.fori_loop(0, nb, fill, 0)

    for copy in own_copies():
        copy.wait()

    row = lax.broadcasted_iota(jnp.int32, (1, 3 * BLOCK), 1) // BLOCK
    lane = lax.broadcasted_iota(jnp.int32, (BLOCK, 128), 1)
    pick_row = lax.broadcasted_iota(jnp.int32, (1, picks * BLOCK), 1) // BLOCK

    def stat(i, value, table):
        return jnp.where(lane == i, value, table)

    def read_stat(i, table):
        return jnp.sum(jnp.where(lane == i, table, 0.0), axis=1, keepdims=True)

    def window_bias(b):
        gone = jnp.logical_or(
            jnp.logical_and(row == 0, b == 0), jnp.logical_and(row == 2, b == nb - 1)
        )
        return jnp.where(gone, masked_score, 0.0).astype(jnp.float32)

    def listed(i, number, count):
        cells = [cell_ref[number * picks + r] for r in range(count)]
        keys = [kcol[i][cell] for cell in cells]
        values = [vcol[i][cell] for cell in cells]
        bias = jnp.full((1, count * BLOCK), bias_ref[number * picks], jnp.float32)
        for r in range(1, count):
            bias = jnp.where(pick_row[:, :count * BLOCK] == r, bias_ref[number * picks + r], bias)
        return keys, values, bias

    def window(i, b):
        keys = [kwin[b + s, :, lanes(i)] for s in range(3)]
        values = [vwin[b + s, :, lanes(i)] for s in range(3)]
        return keys, values, window_bias(b)

    def item(query, lists):
        keys = jnp.concatenate([k for part in lists for k in part[0]], axis=0)
        values = jnp.concatenate([v for part in lists for v in part[1]], axis=0)
        bias = jnp.concatenate([part[2] for part in lists], axis=1) if len(lists) > 1 else lists[0][2]
        return query, keys, values, bias

    def looped(count, unroll, body, table):
        def step(j, table):
            return body([j * unroll + u for u in range(unroll)], table)

        return lax.fori_loop(0, count // unroll, step, table)

    def attend_loop(unroll, item_of, store, base, table, lse_of=None):
        def body(blocks, table):
            done = attend_group([item_of(b) for b in blocks])
            for b, (out, lse) in zip(blocks, done):
                store(b, out)
                table = stat(base + b, lse if lse_of is None else lse_of(b, lse), table)
            return table

        return looped(nb, unroll, body, table)

    def global_rows(i, query_of, store, table, base):
        query = jnp.concatenate([query_of(g) for g in range(GLOBAL // BLOCK)], axis=0)
        out, lse = attend_all(query, kcol[i], vcol[i], 8)
        for g in range(GLOBAL // BLOCK):
            part = slice(g * BLOCK, (g + 1) * BLOCK)
            store(g, out[part])
            table[...] = stat(base + g, lse[part], table[...])

    def packed(table):
        return jnp.transpose(table)[:nb]

    def unpacked(rows):
        wide_rows = jnp.concatenate([rows, jnp.zeros((128 - nb, BLOCK), jnp.float32)], axis=0)
        return jnp.transpose(wide_rows)

    blank = jnp.zeros((BLOCK, 128), jnp.float32)

    def compute_hub(i):
        landed(forward(i))
        landed(first(i))
        for copy in column(i):
            copy.wait()

        def to_mate_set(j):
            def put_mate(b, out):
                rsend[i, j, b] = out.astype(jnp.bfloat16)

            tmp[...] = attend_loop(
                UNROLL, lambda b: item(qmate[i, j * nb + b], [listed(i, (2 + j) * nb + b, picks)]),
                put_mate, 0, blank,
            )
            if j == 1:
                @pl.when(jnp.logical_and(z == 1, x == 1))
                def _():
                    global_rows(i, lambda g: qmate[i, nb + g], put_mate, tmp, 0)

            ssend[i, j] = packed(tmp[...])
            start(results(i, j))

        def put_end(b, out):
            esend[i, b] = out.astype(jnp.bfloat16)

        to_mate_set(1)
        to_mate_set(0)
        tmp[...] = attend_loop(
            UNROLL, lambda b: item(qend[i, b], [listed(i, nb + b, picks - 1)]), put_end, 0, blank
        )

        @pl.when(jnp.logical_and(z == 1, x == 0))
        def _():
            global_rows(i, lambda g: qend[i, g], put_end, tmp, 0)

        estat[i] = packed(tmp[...])
        start(ended(i))

        def put_own(b, out):
            loc[i % 2, b] = out

        lstat[i % 2] = attend_loop(
            UNROLL // 2, lambda b: item(qown[b, :, lanes(i)], [window(i, b), listed(i, b, picks - 1)]),
            put_own, 0, blank,
        )

    def compute_end(i):
        def put_own(b, out):
            loc[i % 2, b] = out

        def lse_of(b, lse):
            replaced = jnp.logical_and(me == 0, b < GLOBAL // BLOCK)
            return jnp.where(replaced, masked_score, lse)

        lstat[i % 2] = attend_loop(
            UNROLL, lambda b: item(qown[b, :, lanes(i)], [window(i, b)]), put_own, 0, blank, lse_of
        )

    def put_attn(i, b, value):
        per = nb // heads_n
        attn[i, b // per, pl.ds(pl.multiple_of((b % per) * BLOCK, BLOCK), BLOCK)] = value.astype(jnp.bfloat16)

    def merge_own(i, count):
        ours = lstat[i % 2]
        theirs = [unpacked(srecv[i, j]) for j in range(count)]

        def body(blocks, _):
            done = [(loc[i % 2, b], read_stat(b, ours)) for b in blocks]
            for j in range(count):
                done = [
                    joined(*part, rrecv[i, j, b].astype(jnp.float32), read_stat(b, theirs[j]))
                    for part, b in zip(done, blocks)
                ]
            for b, (out, _lse) in zip(blocks, done):
                put_attn(i, b, out)
            return _

        looped(nb, UNROLL, body, 0)

    def merge_hub(i):
        landed(results(i, 0))
        merge_own(i, 1)

    def merge_end(i):
        landed(results(i, 1))
        landed(ended(i))
        merge_own(i, 2)

    def share(i):
        start(shares(i))
        start(kept(i))

    def load_weights(i):
        copies = []
        for k in range(heads_n):
            source = (w_hbm.at[i] if k == 0 else w_all.at[h ^ k, i])
            target = wbuf.at[i % 2, pl.ds((h ^ k) * wide, wide)]
            copies.append(pltpu.make_async_copy(source, target, wl_sem.at[i % 2, k]))
        return copies

    def load_early():
        copies = []
        for i in range(EARLY):
            for k in range(2):
                source = (w_hbm.at[i] if k == 0 else w_all.at[h ^ k, i])
                spot = i % 2 * 2 + k
                target = wbuf.at[i // 2, pl.ds(spot * wide, wide)]
                copies.append(pltpu.make_async_copy(source, target, wl_sem.at[i // 2, spot]))
        return copies

    def settled(i):
        landed(shares(i))
        for copy in kept(i):
            copy.wait()

    def tiles(first, last, body):
        def step(c, _):
            body(pl.ds(pl.multiple_of(c * TILE, TILE), TILE))
            return _

        lax.fori_loop(first // TILE, last // TILE, step, 0)

    def project_early(part):
        if part == 0:
            for i in range(EARLY):
                settled(i)
            for copy in load_early():
                copy.wait()
        both = []
        for k in (0, 2):
            sides = [attn_all[i, h ^ k ^ c] for i in range(EARLY) for c in range(2)]
            both.append([jnp.concatenate(sides[s:s + 4], axis=1) for s in range(0, len(sides), 4)])

        def body(here):
            own, away = [
                sum(
                    jnp.dot(left, wbuf[s, :left.shape[1], here], preferred_element_type=jnp.float32)
                    for s, left in enumerate(lefts)
                )
                for lefts in both
            ]
            acc[:, here] = own
            out_ref[:, here] = away.astype(jnp.bfloat16)

        tiles(part * columns // 2, (part + 1) * columns // 2, body)
        start(partials(part))

    def project(i):
        settled(i)
        for copy in load_weights(i):
            copy.wait()
        left = jnp.concatenate([attn_all[i, g] for g in range(heads_n)], axis=1)

        def body(here):
            term = jnp.dot(left, wbuf[i % 2, :, here], preferred_element_type=jnp.float32)
            term = term + acc[:, here]
            if i < heads - 1:
                acc[:, here] = term
            else:
                term = term + p_in[:, here].astype(jnp.float32)
                out_ref[:, here] = term.astype(jnp.bfloat16)

        tiles(0, columns, body)

    @pl.when(hub)
    def _():
        pump(0)
        pump(1)

    def fetch(i):
        landed(weights(i)[1:])
        for copy in load_weights(i):
            copy.start()

    def relay(i):
        weights(i)[0].wait_recv()
        weights(i)[2].start()

    def merge(i):
        @pl.when(hub)
        def _():
            merge_hub(i)

        @pl.when(end)
        def _():
            merge_end(i)

    for t in range(heads):
        if t == EARLY:
            for i in range(EARLY):
                weights(i)[1].wait_recv()
            for copy in load_early():
                copy.start()
        if t - 2 >= EARLY:
            fetch(t - 2)
        if t >= 1:
            merge(t - 1)
            share(t - 1)
        if EARLY <= t + 1 < heads:
            relay(t + 1)
        if t - 2 >= EARLY:
            project(t - 2)

        @pl.when(hub)
        def _():
            compute_hub(t)
            if t + 2 < heads:
                pump(t + 2)

        @pl.when(end)
        def _():
            compute_end(t)

        if 0 <= t - EARLY < 2:
            project_early(t - EARLY)

    fetch(heads - 2)
    fetch(heads - 1)
    project(heads - 2)
    merge(heads - 1)
    share(heads - 1)
    for part in range(2):
        sent(partials(part))
        landed(partials(part))
    project(heads - 1)

    @pl.when(end)
    def _():
        sent([to_hub, to_other])

    @pl.when(hub)
    def _():
        sent([to_mate])

    for i in range(heads):
        @pl.when(end)
        def _():
            sent(m1(i))

        @pl.when(hub)
        def _():
            sent(forward(i))
            sent(first(i))
            sent(results(i, 0))
            sent(results(i, 1))
            sent(ended(i))

        sent(shares(i))
        sent(weights(i)[1:2] if i < EARLY else weights(i))


UNROLL = 4
EARLY = 3
TILE = 1024


def hub_attention(codes, q, k, v, w, picks):
    nb, _, width = q.shape
    heads, wide, columns = w.shape
    heads_n = lax.axis_size("head")
    planes = lax.axis_size("seq") // PAIR
    rows = nb * BLOCK
    share = rows // heads_n
    bf, f32 = jnp.bfloat16, jnp.float32
    dma = pltpu.SemaphoreType.DMA
    col = [pltpu.VMEM((planes * nb, BLOCK, wide), bf)] * (2 * heads)
    scratch = col + [
        pltpu.VMEM((nb, BLOCK, width), bf),
        pltpu.VMEM((heads, nb, BLOCK, wide), bf),
        pltpu.VMEM((heads, 2 * nb, BLOCK, wide), bf),
        pltpu.VMEM((nb + 2, BLOCK, width), bf),
        pltpu.VMEM((nb + 2, BLOCK, width), bf),
        pltpu.VMEM((heads, 2, nb, BLOCK, wide), bf),
        pltpu.VMEM((heads, 2, nb, BLOCK, wide), bf),
        pltpu.VMEM((heads, 2, nb, BLOCK), f32),
        pltpu.VMEM((heads, 2, nb, BLOCK), f32),
        pltpu.VMEM((heads, nb, BLOCK, wide), bf),
        pltpu.VMEM((heads, nb, BLOCK), f32),
        pltpu.VMEM((2, nb, BLOCK, wide), f32),
        pltpu.VMEM((2, BLOCK, 128), f32),
        pltpu.VMEM((BLOCK, 128), f32),
        pltpu.VMEM((heads, heads_n, share, wide), bf),
        pltpu.VMEM((heads, heads_n, share, wide), bf),
        pltpu.VMEM((share, columns), f32),
        pltpu.VMEM((2, heads_n * wide, columns), bf),
        dma((3,)), dma((heads, 2)),
        dma((heads, 3)), dma((heads, 3)), dma((heads, 3)), dma((heads, 3)),
        dma((heads, 3)), dma((heads, 3)), dma((heads, 2, 2)), dma((heads, 2, 2)),
        dma((heads, 2)), dma((heads, 2)), dma((heads, 3)), dma((heads, 3)),
        dma((heads, 3)), dma((heads, 3)), dma((2, heads_n)), dma((heads, 2)),
        pltpu.VMEM((3,) + codes.shape, jnp.int32), pltpu.SMEM((4,) + codes.shape, jnp.int32),
        pltpu.SMEM((4 * nb * picks,), jnp.int32), pltpu.SMEM((4 * nb * picks,), f32),
        dma((3,)), dma((3,)), dma((4,)),
        pltpu.VMEM((share, columns), bf), dma((2,)), dma((2,)),
    ]
    anywhere = pl.BlockSpec(memory_space=pl.ANY)
    out, _ = pl.pallas_call(
        functools.partial(hub_kernel, heads, nb, picks),
        out_shape=(
            jax.ShapeDtypeStruct((share, columns), bf),
            jax.ShapeDtypeStruct((heads_n,) + w.shape, bf),
        ),
        in_specs=[anywhere] * 5,
        out_specs=(pl.BlockSpec(memory_space=pltpu.VMEM), anywhere),
        scratch_shapes=scratch,
        compiler_params=pltpu.CompilerParams(
            has_side_effects=True, vmem_limit_bytes=67043328
        ),
    )(codes, q, k, v, w)
    return out


def local_hub(queries, key_rows, value_rows, random_owner, random_local, output_weight):
    rows, width = queries.shape
    nb = rows // BLOCK
    heads = width // HEAD_DIM
    cell = random_owner // PAIR * nb + random_local
    codes = jnp.stack([cell.reshape(-1), (random_owner % PAIR).reshape(-1)])
    codes = jnp.pad(codes, ((0, 6), (0, 128 - codes.shape[1])))
    blocks = lambda a: a.reshape(nb, BLOCK, width)
    return hub_attention(
        codes, blocks(queries), blocks(key_rows), blocks(value_rows),
        output_weight.reshape(heads, HEAD_DIM, -1), RANDOM + GLOBAL // BLOCK + 1,
    )


def local(queries, *others):
    n, heads_n = lax.axis_size("seq"), lax.axis_size("head")
    if n == 4 * PAIR and heads_n == 4:
        return local_hub(queries, *others)
    return local_plain(queries, *others)


def solution(mesh):
    in_specs = (
        P("seq", "head"),
        P("seq", "head"),
        P("seq", "head"),
        P("seq", None),
        P("seq", None),
        P("head", None),
    )
    out_specs = P(("seq", "head"), None)
    return jax.shard_map(local, mesh=mesh, in_specs=in_specs, out_specs=out_specs, check_vma=False)
```

```python
import functools
import math

import jax
import jax.numpy as jnp
from jax import lax
from jax.experimental import pallas as pl
from jax.experimental.pallas import tpu as pltpu
from jax.sharding import PartitionSpec as P

HEAD_DIM = 128
BLOCK = 64
RANDOM = 3
GLOBAL = 128
CHUNKS = 2
PAIR = 2


masked_score = -1e30


def slot_table(owner_ids, local_ids, seq_count, slot_count):
    owner_hits = (owner_ids[:, None] == jnp.arange(seq_count, dtype=jnp.int32)[None, :]).astype(
        jnp.int32
    )
    earlier = jnp.cumsum(owner_hits, axis=0) - owner_hits
    slot_ids = jnp.sum(earlier * owner_hits, axis=1)
    slot_hits = (slot_ids[:, None] == jnp.arange(slot_count, dtype=jnp.int32)[None, :]).astype(
        jnp.int32
    )
    request_table = jnp.sum(
        (owner_hits * local_ids[:, None])[:, :, None] * slot_hits[:, None, :], axis=0
    )
    return (request_table, slot_ids)


def attend_kernel(heads, index_ref, flag_ref, q_ref, *refs):
    near, out_ref = refs[:-1], refs[-1]
    step = pl.program_id(0)
    rate = HEAD_DIM ** (-0.5) * math.log2(math.e)
    first, last = flag_ref[0, step], flag_ref[1, step]
    listed = len(near) * BLOCK
    column = lax.broadcasted_iota(jnp.int32, (1, listed), 1) // BLOCK
    hidden = jnp.logical_or(
        jnp.logical_and(column == 0, first == 1), jnp.logical_and(column == 2, last == 1)
    )
    bias = jnp.where(hidden, masked_score, 0.0).astype(jnp.float32)
    for head in range(heads):
        here = pl.ds(head * HEAD_DIM, HEAD_DIM)
        keys = jnp.concatenate([ref[0, 0, :, here] for ref in near], axis=0)
        values = jnp.concatenate([ref[0, 1, :, here] for ref in near], axis=0)
        scores = lax.dot_general(
            q_ref[:, here], keys, (((1,), (1,)), ((), ())), preferred_element_type=jnp.float32
        )
        scores = scores + bias
        top = jnp.max(scores, axis=1, keepdims=True)
        weight = jnp.exp2((scores - top) * rate)
        total = jnp.sum(weight, axis=1, keepdims=True)
        context = jnp.dot(
            weight.astype(jnp.bfloat16), values, preferred_element_type=jnp.float32
        )
        out_ref[:, here] = (context / total).astype(out_ref.dtype)


def attend(queries, pool, index, flags):
    tokens, width = queries.shape
    blocks = tokens // BLOCK
    heads = width // HEAD_DIM
    listed = index.shape[0]

    def picked(r):
        return pl.BlockSpec(
            (1, 2, BLOCK, width), lambda i, index_ref, flag_ref: (index_ref[r, i], 0, 0, 0)
        )

    return pl.pallas_call(
        functools.partial(attend_kernel, heads),
        grid_spec=pltpu.PrefetchScalarGridSpec(
            num_scalar_prefetch=2,
            grid=(blocks,),
            in_specs=[pl.BlockSpec((BLOCK, width), lambda i, a, b: (i, 0))]
            + [picked(r) for r in range(listed)],
            out_specs=pl.BlockSpec((BLOCK, width), lambda i, a, b: (i, 0)),
        ),
        out_shape=jax.ShapeDtypeStruct(queries.shape, jnp.bfloat16),
        compiler_params=pltpu.CompilerParams(dimension_semantics=("arbitrary",)),
        cost_estimate=pl.CostEstimate(
            flops=60 * tokens * width * 8 * BLOCK,
            bytes_accessed=blocks * 14 * BLOCK * width * 2,
            transcendentals=tokens * heads * 8 * BLOCK,
        ),
    )(index, flags, queries, *([pool] * listed))


def merged(left, right):
    joint = jnp.maximum(left[0], right[0])
    a, b = jnp.exp(left[0] - joint), jnp.exp(right[0] - joint)
    return (
        joint,
        left[1] * a + right[1] * b,
        left[2] * a[:, :, None] + right[2] * b[:, :, None],
    )


def partial_softmax(query, keys, values):
    tokens, width = query.shape
    heads = width // HEAD_DIM
    query = query.reshape(tokens, heads, HEAD_DIM)
    keys, values = (a.reshape(-1, heads, HEAD_DIM) for a in (keys, values))
    scores = jnp.einsum("qhd,khd->hqk", query, keys, preferred_element_type=jnp.float32)
    scores = scores * HEAD_DIM ** (-0.5)
    row_max = jnp.max(scores, axis=2)
    weight = jnp.exp(scores - row_max[:, :, None])
    row_total = jnp.sum(weight, axis=2)
    value = jnp.einsum(
        "hqk,khd->hqd", weight.astype(jnp.bfloat16), values, preferred_element_type=jnp.float32
    )
    return row_max, row_total, value


def after(array, *others):
    return lax.optimization_barrier((array,) + others)[0]


def local_plain(queries, key_rows, value_rows, random_owner, random_local, output_weight):
    n = lax.axis_size("seq")
    me = lax.axis_index("seq")
    heads_n = lax.axis_size("head")
    h = lax.axis_index("head")
    token_count, width_here = queries.shape
    nb = token_count // BLOCK
    gb = GLOBAL // BLOCK
    heads_here = width_here // HEAD_DIM
    slot_count = max(2, 4 * nb // n)
    depth = n // PAIR
    z, x = me // PAIR, me % PAIR

    def send(array, pairs, axis="seq"):
        return jax.tree.map(lambda part: lax.ppermute(part, axis, pairs), array)

    def swapped(array, m):
        return lax.ppermute(array, "head", [(i, i ^ m) for i in range(heads_n)])

    def folded(part, pairs, here):
        packed = jnp.concatenate([part[2], part[0][:, None], part[1][:, None]], axis=1)
        got = send(packed, pairs)
        both = merged(part, (got[:, GLOBAL], got[:, GLOBAL + 1], got[:, :GLOBAL]))
        return jax.tree.map(lambda a, b: jnp.where(here, a, b), both, part)

    def finished(part):
        out = jnp.transpose(part[2] / part[1][:, :, None], (1, 0, 2))
        return out.reshape(GLOBAL, -1).astype(jnp.bfloat16)

    chunks = math.gcd(CHUNKS, heads_here)
    cw = width_here // chunks
    cuts = [slice(c * cw, (c + 1) * cw) for c in range(chunks)]
    key_blocks = key_rows.reshape(nb, BLOCK, width_here)
    value_blocks = value_rows.reshape(nb, BLOCK, width_here)
    owned = [jnp.stack([key_blocks[..., sl], value_blocks[..., sl]], axis=1) for sl in cuts]
    up = [(i, i + 1) for i in range(n - 1)]
    down = [(i + 1, i) for i in range(n - 1)]
    mates = [(i, i + 1 if i % PAIR == 0 else i - 1) for i in range(n)]
    owner_flat = random_owner.reshape(-1)
    local_flat = random_local.reshape(-1)
    request_table, slot_ids = slot_table(owner_flat, local_flat, n, slot_count)
    line_wins = n % PAIR == 0 and nb <= PAIR * slot_count
    global_ids = jnp.arange(gb, dtype=jnp.int32)
    pools, tops, last = [], [], None

    if line_wins:
        mate_owner, mate_local = send((owner_flat, local_flat), mates)
        near_query = jnp.where(me == 1, send(queries[:GLOBAL], [(0, 1)]), queries[:GLOBAL])
        befores = [send(own[-1:], up) for own in owned]
        afters = [send(own[:1], down) for own in owned]
        mate_table, _ = slot_table(mate_owner, mate_local, n, slot_count)
        fetch = slot_count + gb
        mate_table = jnp.concatenate(
            [mate_table, jnp.broadcast_to(global_ids[None], (n, gb))], axis=1
        )
        offsets = [0]
        for s in range(1, depth):
            offsets += [-s, s]
        bufs = [{0: own} for own in owned]
        for s in range(1, depth):
            upward = [(i, i + PAIR) for i in range((s - 1) * PAIR, n - PAIR)]
            downward = [(i, i - PAIR) for i in range(PAIR, n - (s - 1) * PAIR)]
            for held in bufs:
                held[-s] = send(held[1 - s], upward)
                held[s] = send(held[s - 1], downward)
        for c in range(chunks):
            crossed = []
            for d in offsets:
                holder = jnp.clip((z + d) * PAIR + x, 0, n - 1)
                asked = jnp.take(bufs[c][d], mate_table[holder], axis=0)
                good = [(i, j) for i, j in mates if 0 <= i // PAIR + d < depth]
                crossed.append(send(asked, good))
            part = None
            for s in range(depth):
                held = bufs[c][s]
                term = partial_softmax(near_query[:, cuts[c]], held[:, 0], held[:, 1])
                part = term if part is None else merged(part, term)
            tops.append(finished(folded(part, [(1, 0)], me == 0)))
            pools.append(
                jnp.concatenate(
                    [bufs[c][d] for d in offsets] + crossed + [befores[c], afters[c]], axis=0
                )
            )
        last = bufs[0][depth - 1]
        place = jnp.where(owner_flat // PAIR < z, 2 * (z - owner_flat // PAIR) - 1,
                          2 * (owner_flat // PAIR - z))
        line_total = len(offsets) * nb
        cell = jnp.where(
            owner_flat % PAIR == x,
            place * nb + local_flat,
            line_total + place * fetch + slot_ids,
        )
        root = jnp.maximum(2 * z - 1, 0)
        global_cell = global_ids + jnp.where(
            x == 0, root * nb, line_total + root * fetch + slot_count
        )
        edge = line_total + len(offsets) * fetch
    else:
        rows = jnp.stack([queries[:GLOBAL], key_rows[:GLOBAL], value_rows[:GLOBAL]])
        rows = jnp.where(me == 1, send(rows, [(0, 1)]), rows)
        for s in range(1, depth):
            got = send(rows, [((s - 1) * PAIR + q, s * PAIR + q) for q in range(PAIR)])
            rows = jnp.where(z == s, got, rows)
        part = partial_softmax(rows[0], key_rows, value_rows)
        for s in range(depth - 1, 0, -1):
            pairs = [(s * PAIR + q, (s - 1) * PAIR + q) for q in range(PAIR)]
            part = folded(part, pairs, z == s - 1)
        top = finished(folded(part, [(1, 0)], me == 0))
        wanted = lax.all_to_all(request_table, "seq", split_axis=0, concat_axis=0, tiled=True)
        for c, own in enumerate(owned):
            tops.append(top[:, cuts[c]])
            sent = jnp.take(own, wanted.reshape(-1), axis=0)
            got = lax.all_to_all(sent, "seq", split_axis=0, concat_axis=0, tiled=True)
            shared = jnp.stack(
                [rows[i][:, cuts[c]].reshape(gb, BLOCK, cw) for i in (1, 2)], axis=1
            )
            edges = [send(own[-1:], up), send(own[:1], down)]
            pools.append(jnp.concatenate([own, got, shared] + edges, axis=0))
        cell = nb + owner_flat * slot_count + slot_ids
        global_cell = nb + n * slot_count + global_ids
        edge = nb + n * slot_count + gb

    weights, order, bit = [output_weight], [0], heads_n
    while bit > 1:
        bit //= 2
        for m in list(order):
            held = weights[order.index(m)]
            if m and last is not None:
                held = after(held, last)
            weights.append(swapped(held, bit))
            order.append(m ^ bit)

    steps = jnp.arange(nb, dtype=jnp.int32)
    cell = cell.reshape(nb, RANDOM)
    index = jnp.stack(
        [
            jnp.where(steps == 0, edge, steps - 1),
            steps,
            jnp.where(steps == nb - 1, edge + 1, steps + 1),
        ]
        + [cell[:, r] for r in range(RANDOM)]
        + [jnp.broadcast_to(global_cell[g], (nb,)) for g in range(gb)]
    ).astype(jnp.int32)
    numbers = me * nb + steps
    flags = jnp.stack([numbers == 0, numbers == n * nb - 1]).astype(jnp.int32)

    share = token_count // heads_n
    pieces = [[] for _ in order]
    for c, sl in enumerate(cuts):
        sparse = attend(queries[:, sl], pools[c], index, flags)
        top = jnp.where(me == 0, tops[c], sparse[:GLOBAL])
        sparse = jnp.concatenate([top, sparse[GLOBAL:]], axis=0)
        for k, m in enumerate(order):
            piece = lax.dynamic_slice_in_dim(sparse, (h ^ m) * share, share, 0)
            pieces[k].append(piece if m == 0 else swapped(piece, m))
    total = None
    for k in range(len(order)):
        term = jnp.dot(
            jnp.concatenate(pieces[k], axis=1), weights[k], preferred_element_type=jnp.float32
        )
        total = term if total is None else total + term
    return total.astype(jnp.bfloat16)


MESH = pl.DeviceIdType.MESH
RATE = HEAD_DIM ** (-0.5) * math.log2(math.e)
NT = (((1,), (1,)), ((), ()))


def attend_group(items):
    scores = [
        lax.dot_general(query, keys, NT, preferred_element_type=jnp.float32)
        for query, keys, _, _ in items
    ]
    scores = [a if item[3] is None else a + item[3] for a, item in zip(scores, items)]
    tops = [jnp.max(a, axis=1, keepdims=True) for a in scores]
    parts = [jnp.exp2((a - top) * RATE) for a, top in zip(scores, tops)]
    totals = [jnp.sum(a, axis=1, keepdims=True) for a in parts]
    accs = [
        jnp.dot(a.astype(jnp.bfloat16), item[2], preferred_element_type=jnp.float32)
        for a, item in zip(parts, items)
    ]
    return [
        (acc * (1.0 / total), top * RATE + jnp.log2(total))
        for acc, total, top in zip(accs, totals, tops)
    ]


def attend_all(query, k_ref, v_ref, step):
    rows = query.shape[0]
    cells = k_ref.shape[0]

    def chunk(c):
        keys = k_ref[pl.ds(c * step, step)].reshape(step * BLOCK, HEAD_DIM)
        values = v_ref[pl.ds(c * step, step)].reshape(step * BLOCK, HEAD_DIM)
        return query, keys, values, None

    def body(c, carry):
        for part in attend_group([chunk(2 * c), chunk(2 * c + 1)]):
            carry = joined(*carry, *part)
        return carry

    start = (
        jnp.zeros((rows, HEAD_DIM), jnp.float32),
        jnp.full((rows, 1), masked_score, jnp.float32),
    )
    return lax.fori_loop(0, cells // (2 * step), body, start)


def joined(o1, l1, o2, l2):
    top = jnp.maximum(l1, l2)
    a, b = jnp.exp2(l1 - top), jnp.exp2(l2 - top)
    total = a + b
    return (o1 * a + o2 * b) / total, top + jnp.log2(total)


def hub_kernel(heads, nb, picks, codes, q_hbm, k_hbm, v_hbm, w_hbm, out_ref, w_all, *rest):
    kcol, vcol = rest[:heads], rest[heads:2 * heads]
    (qown, qend, qmate, kwin, vwin, rsend, rrecv, ssend, srecv, esend, estat, loc, lstat, tmp,
     attn, attn_all, acc, wbuf, own_sem, col_sem, m1_s, m1_r, fw_s, fw_r,
     hb_s, hb_r, re_s, re_r, er_s, er_r, at_s, at_r, w_s, w_r, wl_sem, lc_sem,
     landed_codes, codes_s, cell_ref, bias_ref, cd_s, cd_r, cd_sem, p_in, p_s, p_r) = rest[2 * heads:]
    me = lax.axis_index("seq")
    h = lax.axis_index("head")
    n = lax.axis_size("seq")
    heads_n = lax.axis_size("head")
    z, x = me // PAIR, me % PAIR
    hub = jnp.logical_or(z == 1, z == 2)
    end = jnp.logical_not(hub)
    own_end = jnp.where(z == 1, 0, 3)
    partner = jnp.where(hub, jnp.where(z == 1, 0, 3), jnp.where(z == 0, 1, 2)) * PAIR + x
    other = (3 - z) * PAIR + x
    mate = z * PAIR + (1 - x)
    wide = HEAD_DIM
    columns = acc.shape[1]
    lanes = lambda i: slice(i * wide, (i + 1) * wide)
    finish = []

    def remote(src, dst, ss, rs, seq, head=None):
        return pltpu.make_async_remote_copy(
            src_ref=src, dst_ref=dst, send_sem=ss, recv_sem=rs,
            device_id=(seq, h if head is None else head), device_id_type=MESH,
        )

    def planes(p):
        return pl.ds(p * nb, nb)

    def m1(i):
        return [
            remote(k_hbm.at[:, :, lanes(i)], kcol[i].at[planes(z)], m1_s.at[i, 0], m1_r.at[i, 0], partner),
            remote(v_hbm.at[:, :, lanes(i)], vcol[i].at[planes(z)], m1_s.at[i, 1], m1_r.at[i, 1], partner),
            remote(q_hbm.at[:, :, lanes(i)], qend.at[i], m1_s.at[i, 2], m1_r.at[i, 2], partner),
        ]

    def forward(i):
        return [
            remote(kcol[i].at[planes(own_end)], kcol[i].at[planes(own_end)], fw_s.at[i, 0], fw_r.at[i, 0], other),
            remote(vcol[i].at[planes(own_end)], vcol[i].at[planes(own_end)], fw_s.at[i, 1], fw_r.at[i, 1], other),
            remote(qend.at[i], qmate.at[i, pl.ds(nb, nb)], fw_s.at[i, 2], fw_r.at[i, 2], mate),
        ]

    def first(i):
        return [
            remote(k_hbm.at[:, :, lanes(i)], kcol[i].at[planes(z)], hb_s.at[i, 0], hb_r.at[i, 0], other),
            remote(v_hbm.at[:, :, lanes(i)], vcol[i].at[planes(z)], hb_s.at[i, 1], hb_r.at[i, 1], other),
            remote(q_hbm.at[:, :, lanes(i)], qmate.at[i, pl.ds(0, nb)], hb_s.at[i, 2], hb_r.at[i, 2], mate),
        ]

    def results(i, j):
        to = (mate, own_end * PAIR + 1 - x)[j]
        return [
            remote(part.at[i, j], into.at[i, j], re_s.at[i, j, k], re_r.at[i, j, k], to)
            for k, (part, into) in enumerate(((rsend, rrecv), (ssend, srecv)))
        ]

    def ended(i):
        return [
            remote(esend.at[i], rrecv.at[i, 0], er_s.at[i, 0], er_r.at[i, 0], partner),
            remote(estat.at[i], srecv.at[i, 0], er_s.at[i, 1], er_r.at[i, 1], partner),
        ]

    def shares(i):
        if i < EARLY:
            return [
                remote(attn.at[i, h ^ 1], attn_all.at[i, h], at_s.at[i, 0], at_r.at[i, 0], me, h ^ 1),
                remote(attn.at[i, h ^ 3], attn_all.at[i, h ^ 2], at_s.at[i, 1], at_r.at[i, 1], me, h ^ 1),
            ]
        return [
            remote(attn.at[i, h ^ k], attn_all.at[i, h], at_s.at[i, k - 1], at_r.at[i, k - 1], me, h ^ k)
            for k in range(1, heads_n)
        ]

    def kept(i):
        return [
            pltpu.make_async_copy(attn.at[i, h ^ k], attn_all.at[i, h ^ k], lc_sem.at[i, k // 2])
            for k in ((0, 2) if i < EARLY else (0,))
        ]

    def partials(part):
        half = pl.ds(part * columns // 2, columns // 2)
        return [remote(out_ref.at[:, half], p_in.at[:, half], p_s.at[part], p_r.at[part], me, h ^ 2)]

    def weights(i):
        return [
            remote(w_hbm.at[i], w_all.at[h, i], w_s.at[i, 0], w_r.at[i, 0], me, h ^ 2),
            remote(w_hbm.at[i], w_all.at[h, i], w_s.at[i, 1], w_r.at[i, 1], me, h ^ 1),
            remote(w_all.at[h ^ 2, i], w_all.at[h ^ 2, i], w_s.at[i, 2], w_r.at[i, 2], me, h ^ 1),
        ]

    def own_copies():
        return [
            pltpu.make_async_copy(q_hbm, qown, own_sem.at[0]),
            pltpu.make_async_copy(k_hbm, kwin.at[pl.ds(1, nb)], own_sem.at[1]),
            pltpu.make_async_copy(v_hbm, vwin.at[pl.ds(1, nb)], own_sem.at[2]),
        ]

    def column(i):
        return [
            pltpu.make_async_copy(k_hbm.at[:, :, lanes(i)], kcol[i].at[planes(z)], col_sem.at[i, 0]),
            pltpu.make_async_copy(v_hbm.at[:, :, lanes(i)], vcol[i].at[planes(z)], col_sem.at[i, 1]),
        ]

    def start(copies):
        for copy in copies:
            copy.start()

    def landed(copies):
        for copy in copies:
            copy.wait_recv()

    def sent(copies):
        for copy in copies:
            copy.wait_send()

    def pump(i):
        coming = m1(i)
        landed(coming[:2])
        start(forward(i)[:2])
        coming[2].wait_recv()
        start(forward(i)[2:])
        if i + 1 < heads:
            start(first(i + 1))

    def code_copies():
        hub_of = jnp.where(hub, z, jnp.where(z == 0, 1, 2)) * PAIR
        return [
            remote(codes, landed_codes.at[0], cd_s.at[0], cd_r.at[0], hub_of + x),
            remote(codes, landed_codes.at[1], cd_s.at[1], cd_r.at[1], mate),
            remote(codes, landed_codes.at[2], cd_s.at[2], cd_r.at[2], hub_of + 1 - x),
        ]

    to_hub, to_mate, to_other = code_copies()

    @pl.when(end)
    def _():
        start([to_hub, to_other])
        start(m1(0))

    @pl.when(hub)
    def _():
        start([to_mate])
        start(first(0))

    for copy in own_copies():
        copy.start()
    own_code = pltpu.make_async_copy(codes, codes_s.at[0], cd_sem.at[0])
    own_code.start()

    @pl.when(end)
    def _():
        for i in range(1, heads):
            start(m1(i))

    @pl.when(hub)
    def _():
        for i in range(heads):
            start(column(i))

    for i in range(EARLY, heads):
        weights(i)[0].start()
    for i in range(heads):
        weights(i)[1].start()

    for spot in (0, nb + 1):
        kwin[spot] = jnp.zeros(kwin.shape[1:], kwin.dtype)
        vwin[spot] = jnp.zeros(vwin.shape[1:], vwin.dtype)

    own_code.wait()

    @pl.when(hub)
    def _():
        landed([to_hub, to_mate, to_other])
        for j in range(3):
            pltpu.make_async_copy(landed_codes.at[j], codes_s.at[1 + j], cd_sem.at[1 + j]).start()
        for j in range(3):
            pltpu.make_async_copy(landed_codes.at[j], codes_s.at[1 + j], cd_sem.at[1 + j]).wait()
        for j in range(4):
            def fill(b, _):
                for r in range(RANDOM):
                    here = codes_s[j, 1, b * RANDOM + r] == x
                    spot = (j * nb + b) * picks + r
                    cell_ref[spot] = jnp.where(here, codes_s[j, 0, b * RANDOM + r], 0)
                    bias_ref[spot] = jnp.where(here, 0.0, masked_score)
                for r in range(RANDOM, picks - 1):
                    spot = (j * nb + b) * picks + r
                    cell_ref[spot] = r - RANDOM
                    bias_ref[spot] = jnp.where(x == 0, 0.0, masked_score)
                home = jnp.where(j % 2 == 0, z, own_end) * PAIR + jnp.where(j < 2, x, 1 - x)
                beside = jnp.where(b == 0, home - 1, home + 1)
                known = jnp.logical_and(beside >= 0, beside < n)
                known = jnp.logical_and(known, jnp.logical_or(b == 0, b == nb - 1))
                spot = (j * nb + b) * picks + picks - 1
                cell_ref[spot] = jnp.where(known, beside // PAIR * nb + jnp.where(b == 0, nb - 1, 0), 0)
                bias_ref[spot] = jnp.where(known, 0.0, masked_score)
                return _

            lax.fori_loop(0, nb, fill, 0)

    for copy in own_copies():
        copy.wait()

    row = lax.broadcasted_iota(jnp.int32, (1, 3 * BLOCK), 1) // BLOCK
    lane = lax.broadcasted_iota(jnp.int32, (BLOCK, 128), 1)
    pick_row = lax.broadcasted_iota(jnp.int32, (1, picks * BLOCK), 1) // BLOCK

    def stat(i, value, table):
        return jnp.where(lane == i, value, table)

    def read_stat(i, table):
        return jnp.sum(jnp.where(lane == i, table, 0.0), axis=1, keepdims=True)

    def window_bias(b):
        gone = jnp.logical_or(
            jnp.logical_and(row == 0, b == 0), jnp.logical_and(row == 2, b == nb - 1)
        )
        return jnp.where(gone, masked_score, 0.0).astype(jnp.float32)

    def listed(i, number, count):
        cells = [cell_ref[number * picks + r] for r in range(count)]
        keys = [kcol[i][cell] for cell in cells]
        values = [vcol[i][cell] for cell in cells]
        bias = jnp.full((1, count * BLOCK), bias_ref[number * picks], jnp.float32)
        for r in range(1, count):
            bias = jnp.where(pick_row[:, :count * BLOCK] == r, bias_ref[number * picks + r], bias)
        return keys, values, bias

    def window(i, b):
        keys = [kwin[b + s, :, lanes(i)] for s in range(3)]
        values = [vwin[b + s, :, lanes(i)] for s in range(3)]
        return keys, values, window_bias(b)

    def item(query, lists):
        keys = jnp.concatenate([k for part in lists for k in part[0]], axis=0)
        values = jnp.concatenate([v for part in lists for v in part[1]], axis=0)
        bias = jnp.concatenate([part[2] for part in lists], axis=1) if len(lists) > 1 else lists[0][2]
        return query, keys, values, bias

    def looped(count, unroll, body, table):
        def step(j, table):
            return body([j * unroll + u for u in range(unroll)], table)

        return lax.fori_loop(0, count // unroll, step, table)

    def attend_loop(unroll, item_of, store, base, table, lse_of=None):
        def body(blocks, table):
            done = attend_group([item_of(b) for b in blocks])
            for b, (out, lse) in zip(blocks, done):
                store(b, out)
                table = stat(base + b, lse if lse_of is None else lse_of(b, lse), table)
            return table

        return looped(nb, unroll, body, table)

    def global_rows(i, query_of, store, table, base):
        query = jnp.concatenate([query_of(g) for g in range(GLOBAL // BLOCK)], axis=0)
        out, lse = attend_all(query, kcol[i], vcol[i], 8)
        for g in range(GLOBAL // BLOCK):
            part = slice(g * BLOCK, (g + 1) * BLOCK)
            store(g, out[part])
            table[...] = stat(base + g, lse[part], table[...])

    def packed(table):
        return jnp.transpose(table)[:nb]

    def unpacked(rows):
        wide_rows = jnp.concatenate([rows, jnp.zeros((128 - nb, BLOCK), jnp.float32)], axis=0)
        return jnp.transpose(wide_rows)

    blank = jnp.zeros((BLOCK, 128), jnp.float32)

    def compute_hub(i):
        landed(forward(i))
        landed(first(i))
        for copy in column(i):
            copy.wait()

        def to_mate_set(j):
            def put_mate(b, out):
                rsend[i, j, b] = out.astype(jnp.bfloat16)

            tmp[...] = attend_loop(
                UNROLL, lambda b: item(qmate[i, j * nb + b], [listed(i, (2 + j) * nb + b, picks)]),
                put_mate, 0, blank,
            )
            if j == 1:
                @pl.when(jnp.logical_and(z == 1, x == 1))
                def _():
                    global_rows(i, lambda g: qmate[i, nb + g], put_mate, tmp, 0)

            ssend[i, j] = packed(tmp[...])
            start(results(i, j))

        def put_end(b, out):
            esend[i, b] = out.astype(jnp.bfloat16)

        to_mate_set(1)
        to_mate_set(0)
        tmp[...] = attend_loop(
            UNROLL, lambda b: item(qend[i, b], [listed(i, nb + b, picks - 1)]), put_end, 0, blank
        )

        @pl.when(jnp.logical_and(z == 1, x == 0))
        def _():
            global_rows(i, lambda g: qend[i, g], put_end, tmp, 0)

        estat[i] = packed(tmp[...])
        start(ended(i))

        def put_own(b, out):
            loc[i % 2, b] = out

        lstat[i % 2] = attend_loop(
            UNROLL // 2, lambda b: item(qown[b, :, lanes(i)], [window(i, b), listed(i, b, picks - 1)]),
            put_own, 0, blank,
        )

    def compute_end(i):
        def put_own(b, out):
            loc[i % 2, b] = out

        def lse_of(b, lse):
            replaced = jnp.logical_and(me == 0, b < GLOBAL // BLOCK)
            return jnp.where(replaced, masked_score, lse)

        lstat[i % 2] = attend_loop(
            UNROLL, lambda b: item(qown[b, :, lanes(i)], [window(i, b)]), put_own, 0, blank, lse_of
        )

    def put_attn(i, b, value):
        per = nb // heads_n
        attn[i, b // per, pl.ds(pl.multiple_of((b % per) * BLOCK, BLOCK), BLOCK)] = value.astype(jnp.bfloat16)

    def merge_own(i, count):
        ours = lstat[i % 2]
        theirs = [unpacked(srecv[i, j]) for j in range(count)]

        def body(blocks, _):
            done = [(loc[i % 2, b], read_stat(b, ours)) for b in blocks]
            for j in range(count):
                done = [
                    joined(*part, rrecv[i, j, b].astype(jnp.float32), read_stat(b, theirs[j]))
                    for part, b in zip(done, blocks)
                ]
            for b, (out, _lse) in zip(blocks, done):
                put_attn(i, b, out)
            return _

        looped(nb, UNROLL, body, 0)

    def merge_hub(i):
        landed(results(i, 0))
        merge_own(i, 1)

    def merge_end(i):
        landed(results(i, 1))
        landed(ended(i))
        merge_own(i, 2)

    def share(i):
        start(shares(i))
        start(kept(i))

    def load_weights(i):
        copies = []
        for k in range(heads_n):
            source = (w_hbm.at[i] if k == 0 else w_all.at[h ^ k, i])
            target = wbuf.at[i % 2, pl.ds((h ^ k) * wide, wide)]
            copies.append(pltpu.make_async_copy(source, target, wl_sem.at[i % 2, k]))
        return copies

    def load_early():
        copies = []
        for i in range(EARLY):
            for k in range(2):
                source = (w_hbm.at[i] if k == 0 else w_all.at[h ^ k, i])
                spot = i % 2 * 2 + k
                target = wbuf.at[i // 2, pl.ds(spot * wide, wide)]
                copies.append(pltpu.make_async_copy(source, target, wl_sem.at[i // 2, spot]))
        return copies

    def settled(i):
        landed(shares(i))
        for copy in kept(i):
            copy.wait()

    def tiles(first, last, body):
        def step(c, _):
            body(pl.ds(pl.multiple_of(c * TILE, TILE), TILE))
            return _

        lax.fori_loop(first // TILE, last // TILE, step, 0)

    def project_early(part):
        if part == 0:
            for i in range(EARLY):
                settled(i)
            for copy in load_early():
                copy.wait()
        both = []
        for k in (0, 2):
            sides = [attn_all[i, h ^ k ^ c] for i in range(EARLY) for c in range(2)]
            both.append([jnp.concatenate(sides[s:s + 4], axis=1) for s in range(0, len(sides), 4)])

        def body(here):
            own, away = [
                sum(
                    jnp.dot(left, wbuf[s, :left.shape[1], here], preferred_element_type=jnp.float32)
                    for s, left in enumerate(lefts)
                )
                for lefts in both
            ]
            acc[:, here] = own
            out_ref[:, here] = away.astype(jnp.bfloat16)

        tiles(part * columns // 2, (part + 1) * columns // 2, body)
        start(partials(part))

    def project(i):
        settled(i)
        for copy in load_weights(i):
            copy.wait()
        left = jnp.concatenate([attn_all[i, g] for g in range(heads_n)], axis=1)

        def body(here):
            term = jnp.dot(left, wbuf[i % 2, :, here], preferred_element_type=jnp.float32)
            term = term + acc[:, here]
            if i < heads - 1:
                acc[:, here] = term
            else:
                term = term + p_in[:, here].astype(jnp.float32)
                out_ref[:, here] = term.astype(jnp.bfloat16)

        tiles(0, columns, body)

    @pl.when(hub)
    def _():
        pump(0)
        pump(1)

    def fetch(i):
        landed(weights(i)[1:])
        for copy in load_weights(i):
            copy.start()

    def relay(i):
        weights(i)[0].wait_recv()
        weights(i)[2].start()

    def merge(i):
        @pl.when(hub)
        def _():
            merge_hub(i)

        @pl.when(end)
        def _():
            merge_end(i)

    for t in range(heads):
        if t == EARLY:
            for i in range(EARLY):
                weights(i)[1].wait_recv()
            for copy in load_early():
                copy.start()
        if t - 2 >= EARLY:
            fetch(t - 2)
        if t >= 1:
            merge(t - 1)
            share(t - 1)
        if EARLY <= t + 1 < heads:
            relay(t + 1)
        if t - 2 >= EARLY:
            project(t - 2)

        @pl.when(hub)
        def _():
            compute_hub(t)
            if t + 2 < heads:
                pump(t + 2)

        @pl.when(end)
        def _():
            compute_end(t)

        if 0 <= t - EARLY < 2:
            project_early(t - EARLY)

    fetch(heads - 2)
    fetch(heads - 1)
    project(heads - 2)
    merge(heads - 1)
    share(heads - 1)
    for part in range(2):
        sent(partials(part))
        landed(partials(part))
    project(heads - 1)

    @pl.when(end)
    def _():
        sent([to_hub, to_other])

    @pl.when(hub)
    def _():
        sent([to_mate])

    for i in range(heads):
        @pl.when(end)
        def _():
            sent(m1(i))

        @pl.when(hub)
        def _():
            sent(forward(i))
            sent(first(i))
            sent(results(i, 0))
            sent(results(i, 1))
            sent(ended(i))

        sent(shares(i))
        sent(weights(i)[1:2] if i < EARLY else weights(i))


UNROLL = 4
EARLY = 3
TILE = 2048


def hub_attention(codes, q, k, v, w, picks):
    nb, _, width = q.shape
    heads, wide, columns = w.shape
    heads_n = lax.axis_size("head")
    planes = lax.axis_size("seq") // PAIR
    rows = nb * BLOCK
    share = rows // heads_n
    bf, f32 = jnp.bfloat16, jnp.float32
    dma = pltpu.SemaphoreType.DMA
    col = [pltpu.VMEM((planes * nb, BLOCK, wide), bf)] * (2 * heads)
    scratch = col + [
        pltpu.VMEM((nb, BLOCK, width), bf),
        pltpu.VMEM((heads, nb, BLOCK, wide), bf),
        pltpu.VMEM((heads, 2 * nb, BLOCK, wide), bf),
        pltpu.VMEM((nb + 2, BLOCK, width), bf),
        pltpu.VMEM((nb + 2, BLOCK, width), bf),
        pltpu.VMEM((heads, 2, nb, BLOCK, wide), bf),
        pltpu.VMEM((heads, 2, nb, BLOCK, wide), bf),
        pltpu.VMEM((heads, 2, nb, BLOCK), f32),
        pltpu.VMEM((heads, 2, nb, BLOCK), f32),
        pltpu.VMEM((heads, nb, BLOCK, wide), bf),
        pltpu.VMEM((heads, nb, BLOCK), f32),
        pltpu.VMEM((2, nb, BLOCK, wide), f32),
        pltpu.VMEM((2, BLOCK, 128), f32),
        pltpu.VMEM((BLOCK, 128), f32),
        pltpu.VMEM((heads, heads_n, share, wide), bf),
        pltpu.VMEM((heads, heads_n, share, wide), bf),
        pltpu.VMEM((share, columns), f32),
        pltpu.VMEM((2, heads_n * wide, columns), bf),
        dma((3,)), dma((heads, 2)),
        dma((heads, 3)), dma((heads, 3)), dma((heads, 3)), dma((heads, 3)),
        dma((heads, 3)), dma((heads, 3)), dma((heads, 2, 2)), dma((heads, 2, 2)),
        dma((heads, 2)), dma((heads, 2)), dma((heads, 3)), dma((heads, 3)),
        dma((heads, 3)), dma((heads, 3)), dma((2, heads_n)), dma((heads, 2)),
        pltpu.VMEM((3,) + codes.shape, jnp.int32), pltpu.SMEM((4,) + codes.shape, jnp.int32),
        pltpu.SMEM((4 * nb * picks,), jnp.int32), pltpu.SMEM((4 * nb * picks,), f32),
        dma((3,)), dma((3,)), dma((4,)),
        pltpu.VMEM((share, columns), bf), dma((2,)), dma((2,)),
    ]
    anywhere = pl.BlockSpec(memory_space=pl.ANY)
    out, _ = pl.pallas_call(
        functools.partial(hub_kernel, heads, nb, picks),
        out_shape=(
            jax.ShapeDtypeStruct((share, columns), bf),
            jax.ShapeDtypeStruct((heads_n,) + w.shape, bf),
        ),
        in_specs=[anywhere] * 5,
        out_specs=(pl.BlockSpec(memory_space=pltpu.VMEM), anywhere),
        scratch_shapes=scratch,
        compiler_params=pltpu.CompilerParams(
            has_side_effects=True, vmem_limit_bytes=67043328
        ),
    )(codes, q, k, v, w)
    return out


def local_hub(queries, key_rows, value_rows, random_owner, random_local, output_weight):
    rows, width = queries.shape
    nb = rows // BLOCK
    heads = width // HEAD_DIM
    cell = random_owner // PAIR * nb + random_local
    codes = jnp.stack([cell.reshape(-1), (random_owner % PAIR).reshape(-1)])
    codes = jnp.pad(codes, ((0, 6), (0, 128 - codes.shape[1])))
    blocks = lambda a: a.reshape(nb, BLOCK, width)
    return hub_attention(
        codes, blocks(queries), blocks(key_rows), blocks(value_rows),
        output_weight.reshape(heads, HEAD_DIM, -1), RANDOM + GLOBAL // BLOCK + 1,
    )


def local(queries, *others):
    n, heads_n = lax.axis_size("seq"), lax.axis_size("head")
    if n == 4 * PAIR and heads_n == 4:
        return local_hub(queries, *others)
    return local_plain(queries, *others)


def solution(mesh):
    in_specs = (
        P("seq", "head"),
        P("seq", "head"),
        P("seq", "head"),
        P("seq", None),
        P("seq", None),
        P("head", None),
    )
    out_specs = P(("seq", "head"), None)
    return jax.shard_map(local, mesh=mesh, in_specs=in_specs, out_specs=out_specs, check_vma=False)
```
